32 devices in a mesh: dp: 8 (over y, x, core), tensor: 4 (over z).
Axes of the slice: x: 2, y: 2, z: 4, core: 2. Of those that a mesh axis runs over, the one named last changes fastest.
Arguments:
- block_input: bfloat16 [8192, 2048], P(('dp', 'tensor')), may hold values from -60 to 60
- gain_attn: float32 [2048], P(('dp', 'tensor')), may hold values from 0.1 to 1.9
- gain_mlp: float32 [2048], P(('dp', 'tensor')), may hold values from 0.1 to 1.9
- w_query: bfloat16 [2048, 2048], P('dp', 'tensor'), may hold values from -4 to 4
- key_projection_weight: bfloat16 [2048, 256], P('dp', 'tensor'), may hold values from -0.125 to 0.125
- value_projection_weight: bfloat16 [2048, 256], P('dp', 'tensor'), may hold values from -0.125 to 0.125
- w_out: bfloat16 [2048, 2048], P('tensor', 'dp'), may hold values from -0.75 to 0.75
- w_gate: bfloat16 [2048, 5632], P('dp', 'tensor'), may hold values from -0.125 to 0.125
- w_up: bfloat16 [2048, 5632], P('dp', 'tensor'), may hold values from -0.125 to 0.125
- w_down: bfloat16 [5632, 2048], P('tensor', 'dp'), may hold values from -0.078125 to 0.078125
- cotangent: bfloat16 [8192, 2048], P(('dp', 'tensor')), may hold values from -6 to 6
Outputs:
- block_output: bfloat16 [8192, 2048], P(('dp', 'tensor'))
- input_grad: bfloat16 [8192, 2048], P(('dp', 'tensor'))
- grad_gain_attn: float32 [2048], P(('dp', 'tensor'))
- grad_gain_mlp: float32 [2048], P(('dp', 'tensor'))
- grad_query: float32 [2048, 2048], P('dp', 'tensor')
- grad_key: float32 [2048, 256], P('dp', 'tensor')
- grad_value: float32 [2048, 256], P('dp', 'tensor')
- grad_out: float32 [2048, 2048], P('tensor', 'dp')
- grad_gate: float32 [2048, 5632], P('dp', 'tensor')
- grad_up: float32 [2048, 5632], P('dp', 'tensor')
- grad_down: float32 [5632, 2048], P('tensor', 'dp')
The draws below stay inside these ranges and needn't reach their ends.
All inputs are finite; a program needn't handle non-finite values.
Results may differ from the reference program's by a relative error of at most 0.025.
The reference program's roundings to bfloat16 on the way count: a program that leaves them out, or rounds other values in their place, can miss the bound.
Values may be sent and summed in bfloat16 or wider, within the bound.
A program may use at most 256 MiB of HBM per device.

```python
import math
import jax
import jax.numpy as jnp
from jax import lax

MODEL_WIDTH = 2048
HQ = 32
KEY_VALUE_HEADS = 4
HEAD_SIZE = 64
FF = 5632
SEQ = 1024
TOKENS = 8192
N_DP = 8
N_TENSOR = 4


def draw_block_input(key, part):
    key_base = jax.random.fold_in(key, 11)
    key_scale = jax.random.fold_in(key, 12)
    row_scales = jnp.exp(jax.random.uniform(key_scale, (TOKENS, 1), jnp.float32, 0.0, math.log(10.0)))
    base = jnp.clip(jax.random.normal(key_base, (TOKENS, MODEL_WIDTH), jnp.float32), -6.0, 6.0)
    return (base * row_scales).astype(jnp.bfloat16)


def draw_w_query(key, part):
    key_base = jax.random.fold_in(key, 21)
    base = jnp.clip(jax.random.normal(key_base, (MODEL_WIDTH, HQ * HEAD_SIZE), jnp.float32), -6.0, 6.0) * MODEL_WIDTH ** (-0.5)
    base = jnp.clip(base, -4.0, 4.0)
    return base.astype(jnp.bfloat16)


def block_scale(rng, extent, shards, least, largest):
    level = 1.0
    for dim, blocks in shards:
        draws = jax.random.uniform(jax.random.fold_in(jax.random.fold_in(rng, 6), dim), (blocks,), jnp.float32, least / len(shards), largest / len(shards))
        level = level * jnp.repeat(jnp.exp(draws), extent[dim] // blocks).reshape((-1,) + (1,) * (len(extent) - 1 - dim))
    return level


def scatter_about(stream_key, dims, scale, bound, shards=(), held_as=jnp.bfloat16):
    gain = block_scale(stream_key, dims, shards, -0.22, 0.18) if shards else 1.0
    entries = jax.random.normal(stream_key, dims, jnp.float32) * scale * gain
    return jnp.minimum(jnp.maximum(entries, -bound), bound).astype(held_as)


def setup_inputs(seed: int = 0) -> dict:
    arg_keys = jax.random.split(jax.random.key(seed), 12)
    return {
        "block_input": draw_block_input(jax.random.fold_in(arg_keys[11], 71), 0),
        "gain_attn": jnp.clip(1.0 + 0.18 * jax.random.normal(arg_keys[1], (MODEL_WIDTH,), jnp.float32), 0.1, 1.9),
        "gain_mlp": jnp.clip(1.0 + 0.18 * jax.random.normal(arg_keys[2], (MODEL_WIDTH,), jnp.float32), 0.1, 1.9),
        "w_query": draw_w_query(jax.random.fold_in(arg_keys[11], 71), 0),
        "key_projection_weight": scatter_about(arg_keys[4], (MODEL_WIDTH, KEY_VALUE_HEADS * HEAD_SIZE), MODEL_WIDTH ** -0.5, 0.125, ((0, 8), (1, 4))),
        "value_projection_weight": scatter_about(arg_keys[5], (MODEL_WIDTH, KEY_VALUE_HEADS * HEAD_SIZE), MODEL_WIDTH ** -0.5, 0.125, ((0, 8), (1, 4))),
        "w_out": scatter_about(arg_keys[6], (HQ * HEAD_SIZE, MODEL_WIDTH), HEAD_SIZE ** -0.5, 0.75, ((0, 4), (1, 8))),
        "w_gate": scatter_about(arg_keys[7], (MODEL_WIDTH, FF), MODEL_WIDTH ** -0.5, 0.125, ((0, 8), (1, 4))),
        "w_up": scatter_about(arg_keys[8], (MODEL_WIDTH, FF), MODEL_WIDTH ** -0.5, 0.125, ((0, 8), (1, 4))),
        "w_down": scatter_about(arg_keys[9], (FF, MODEL_WIDTH), FF ** -0.5, 0.078125, ((0, 4), (1, 8))),
        "cotangent": scatter_about(arg_keys[10], (TOKENS, MODEL_WIDTH), 1.0, 6.0, ((0, 32),)),
    }


EPS = 1e-05
ROPE_BASE = 10000.0
NEG_LARGE = -1e+30

def widen(tensor):
    return lax.optimization_barrier(tensor).astype(jnp.float32)

def split_sum(pairs):
    total = jnp.zeros((pairs[0][0].shape[0], pairs[0][1].shape[1]), jnp.float32)
    for group in range(N_TENSOR):
        partial_term = jnp.zeros(total.shape, jnp.float32)
        for left, right in pairs:
            width = left.shape[1] // N_TENSOR
            partial_term = partial_term + jnp.dot(left[:, group * width:(group + 1) * width], right[group * width:(group + 1) * width], preferred_element_type=jnp.float32)
        total = total + widen(partial_term.astype(jnp.bfloat16))
    return total

def rope_tables(sequence_length, head_dim):
    half_dim = head_dim // 2
    frequency = ROPE_BASE ** (-(jnp.arange(half_dim, dtype=jnp.float32) * 2.0) / head_dim)
    angles = jnp.arange(sequence_length, dtype=jnp.float32)[:, None] * frequency[None, :]
    return (jnp.cos(angles)[:, None, :], jnp.sin(angles)[:, None, :])

def apply_rotary(tensor, cosine_lookup, sine_lookup):
    half_dim = tensor.shape[-1] // 2
    lower_half = tensor[..., :half_dim]
    upper_half = tensor[..., half_dim:]
    return jnp.concatenate([lower_half * cosine_lookup - upper_half * sine_lookup, upper_half * cosine_lookup + lower_half * sine_lookup], axis=-1)

def invert_rotary(tensor, cosine_lookup, sine_lookup):
    half_dim = tensor.shape[-1] // 2
    lower_half = tensor[..., :half_dim]
    upper_half = tensor[..., half_dim:]
    return jnp.concatenate([lower_half * cosine_lookup + upper_half * sine_lookup, upper_half * cosine_lookup - lower_half * sine_lookup], axis=-1)

def causal_scores(query_block, keys_seen, first_row, score_scale):
    block_rows, q_heads, head_dim = query_block.shape
    kv_heads = keys_seen.shape[1]
    grouped = query_block.reshape(block_rows, kv_heads, q_heads // kv_heads, head_dim)
    scores = jnp.einsum('qhgd,khd->hgqk', widen(grouped), widen(keys_seen)) * score_scale
    row_pos = first_row + jnp.arange(block_rows)[:, None]
    col_pos = jnp.arange(keys_seen.shape[0])[None, :]
    return (jnp.where(col_pos <= row_pos, scores, NEG_LARGE), grouped)

def attend(queries, key_rows, value_rows):
    sequence_length, q_heads, head_dim = queries.shape
    block_rows = min(512, sequence_length)
    score_scale = 1.0 / math.sqrt(head_dim)
    outputs = []
    totals = []
    for first_row in range(0, sequence_length, block_rows):
        last_row = first_row + block_rows
        scores, grouped = causal_scores(queries[first_row:last_row], key_rows[:last_row], first_row, score_scale)
        peak = lax.optimization_barrier(jnp.max(scores, axis=-1, keepdims=True))
        log_total = peak + jnp.log(lax.optimization_barrier(jnp.sum(jnp.exp(scores - peak), axis=-1, keepdims=True)))
        weights = jnp.exp(scores - log_total).astype(jnp.bfloat16)
        mixed = jnp.einsum('hgqk,khd->qhgd', widen(weights), widen(value_rows[:last_row]))
        outputs.append(mixed.reshape(block_rows, q_heads, head_dim).astype(jnp.bfloat16))
        totals.append(log_total[..., 0])
    return (jnp.concatenate(outputs, axis=0), jnp.concatenate(totals, axis=2))

def attend_back(queries, key_rows, value_rows, outputs, log_totals, grad_outputs):
    sequence_length, q_heads, head_dim = queries.shape
    kv_heads = key_rows.shape[1]
    block_rows = min(512, sequence_length)
    score_scale = 1.0 / math.sqrt(head_dim)
    grad_keys = jnp.zeros(key_rows.shape, jnp.float32)
    grad_values = jnp.zeros(value_rows.shape, jnp.float32)
    query_parts = []
    for first_row in range(0, sequence_length, block_rows):
        last_row = first_row + block_rows
        scores, grouped = causal_scores(queries[first_row:last_row], key_rows[:last_row], first_row, score_scale)
        probs = jnp.exp(scores - log_totals[:, :, first_row:last_row, None])
        weights = probs.astype(jnp.bfloat16)
        grad_block = grad_outputs[first_row:last_row].reshape(block_rows, kv_heads, q_heads // kv_heads, head_dim)
        out_block = outputs[first_row:last_row].reshape(block_rows, kv_heads, q_heads // kv_heads, head_dim)
        grad_values = grad_values.at[:last_row].add(jnp.einsum('hgqk,qhgd->khd', widen(weights), widen(grad_block)))
        grad_probs = jnp.einsum('qhgd,khd->hgqk', widen(grad_block), widen(value_rows[:last_row]))
        delta = jnp.einsum('qhgd,qhgd->hgq', widen(grad_block), widen(out_block))
        grad_scores = (probs * (grad_probs - delta[..., None]) * score_scale).astype(jnp.bfloat16)
        query_parts.append(jnp.einsum('hgqk,khd->qhgd', widen(grad_scores), widen(key_rows[:last_row])).reshape(block_rows, q_heads, head_dim))
        grad_keys = grad_keys.at[:last_row].add(jnp.einsum('hgqk,qhgd->khd', widen(grad_scores), widen(grouped)))
    return (jnp.concatenate(query_parts, axis=0), grad_keys, grad_values)

def layer(block_rows_in, gain_attn, gain_mlp, w_query, key_projection_weight, value_projection_weight, w_out, w_gate, w_up, w_down, cotangent):
    sequence_length = block_rows_in.shape[0]
    cosine_lookup, sine_lookup = rope_tables(sequence_length, HEAD_SIZE)
    xfloat = block_rows_in.astype(jnp.float32)
    inv_rms_attn = lax.rsqrt(lax.optimization_barrier(jnp.mean(xfloat * xfloat, axis=1, keepdims=True)) + EPS)
    attention_norm = (xfloat * inv_rms_attn * gain_attn).astype(jnp.bfloat16)
    queries = apply_rotary(jnp.dot(attention_norm, w_query, preferred_element_type=jnp.float32).reshape(sequence_length, HQ, HEAD_SIZE), cosine_lookup, sine_lookup).astype(jnp.bfloat16)
    key_rows = apply_rotary(jnp.dot(attention_norm, key_projection_weight, preferred_element_type=jnp.float32).reshape(sequence_length, KEY_VALUE_HEADS, HEAD_SIZE), cosine_lookup, sine_lookup).astype(jnp.bfloat16)
    value_rows = jnp.dot(attention_norm, value_projection_weight, preferred_element_type=jnp.float32).astype(jnp.bfloat16).reshape(sequence_length, KEY_VALUE_HEADS, HEAD_SIZE)
    attended, log_totals = attend(queries, key_rows, value_rows)
    attended_flat = attended.reshape(sequence_length, HQ * HEAD_SIZE)
    mid = xfloat + split_sum([(attended_flat, w_out)])
    inv_rms_mlp = lax.rsqrt(lax.optimization_barrier(jnp.mean(mid * mid, axis=1, keepdims=True)) + EPS)
    norm_mlp = (mid * inv_rms_mlp * gain_mlp).astype(jnp.bfloat16)
    gate_act = jnp.dot(norm_mlp, w_gate, preferred_element_type=jnp.float32)
    up_act = jnp.dot(norm_mlp, w_up, preferred_element_type=jnp.float32)
    sigmoid_gate = jax.nn.sigmoid(gate_act)
    hidden = (gate_act * sigmoid_gate * up_act).astype(jnp.bfloat16)
    block_output = (mid + split_sum([(hidden, w_down)])).astype(jnp.bfloat16)
    grad_down = jnp.dot(hidden.T, cotangent, preferred_element_type=jnp.float32)
    grad_hidden = jnp.dot(cotangent, w_down.T, preferred_element_type=jnp.float32)
    grad_gate_act = (grad_hidden * up_act * sigmoid_gate * (1.0 + gate_act * (1.0 - sigmoid_gate))).astype(jnp.bfloat16)
    grad_up_act = (grad_hidden * gate_act * sigmoid_gate).astype(jnp.bfloat16)
    grad_gate = jnp.dot(norm_mlp.T, grad_gate_act, preferred_element_type=jnp.float32)
    grad_up = jnp.dot(norm_mlp.T, grad_up_act, preferred_element_type=jnp.float32)
    grad_norm_mlp = split_sum([(grad_gate_act, w_gate.T), (grad_up_act, w_up.T)])
    grad_gain_mlp = lax.optimization_barrier(jnp.sum(grad_norm_mlp * mid * inv_rms_mlp, axis=0))
    scaled_mlp = grad_norm_mlp * gain_mlp
    grad_mid = cotangent.astype(jnp.float32) + inv_rms_mlp * (scaled_mlp - mid * inv_rms_mlp * inv_rms_mlp * lax.optimization_barrier(jnp.mean(scaled_mlp * mid, axis=1, keepdims=True)))
    grad_mid_low = grad_mid.astype(jnp.bfloat16)
    grad_out = jnp.dot(attended_flat.T, grad_mid_low, preferred_element_type=jnp.float32)
    grad_attended = jnp.dot(grad_mid_low, w_out.T, preferred_element_type=jnp.float32).astype(jnp.bfloat16).reshape(sequence_length, HQ, HEAD_SIZE)
    grad_q, grad_key_rows, grad_value_rows = attend_back(queries, key_rows, value_rows, attended, log_totals, grad_attended)
    grad_queries_act = invert_rotary(grad_q, cosine_lookup, sine_lookup).astype(jnp.bfloat16).reshape(sequence_length, HQ * HEAD_SIZE)
    grad_keys_rotated = invert_rotary(grad_key_rows, cosine_lookup, sine_lookup).astype(jnp.bfloat16).reshape(sequence_length, KEY_VALUE_HEADS * HEAD_SIZE)
    grad_values_projected = grad_value_rows.astype(jnp.bfloat16).reshape(sequence_length, KEY_VALUE_HEADS * HEAD_SIZE)
    grad_query = jnp.dot(attention_norm.T, grad_queries_act, preferred_element_type=jnp.float32)
    grad_key = jnp.dot(attention_norm.T, grad_keys_rotated, preferred_element_type=jnp.float32)
    grad_value = jnp.dot(attention_norm.T, grad_values_projected, preferred_element_type=jnp.float32)
    grad_norm_attn = split_sum([(grad_queries_act, w_query.T), (grad_keys_rotated, key_projection_weight.T), (grad_values_projected, value_projection_weight.T)])
    grad_gain_attn = lax.optimization_barrier(jnp.sum(grad_norm_attn * xfloat * inv_rms_attn, axis=0))
    scaled_attn = grad_norm_attn * gain_attn
    input_grad = (grad_mid + inv_rms_attn * (scaled_attn - xfloat * inv_rms_attn * inv_rms_attn * lax.optimization_barrier(jnp.mean(scaled_attn * xfloat, axis=1, keepdims=True)))).astype(jnp.bfloat16)
    grads = (grad_gain_attn, grad_gain_mlp, grad_query, grad_key, grad_value, grad_out, grad_gate, grad_up, grad_down)
    return (block_output, input_grad, grads)

def reference(block_input, gain_attn, gain_mlp, w_query, key_projection_weight, value_projection_weight, w_out, w_gate, w_up, w_down, cotangent):
    inputs_seq = block_input.reshape(N_DP, SEQ, MODEL_WIDTH)
    cotangent_seq = cotangent.reshape(N_DP, SEQ, MODEL_WIDTH)
    weights = (w_query, key_projection_weight, value_projection_weight, w_out, w_gate, w_up, w_down)

    def one_sequence(totals, sequence_pair):
        block_output, input_grad, grads = layer(sequence_pair[0], gain_attn, gain_mlp, *weights, sequence_pair[1])
        return (jax.tree.map(lambda left, right: left + right, totals, grads), (block_output, input_grad))
    zero_grads = (jnp.zeros((MODEL_WIDTH,), jnp.float32), jnp.zeros((MODEL_WIDTH,), jnp.float32)) + tuple((jnp.zeros(weight.shape, jnp.float32) for weight in weights))
    totals, (outputs, input_grads) = lax.scan(one_sequence, zero_grads, (inputs_seq, cotangent_seq))
    return (outputs.reshape(TOKENS, MODEL_WIDTH), input_grads.reshape(TOKENS, MODEL_WIDTH), totals[0], totals[1], totals[2], totals[3], totals[4], totals[5], totals[6], totals[7], totals[8])
```

```python
import functools
import math

import jax
import jax.numpy as jnp
from jax import lax
from jax.experimental import pallas as pl
from jax.experimental.pallas import tpu as pltpu
from jax.sharding import PartitionSpec as P

HEAD_SIZE = 64
EPS = 1e-05
ROPE_BASE = 10000.0
NEG_LARGE = -1e30
LANES = 128
MESH = pl.DeviceIdType.MESH
F32 = jnp.float32
BF16 = jnp.bfloat16
VMEM_SPEC = pl.BlockSpec(memory_space=pltpu.VMEM)


def tables(sequence_length):
    half = HEAD_SIZE // 2
    frequency = ROPE_BASE ** (-(jnp.arange(half, dtype=F32) * 2.0) / HEAD_SIZE)
    angles = frequency[:, None] * jnp.arange(sequence_length, dtype=F32)[None, :]
    return jnp.cos(angles), jnp.sin(angles)


def dims(contract_left, contract_right):
    return (((contract_left,), (contract_right,)), ((), ()))


def mm(left, right, contract_left=1, contract_right=0):
    return lax.dot_general(
        left, right, dims(contract_left, contract_right), preferred_element_type=F32
    )


class Line:
    def __init__(self, n):
        self.n = n
        self.me = lax.axis_index("tensor")
        self.waits = []

    def barrier(self):
        barrier = pltpu.get_barrier_semaphore()
        n, me = self.n, self.me

        @pl.when(me > 0)
        def _():
            pl.semaphore_signal(barrier, inc=1, device_id={"tensor": me - 1}, device_id_type=MESH)

        @pl.when(me < n - 1)
        def _():
            pl.semaphore_signal(barrier, inc=1, device_id={"tensor": me + 1}, device_id_type=MESH)

        inner = (me > 0) & (me < n - 1)

        @pl.when(inner)
        def _():
            pl.semaphore_wait(barrier, 2)

        @pl.when(jnp.logical_not(inner))
        def _():
            pl.semaphore_wait(barrier, 1)

    def copy(self, src, dst, send, recv, step):
        return pltpu.make_async_remote_copy(
            src_ref=src,
            dst_ref=dst,
            send_sem=send,
            recv_sem=recv,
            device_id={"tensor": self.me + step},
            device_id_type=MESH,
        )


class Gather:
    def __init__(self, line, buf, send, recv, pieces):
        self.line, self.buf, self.send, self.recv, self.pieces = line, buf, send, recv, pieces
        self.size = buf.shape[1] // pieces

    def message(self, right, hop, piece, shard):
        d = 0 if right else 1
        part = self.buf.at[shard, pl.ds(piece * self.size, self.size)]
        return self.line.copy(
            part, part, self.send.at[d, hop - 1, piece], self.recv.at[d, hop - 1, piece], 1 if right else -1
        )

    def start_own(self, piece):
        line = self.line
        me, n = line.me, line.n

        @pl.when(me < n - 1)
        def _():
            self.message(True, 1, piece, me).start()

        @pl.when(me > 0)
        def _():
            self.message(False, 1, piece, me).start()

    def receive(self, hop, piece, use=None):
        line = self.line
        me, n = line.me, line.n

        @pl.when(me - hop >= 0)
        def _():
            shard = me - hop
            self.message(True, hop, piece, shard).wait_recv()
            if hop < n - 1:

                @pl.when(me < n - 1)
                def _():
                    self.message(True, hop + 1, piece, shard).start()

            if use is not None:
                use(shard, piece)

        @pl.when(me + hop <= n - 1)
        def _():
            shard = me + hop
            self.message(False, hop, piece, shard).wait_recv()
            if hop < n - 1:

                @pl.when(me > 0)
                def _():
                    self.message(False, hop + 1, piece, shard).start()

            if use is not None:
                use(shard, piece)

    def finish(self):
        line = self.line
        me, n = line.me, line.n
        for piece in range(self.pieces):
            for hop in range(1, n):

                @pl.when((me - (hop - 1) >= 0) & (me < n - 1))
                def _():
                    self.message(True, hop, piece, me - (hop - 1)).wait_send()

                @pl.when((me + (hop - 1) <= n - 1) & (me > 0))
                def _():
                    self.message(False, hop, piece, me + (hop - 1)).wait_send()


class Scatter:
    def __init__(self, line, part, buf, send, recv, pieces):
        self.line, self.part, self.buf, self.pieces = line, part, buf, pieces
        self.send, self.recv = send, recv
        self.size = part.shape[1] // pieces

    def rows(self, piece):
        return pl.ds(piece * self.size, self.size)

    def outgoing(self, d, target, piece, from_part=False):
        rows, line = self.rows(piece), self.line
        src = (self.part if from_part else self.buf).at[target, rows]
        slot = target
        if d == 1:
            slot = jnp.where(target == line.me - 1, line.n, target)
        return line.copy(
            src,
            self.buf.at[slot, rows],
            self.send.at[d, target, piece],
            self.recv.at[d, target, piece],
            1 if d == 0 else -1,
        )

    def incoming(self, d, target, slot, piece):
        part = self.buf.at[slot, self.rows(piece)]
        return self.line.copy(
            part, part, self.send.at[d, target, piece], self.recv.at[d, target, piece], 1 if d == 0 else -1
        )

    def start_ends(self, piece):
        line = self.line
        me, n = line.me, line.n

        @pl.when(me == 0)
        def _():
            for target in range(n - 1, 0, -1):
                self.outgoing(0, target, piece, True).start()

        @pl.when(me == n - 1)
        def _():
            for target in range(0, n - 1):
                self.outgoing(1, target, piece, True).start()

    def pass_on(self, d, target, piece):
        buf = self.buf
        self.incoming(d, target, target, piece).wait_recv()
        rows = self.rows(piece)
        total = buf[target, rows].astype(F32) + self.part[target, rows].astype(F32)
        buf[target, rows] = total.astype(BF16)
        self.outgoing(d, target, piece).start()

    def middle(self, piece):
        line = self.line
        me, n = line.me, line.n

        def rightward(near):
            for target in range(n - 1, 0, -1):

                @pl.when(near & (me > 0) & (me < target))
                def _():
                    self.pass_on(0, target, piece)

        def leftward(near):
            for target in range(0, n - 1):

                @pl.when(near & (me < n - 1) & (me > target))
                def _():
                    self.pass_on(1, target, piece)

        rightward(me < n // 2)
        leftward(me >= 0)
        rightward(me >= n // 2)

    def result(self, piece, store):
        line = self.line
        me, n = line.me, line.n
        rows = self.rows(piece)

        @pl.when(me > 0)
        def _():
            self.incoming(0, me, me, piece).wait_recv()

        @pl.when(me < n - 1)
        def _():
            self.incoming(1, me, n, piece).wait_recv()

        own = self.part[me, rows].astype(F32)

        @pl.when(me == 0)
        def _():
            store(own + self.buf[n, rows].astype(F32))

        @pl.when(me == n - 1)
        def _():
            store(own + self.buf[me, rows].astype(F32))

        @pl.when((me > 0) & (me < n - 1))
        def _():
            store(own + self.buf[me, rows].astype(F32) + self.buf[n, rows].astype(F32))

    def finish(self):
        line = self.line
        me, n = line.me, line.n
        for piece in range(self.pieces):
            for target in range(1, n):

                @pl.when(me < target)
                def _():
                    self.outgoing(0, target, piece).wait_send()

            for target in range(0, n - 1):

                @pl.when(me > target)
                def _():
                    self.outgoing(1, target, piece).wait_send()


def sems(n, pieces):
    return [pltpu.SemaphoreType.DMA((2, n, pieces)), pltpu.SemaphoreType.DMA((2, n, pieces))]


def comm_params(collective_id):
    return pltpu.CompilerParams(
        collective_id=collective_id, has_side_effects=True, vmem_limit_bytes=56 * 1024 * 1024
    )


def exchange_all(n, dp, send_row, recv_row, send, recv, start_only=False, wait_only=False):
    devices = n * dp
    me = lax.axis_index("dp") * n + lax.axis_index("tensor")

    def message(offset, peer, source):
        return pltpu.make_async_remote_copy(
            src_ref=send_row(peer),
            dst_ref=recv_row(source),
            send_sem=send.at[offset],
            recv_sem=recv.at[offset],
            device_id={"dp": peer // n, "tensor": peer % n},
            device_id_type=MESH,
        )

    if not wait_only:

        @pl.loop(1, devices)
        def _(offset):
            message(offset, lax.rem(me + offset, devices), me).start()

    if not start_only:

        @pl.loop(1, devices)
        def _(offset):
            copy = message(offset, lax.rem(me + offset, devices), me)
            copy.wait_send()
            copy.wait_recv()


def barrier_all(n, dp):
    devices = n * dp
    me = lax.axis_index("dp") * n + lax.axis_index("tensor")
    barrier = pltpu.get_barrier_semaphore()

    @pl.loop(1, devices)
    def _(offset):
        peer = lax.rem(me + offset, devices)
        pl.semaphore_signal(
            barrier, inc=1, device_id={"dp": peer // n, "tensor": peer % n}, device_id_type=MESH
        )

    pl.semaphore_wait(barrier, devices - 1)


def gather_kernel(n, dp, pieces, x_ref, gain_ref, seq_ref, gains_ref, send, recv, gsend, grecv):
    line = Line(n)
    me = line.me
    all_me = lax.axis_index("dp") * n + me
    barrier_all(n, dp)
    seq_ref[me] = x_ref[...]
    gains_ref[all_me] = gain_ref[...]
    gather = Gather(line, seq_ref, send, recv, pieces)
    exchange_all(
        n, dp, lambda peer: gain_ref, lambda source: gains_ref.at[source], gsend, grecv, start_only=True
    )
    for piece in range(pieces):
        gather.start_own(piece)
    for hop in range(1, n):
        for piece in range(pieces):
            gather.receive(hop, piece)
    gather.finish()
    exchange_all(
        n, dp, lambda peer: gain_ref, lambda source: gains_ref.at[source], gsend, grecv, wait_only=True
    )


def gather_rows_and_gains(n, dp, x, gains, pieces=2):
    rows, width = x.shape
    seq, all_gains = pl.pallas_call(
        functools.partial(gather_kernel, n, dp, pieces),
        out_shape=(
            jax.ShapeDtypeStruct((n, rows, width), BF16),
            jax.ShapeDtypeStruct((n * dp, 1, gains.shape[1]), F32),
        ),
        in_specs=[VMEM_SPEC] * 2,
        out_specs=(VMEM_SPEC,) * 2,
        scratch_shapes=sems(n, pieces)
        + [pltpu.SemaphoreType.DMA((n * dp,)), pltpu.SemaphoreType.DMA((n * dp,))],
        compiler_params=comm_params(1),
        name="gather_rows",
    )(x, gains)
    return seq.reshape(n * rows, width), all_gains


def tiles(extent, size):
    return [(start, min(size, extent - start)) for start in range(0, extent, size)]


def mlp_kernel(n, pieces, *refs):
    part_ref, x_ref, gain_ref, w_hbm = refs[:4]
    cot_hbm = refs[4 : 4 + n]
    npart_ref, mid_ref, inv_ref, down_ref, grad_hbm = refs[4 + n : 9 + n]
    (w, cot, seq, buf, hid, dgate, dup, stage) = refs[9 + n : 17 + n]
    ssend, srecv, gsend, grecv, local_sem, stage_sem = refs[17 + n :]
    line = Line(n)
    me = line.me
    rows_all, width = part_ref.shape[1:]
    units = hid.shape[2]
    loads = [pltpu.make_async_copy(w_hbm, w, local_sem.at[n])]
    for d in range(n):
        loads.append(
            pltpu.make_async_copy(cot_hbm[d], cot.at[lax.rem(me - d + n, n)], local_sem.at[d])
        )
    for load in loads:
        load.start()
    line.barrier()
    scatter = Scatter(line, part_ref, buf, ssend, srecv, pieces)
    gather = Gather(line, seq, gsend, grecv, pieces)
    size = scatter.size
    scatter.start_ends(0)

    def norm(piece):
        rows = scatter.rows(piece)

        def store(total):
            mid_ref[rows, :] = x_ref[rows, :].astype(F32) + total

        scatter.result(piece, store)
        mid = mid_ref[rows, :]
        inv = lax.rsqrt(jnp.mean(mid * mid, axis=1, keepdims=True) + EPS)
        inv_ref[rows, :] = jnp.broadcast_to(inv, (size, LANES))
        seq[me, rows, :] = (mid * inv * gain_ref[...]).astype(BF16)

    def flat(ref, piece):
        value = ref[:, scatter.rows(piece), :]
        return value.reshape(n * size, value.shape[2])

    def feed(piece):
        rows = scatter.rows(piece)
        tasks = []

        def unit_tile(start, count):
            def run():
                x = flat(seq, piece)
                gate = mm(x, w[:, start : start + count])
                up = mm(x, w[:, units + start : units + start + count])
                dhidden = mm(flat(cot, piece), w[:, 2 * units + start : 2 * units + start + count])
                sigmoid = jax.nn.sigmoid(gate)
                act = gate * sigmoid
                cols = slice(start, start + count)
                shape = (n, size, count)
                hid[:, rows, cols] = (act * up).astype(BF16).reshape(shape)
                dup[:, rows, cols] = (dhidden * act).astype(BF16).reshape(shape)
                dgate[:, rows, cols] = (
                    (dhidden * up * sigmoid * (1.0 + gate * (1.0 - sigmoid))).astype(BF16).reshape(shape)
                )

            return run

        def width_tile(start, count):
            def run():
                cols = slice(start, start + count)
                shape = (n, size, count)
                total = mm(flat(dgate, piece), w[cols, :units], 1, 1)
                total += mm(flat(dup, piece), w[cols, units : 2 * units], 1, 1)
                npart_ref[:, rows, cols] = total.astype(BF16).reshape(shape)
                down = mm(flat(hid, piece), w[cols, 2 * units :], 1, 1).astype(BF16).reshape(shape)
                for shard in range(n):
                    down_ref[lax.rem(shard - me + n, n), rows, cols] = down[shard]

            return run

        tasks += [unit_tile(*t) for t in tiles(units, 512)]
        tasks += [width_tile(*t) for t in tiles(width, 512)]
        return tasks

    for step in range(pieces + n - 1):
        if step < pieces:
            if step + 1 < pieces:
                scatter.start_ends(step + 1)
            scatter.middle(step)
            norm(step)
            gather.start_own(step)
        tasks = []
        ready = step - (n - 1)
        for hop in range(1, n):
            if 0 <= step - hop < pieces:
                gather.receive(hop, step - hop)
        if ready >= 0:
            if ready == 0:
                for load in loads:
                    load.wait()
            for task in feed(ready):
                task()

    scatter.finish()
    gather.finish()

    step_rows = min(256, width)
    count = width // step_rows

    def save(index, slot):
        return pltpu.make_async_copy(
            stage.at[slot],
            grad_hbm.at[pl.ds(pl.multiple_of(index * step_rows, step_rows), step_rows), :],
            stage_sem.at[slot],
        )

    @pl.loop(0, count)
    def _(index):
        slot = lax.rem(index, 2)
        cols = pl.ds(pl.multiple_of(index * step_rows, step_rows), step_rows)

        @pl.when(index >= 2)
        def _():
            save(index - 2, slot).wait()

        x = seq[:, :, cols].reshape(n * rows_all, step_rows)
        g = cot[:, :, cols].reshape(n * rows_all, step_rows)
        for at, left, right in ((0, x, dgate), (1, x, dup), (2, g, hid)):
            value = right[...].reshape(n * rows_all, units)
            stage[slot, :, at * units : (at + 1) * units] = mm(left, value, 0, 0).astype(BF16)
        save(index, slot).start()

    for index in range(max(count - 2, 0), count):
        save(index, index % 2).wait()


def mlp(n, part, x, gain, weights, cots, pieces=4):
    rows, width = x.shape
    units = weights.shape[1] // 3
    any_spec = pl.BlockSpec(memory_space=pl.ANY)
    return pl.pallas_call(
        functools.partial(mlp_kernel, n, pieces),
        out_shape=(
            jax.ShapeDtypeStruct((n, rows, width), BF16),
            jax.ShapeDtypeStruct((rows, width), F32),
            jax.ShapeDtypeStruct((rows, LANES), F32),
            jax.ShapeDtypeStruct((n, rows, width), BF16),
            jax.ShapeDtypeStruct((width, 3 * units), BF16),
        ),
        in_specs=[VMEM_SPEC] * 3 + [any_spec] * (1 + n),
        out_specs=(VMEM_SPEC,) * 4 + (any_spec,),
        scratch_shapes=[
            pltpu.VMEM((width, 3 * units), BF16),
            pltpu.VMEM((n, rows, width), BF16),
            pltpu.VMEM((n, rows, width), BF16),
            pltpu.VMEM((n + 1, rows, width), BF16),
            pltpu.VMEM((n, rows, units), BF16),
            pltpu.VMEM((n, rows, units), BF16),
            pltpu.VMEM((n, rows, units), BF16),
            pltpu.VMEM((2, min(256, width), 3 * units), BF16),
        ]
        + sems(n, pieces) * 2
        + [pltpu.SemaphoreType.DMA((n + 1,)), pltpu.SemaphoreType.DMA((2,))],
        compiler_params=pltpu.CompilerParams(
            collective_id=2, has_side_effects=True, vmem_limit_bytes=67043328
        ),
        cost_estimate=pl.CostEstimate(
            flops=18 * n * rows * width * units, bytes_accessed=400 * 1024 * 1024, transcendentals=0
        ),
        name="mlp",
    )(part.reshape(n, rows, width), x, gain, weights, *cots)


def back_kernel(
    n, pieces, part_ref, mid_ref, inv_ref, gain_ref, cot_ref, seq_ref, grad_ref, dgain_ref,
    buf, ssend, srecv, gsend, grecv,
):
    line = Line(n)
    me = line.me
    line.barrier()
    scatter = Scatter(line, part_ref, buf, ssend, srecv, pieces)
    gather = Gather(line, seq_ref, gsend, grecv, pieces)
    scatter.start_ends(0)
    dgain_ref[...] = jnp.zeros_like(dgain_ref)

    def back(piece):
        rows = scatter.rows(piece)

        def store(total):
            grad_ref[rows, :] = total

        scatter.result(piece, store)
        grad = grad_ref[rows, :]
        mid = mid_ref[rows, :]
        inv = inv_ref[rows, 0:1]
        dgain_ref[...] += jnp.sum(grad * mid * inv, axis=0, keepdims=True)
        scaled = grad * gain_ref[...]
        mean = jnp.mean(scaled * mid, axis=1, keepdims=True)
        out = cot_ref[rows, :].astype(F32) + inv * (scaled - mid * (inv * inv * mean))
        grad_ref[rows, :] = out
        seq_ref[me, rows, :] = out.astype(BF16)

    for piece in range(pieces):
        if piece + 1 < pieces:
            scatter.start_ends(piece + 1)
        scatter.middle(piece)
        back(piece)
        gather.start_own(piece)
        for hop in range(1, n):
            if piece - hop >= 0:
                gather.receive(hop, piece - hop)
    for late in range(1, n):
        for hop in range(late, n):
            piece = pieces - 1 - (hop - late)
            if piece >= 0:
                gather.receive(hop, piece)
    scatter.finish()
    gather.finish()


def sum_back_gather(n, part, mid, inv, gain, cotangent, pieces=4):
    rows, width = cotangent.shape
    return pl.pallas_call(
        functools.partial(back_kernel, n, pieces),
        out_shape=(
            jax.ShapeDtypeStruct((n, rows, width), BF16),
            jax.ShapeDtypeStruct((rows, width), F32),
            jax.ShapeDtypeStruct((1, width), F32),
        ),
        in_specs=[VMEM_SPEC] * 5,
        out_specs=(VMEM_SPEC,) * 3,
        scratch_shapes=[pltpu.VMEM((n + 1, rows, width), BF16)] + sems(n, pieces) * 2,
        compiler_params=comm_params(3),
        cost_estimate=pl.CostEstimate(flops=0, bytes_accessed=350 * 1024 * 1024, transcendentals=0),
        name="sum_back_gather",
    )(part.reshape(n, rows, width), mid, inv, gain, cotangent)


def last_kernel(
    n, pieces, part_ref, x_ref, gain_ref, grad_mid_ref, out_ref, dgain_ref, total_ref,
    buf, ssend, srecv,
):
    line = Line(n)
    line.barrier()
    scatter = Scatter(line, part_ref, buf, ssend, srecv, pieces)
    for piece in range(pieces):
        scatter.start_ends(piece)
    dgain_ref[...] = jnp.zeros_like(dgain_ref)
    for piece in range(pieces):
        scatter.middle(piece)
        rows = scatter.rows(piece)

        def store(total):
            total_ref[...] = total

        scatter.result(piece, store)
        grad = total_ref[...]
        x = x_ref[rows, :].astype(F32)
        inv = lax.rsqrt(jnp.mean(x * x, axis=1, keepdims=True) + EPS)
        dgain_ref[...] += jnp.sum(grad * x * inv, axis=0, keepdims=True)
        scaled = grad * gain_ref[...]
        mean = jnp.mean(scaled * x, axis=1, keepdims=True)
        out = grad_mid_ref[rows, :] + inv * (scaled - x * (inv * inv * mean))
        out_ref[rows, :] = out.astype(BF16)
    scatter.finish()


def sum_input_grad(n, part, x, gain, grad_mid, pieces=4):
    rows, width = x.shape
    return pl.pallas_call(
        functools.partial(last_kernel, n, pieces),
        out_shape=(
            jax.ShapeDtypeStruct((rows, width), BF16),
            jax.ShapeDtypeStruct((1, width), F32),
        ),
        in_specs=[VMEM_SPEC] * 4,
        out_specs=(VMEM_SPEC,) * 2,
        scratch_shapes=[pltpu.VMEM((rows // pieces, width), F32)]
        + [pltpu.VMEM((n + 1, rows, width), BF16)]
        + sems(n, pieces),
        compiler_params=comm_params(4),
        cost_estimate=pl.CostEstimate(flops=0, bytes_accessed=250 * 1024 * 1024, transcendentals=0),
        name="sum_input_grad",
    )(part.reshape(n, rows, width), x, gain, grad_mid)


def gains_kernel(n, dp, part_ref, out_ref, held, send, recv):
    me = lax.axis_index("dp") * n + lax.axis_index("tensor")
    barrier_all(n, dp)
    held[me] = part_ref[me]
    exchange_all(n, dp, lambda peer: part_ref.at[peer], lambda source: held.at[source], send, recv)
    out_ref[...] = jnp.sum(held[...], axis=0)


def sum_gains(n, dp, part):
    return pl.pallas_call(
        functools.partial(gains_kernel, n, dp),
        out_shape=jax.ShapeDtypeStruct((1, part.shape[2]), F32),
        in_specs=[VMEM_SPEC],
        out_specs=VMEM_SPEC,
        scratch_shapes=[
            pltpu.VMEM(part.shape, F32),
            pltpu.SemaphoreType.DMA((n * dp,)),
            pltpu.SemaphoreType.DMA((n * dp,)),
        ],
        compiler_params=comm_params(5),
        name="sum_gains",
    )(part)


def rotate(half_a, half_b, cos, sin):
    return half_a * cos - half_b * sin, half_b * cos + half_a * sin


def unrotate(half_a, half_b, cos, sin):
    return half_a * cos + half_b * sin, half_b * cos - half_a * sin


def mask_block(size, scores):
    key = lax.broadcasted_iota(jnp.int32, (size, size), 0)
    row = lax.broadcasted_iota(jnp.int32, (size, size), 1)
    return jnp.where(key <= row, scores, NEG_LARGE)


def attend_kernel(heads, block, act_ref, cos_ref, sin_ref, qkv_ref, kv_ref, out_ref, log_ref):
    half = HEAD_SIZE // 2
    cos, sin = cos_ref[...], sin_ref[...]

    @pl.loop(0, heads + 1)
    def _(h):
        base = pl.multiple_of(h * HEAD_SIZE, HEAD_SIZE)
        a, b = rotate(act_ref[pl.ds(base, half), :], act_ref[pl.ds(base + half, half), :], cos, sin)
        qkv_ref[pl.ds(base, half), :] = a.astype(BF16)
        qkv_ref[pl.ds(base + half, half), :] = b.astype(BF16)

    values = pl.ds((heads + 1) * HEAD_SIZE, HEAD_SIZE)
    qkv_ref[values, :] = act_ref[values, :].astype(BF16)
    length = qkv_ref.shape[1]
    scale = 1.0 / math.sqrt(HEAD_SIZE)
    kv_ref[...] = qkv_ref[pl.ds(heads * HEAD_SIZE, 2 * HEAD_SIZE), :].T

    @pl.loop(0, heads)
    def _(h):
        base = pl.multiple_of(h * HEAD_SIZE, HEAD_SIZE)
        for i in range(length // block):
            cols = pl.ds(i * block, block)
            query = qkv_ref[pl.ds(base, HEAD_SIZE), cols]
            scores = []
            peak = None
            for j in range(i + 1):
                s = mm(kv_ref[pl.ds(j * block, block), :HEAD_SIZE], query) * scale
                if i == j:
                    s = mask_block(block, s)
                top = jnp.max(s, axis=0, keepdims=True)
                peak = top if peak is None else jnp.maximum(peak, top)
                scores.append(s)
            weights = [jnp.exp(s - peak) for s in scores]
            total = sum(jnp.sum(w, axis=0, keepdims=True) for w in weights)
            log_ref[pl.ds(h, 1), cols] = peak + jnp.log(total)
            inverse = 1.0 / total
            mixed = None
            for j in range(i + 1):
                w = (weights[j] * inverse).astype(BF16)
                v = qkv_ref[values, pl.ds(j * block, block)]
                term = mm(v, w)
                mixed = term if mixed is None else mixed + term
            out_ref[pl.ds(base, HEAD_SIZE), cols] = mixed.astype(BF16)


def attend(act, cos, sin, block=256):
    width, length = act.shape
    heads = width // HEAD_SIZE - 2
    return pl.pallas_call(
        functools.partial(attend_kernel, heads, block),
        out_shape=(
            jax.ShapeDtypeStruct((width, length), BF16),
            jax.ShapeDtypeStruct((length, 2 * HEAD_SIZE), BF16),
            jax.ShapeDtypeStruct((heads * HEAD_SIZE, length), BF16),
            jax.ShapeDtypeStruct((heads, length), F32),
        ),
        in_specs=[VMEM_SPEC] * 3,
        out_specs=(VMEM_SPEC,) * 4,
        compiler_params=pltpu.CompilerParams(vmem_limit_bytes=56 * 1024 * 1024),
        cost_estimate=pl.CostEstimate(
            flops=4 * heads * HEAD_SIZE * length * length,
            bytes_accessed=12 * width * length,
            transcendentals=heads * length * length,
        ),
        name="attend",
    )(act, cos, sin)


def attend_back_kernel(
    heads, block, qkv_ref, kv_ref, out_ref, log_ref, grad_ref, cos_ref, sin_ref, dqkv_ref, dkv
):
    half = HEAD_SIZE // 2
    length = qkv_ref.shape[1]
    scale = 1.0 / math.sqrt(HEAD_SIZE)
    dkv[...] = jnp.zeros_like(dkv)
    keys = pl.ds(heads * HEAD_SIZE, HEAD_SIZE)

    @pl.loop(0, heads)
    def _(h):
        base = pl.multiple_of(h * HEAD_SIZE, HEAD_SIZE)
        mine = pl.ds(base, HEAD_SIZE)
        for i in range(length // block):
            cols = pl.ds(i * block, block)
            query = qkv_ref[mine, cols]
            grad = grad_ref[mine, cols]
            delta = jnp.sum(
                grad.astype(F32) * out_ref[mine, cols].astype(F32), axis=0, keepdims=True
            )
            log_total = log_ref[pl.ds(h, 1), cols]
            dquery = None
            for j in range(i + 1):
                rows = pl.ds(j * block, block)
                s = mm(kv_ref[rows, :HEAD_SIZE], query) * scale
                if i == j:
                    s = mask_block(block, s)
                probs = jnp.exp(s - log_total)
                dprobs = mm(kv_ref[rows, HEAD_SIZE:], grad)
                dscores = (probs * (dprobs - delta) * scale).astype(BF16)
                dkv[0, rows, :] += mm(dscores, query, 1, 1)
                dkv[1, rows, :] += mm(probs.astype(BF16), grad, 1, 1)
                term = mm(qkv_ref[keys, rows], dscores)
                dquery = term if dquery is None else dquery + term
            cos, sin = cos_ref[:, cols], sin_ref[:, cols]
            a, b = unrotate(dquery[:half], dquery[half:], cos, sin)
            dqkv_ref[pl.ds(base, half), cols] = a.astype(BF16)
            dqkv_ref[pl.ds(base + half, half), cols] = b.astype(BF16)

    dkeys = dkv[0].T
    a, b = unrotate(dkeys[:half], dkeys[half:], cos_ref[...], sin_ref[...])
    dqkv_ref[pl.ds(heads * HEAD_SIZE, half), :] = a.astype(BF16)
    dqkv_ref[pl.ds(heads * HEAD_SIZE + half, half), :] = b.astype(BF16)
    dqkv_ref[pl.ds((heads + 1) * HEAD_SIZE, HEAD_SIZE), :] = dkv[1].T.astype(BF16)


def attend_back(qkv, kv, out, log_total, grad, cos, sin, block=256):
    width, length = qkv.shape
    heads = width // HEAD_SIZE - 2
    return pl.pallas_call(
        functools.partial(attend_back_kernel, heads, block),
        out_shape=jax.ShapeDtypeStruct((width, length), BF16),
        in_specs=[VMEM_SPEC] * 7,
        out_specs=VMEM_SPEC,
        scratch_shapes=[pltpu.VMEM((2, length, HEAD_SIZE), F32)],
        compiler_params=pltpu.CompilerParams(vmem_limit_bytes=56 * 1024 * 1024),
        cost_estimate=pl.CostEstimate(
            flops=10 * heads * HEAD_SIZE * length * length,
            bytes_accessed=12 * width * length,
            transcendentals=heads * length * length,
        ),
        name="attend_back",
    )(qkv, kv, out, log_total, grad, cos, sin)


def local(
    n, dp, x, gain_attn, gain_mlp, w_query, w_key, w_value, w_out, w_gate, w_up, w_down, cotangent
):
    rows, width = x.shape
    length = n * rows
    per = gain_attn.shape[0]
    q_cols, k_cols = w_query.shape[1], w_key.shape[1]

    attn_cols = q_cols + 2 * k_cols
    attn_all = lax.all_gather(
        jnp.concatenate([w_query, w_key, w_value, w_out.T], axis=1), "dp", axis=0, tiled=True
    )
    w_qkv, w_out_t = attn_all[:, :attn_cols], attn_all[:, attn_cols:]
    mlp_all = lax.all_gather(
        jnp.concatenate([w_gate, w_up, w_down.T], axis=1), "dp", axis=0, tiled=True
    )
    units = w_gate.shape[1]

    packed = 2 * per + (-2 * per) % LANES
    gains = jnp.zeros((1, packed), F32)
    gains = gains.at[0, :per].set(gain_attn).at[0, per : 2 * per].set(gain_mlp)
    x_seq, all_gains = gather_rows_and_gains(n, dp, x, gains)
    full_attn = all_gains[:, 0, :per].reshape(1, width)
    full_mlp = all_gains[:, 0, per : 2 * per].reshape(1, width)

    def shift(value, distance):
        pairs = [(i, (i + distance) % n) for i in range(n)]
        return lax.ppermute(value, "tensor", pairs)

    cot_own, x_seq = lax.optimization_barrier((cotangent, x_seq))
    cots = [cot_own] + [shift(cot_own, d) for d in range(1, n)]

    x_float = x_seq.astype(F32)
    inv_attn = lax.rsqrt(jnp.mean(x_float * x_float, axis=1, keepdims=True) + EPS)
    norm_attn = (x_float * inv_attn * full_attn).astype(BF16)
    cos, sin = tables(length)
    act = mm(w_qkv, norm_attn, 0, 1)
    qkv, kv, attended, log_total = attend(act, cos, sin)
    out_part = mm(attended, w_out_t, 0, 1).astype(BF16)
    norm_part, mid, inv_mlp, down_parts, mlp_grad = mlp(n, out_part, x, full_mlp, mlp_all, cots)
    mlp_grad = lax.psum_scatter(mlp_grad, "dp", scatter_dimension=0, tiled=True)

    grad_mid_seq, grad_mid, dgain_mlp = sum_back_gather(n, norm_part, mid, inv_mlp, full_mlp, cotangent)
    down_parts, grad_mid_seq = lax.optimization_barrier((down_parts, grad_mid_seq))
    block_output = mid + down_parts[0].astype(F32)
    for d in range(1, n):
        block_output += shift(down_parts[d], d).astype(F32)
    block_output = block_output.astype(BF16)

    grad_mid_seq = grad_mid_seq.reshape(length, width)
    grad_out_t = mm(grad_mid_seq, attended, 0, 1).astype(BF16)
    dattended = mm(w_out_t, grad_mid_seq, 0, 1).astype(BF16)
    dqkv = attend_back(qkv, kv, attended, log_total, dattended, cos, sin)
    attn_part = mm(dqkv, w_qkv, 0, 1).astype(BF16)
    grad_qkv = mm(norm_attn, dqkv, 0, 1).astype(BF16)
    attn_grad = lax.psum_scatter(
        jnp.concatenate([grad_qkv, grad_out_t], axis=1), "dp", scatter_dimension=0, tiled=True
    ).astype(F32)
    input_grad, dgain_attn = sum_input_grad(n, attn_part, x, full_attn, grad_mid)
    mlp_grad = mlp_grad.astype(F32)

    dgains = jnp.concatenate(
        [dgain_attn.reshape(-1, per), dgain_mlp.reshape(-1, per)]
        + ([jnp.zeros((n * dp, packed - 2 * per), F32)] if packed > 2 * per else []),
        axis=1,
    )
    dgains = sum_gains(n, dp, dgains.reshape(n * dp, 1, packed))

    return (
        block_output,
        input_grad,
        dgains[0, :per],
        dgains[0, per : 2 * per],
        attn_grad[:, :q_cols],
        attn_grad[:, q_cols : q_cols + k_cols],
        attn_grad[:, q_cols + k_cols : attn_cols],
        attn_grad[:, attn_cols:].T,
        mlp_grad[:, :units],
        mlp_grad[:, units : 2 * units],
        mlp_grad[:, 2 * units :].T,
    )


def solution(mesh):
    rows = P(("dp", "tensor"), None)
    gain = P(("dp", "tensor"))
    into = P("dp", "tensor")
    back = P("tensor", "dp")
    in_specs = (rows, gain, gain, into, into, into, back, into, into, back, rows)
    out_specs = (rows, rows, gain, gain, into, into, into, back, into, into, back)
    body = functools.partial(local, mesh.shape["tensor"], mesh.shape["dp"])
    return jax.shard_map(body, mesh=mesh, in_specs=in_specs, out_specs=out_specs, check_vma=False)
```

```python
import functools
import math

import jax
import jax.numpy as jnp
from jax import lax
from jax.experimental import pallas as pl
from jax.experimental.pallas import tpu as pltpu
from jax.sharding import PartitionSpec as P


HEAD_SIZE = 64
EPS = 1e-05
ROPE_BASE = 10000.0
NEG_LARGE = -1e30
LANES = 128
MESH = pl.DeviceIdType.MESH
F32 = jnp.float32
BF16 = jnp.bfloat16
VMEM_SPEC = pl.BlockSpec(memory_space=pltpu.VMEM)


def tables(sequence_length):
    half = HEAD_SIZE // 2
    frequency = ROPE_BASE ** (-(jnp.arange(half, dtype=F32) * 2.0) / HEAD_SIZE)
    angles = frequency[:, None] * jnp.arange(sequence_length, dtype=F32)[None, :]
    return jnp.cos(angles), jnp.sin(angles)


def dims(contract_left, contract_right):
    return (((contract_left,), (contract_right,)), ((), ()))


def mm(left, right, contract_left=1, contract_right=0):
    return lax.dot_general(
        left, right, dims(contract_left, contract_right), preferred_element_type=F32
    )


def piece_rows(piece, size):
    return pl.ds(pl.multiple_of(piece * size, size), size)


class Line:
    def __init__(self, n):
        self.n = n
        self.me = lax.axis_index("tensor")

    def barrier(self):
        barrier = pltpu.get_barrier_semaphore()
        n, me = self.n, self.me

        @pl.when(me > 0)
        def _():
            pl.semaphore_signal(barrier, inc=1, device_id={"tensor": me - 1}, device_id_type=MESH)

        @pl.when(me < n - 1)
        def _():
            pl.semaphore_signal(barrier, inc=1, device_id={"tensor": me + 1}, device_id_type=MESH)

        inner = (me > 0) & (me < n - 1)

        @pl.when(inner)
        def _():
            pl.semaphore_wait(barrier, 2)

        @pl.when(jnp.logical_not(inner))
        def _():
            pl.semaphore_wait(barrier, 1)

    def copy(self, src, dst, send, recv, step):
        return pltpu.make_async_remote_copy(
            src_ref=src,
            dst_ref=dst,
            send_sem=send,
            recv_sem=recv,
            device_id={"tensor": self.me + step},
            device_id_type=MESH,
        )


class Gather:
    def __init__(self, line, buf, send, recv, pieces):
        self.line, self.buf, self.send, self.recv, self.pieces = line, buf, send, recv, pieces
        self.size = buf.shape[1] // pieces

    def message(self, right, hop, piece, shard):
        d = 0 if right else 1
        part = self.buf.at[shard, piece_rows(piece, self.size)]
        return self.line.copy(
            part, part, self.send.at[d, hop - 1, piece], self.recv.at[d, hop - 1, piece], 1 if right else -1
        )

    def start_own(self, piece):
        line = self.line
        me, n = line.me, line.n

        @pl.when(me < n - 1)
        def _():
            self.message(True, 1, piece, me).start()

        @pl.when(me > 0)
        def _():
            self.message(False, 1, piece, me).start()

    def start_hop(self, hop, piece):
        line = self.line
        me, n = line.me, line.n

        @pl.when((me - (hop - 1) >= 0) & (me < n - 1))
        def _():
            self.message(True, hop, piece, me - (hop - 1)).start()

        @pl.when((me + (hop - 1) <= n - 1) & (me > 0))
        def _():
            self.message(False, hop, piece, me + (hop - 1)).start()

    def receive(self, hop, piece, use=None):
        line = self.line
        me, n = line.me, line.n

        @pl.when(me - hop >= 0)
        def _():
            shard = me - hop
            self.message(True, hop, piece, shard).wait_recv()
            if hop < n - 1:

                @pl.when(me < n - 1)
                def _():
                    self.message(True, hop + 1, piece, shard).start()

            if use is not None:
                use(shard, piece)

        @pl.when(me + hop <= n - 1)
        def _():
            shard = me + hop
            self.message(False, hop, piece, shard).wait_recv()
            if hop < n - 1:

                @pl.when(me > 0)
                def _():
                    self.message(False, hop + 1, piece, shard).start()

            if use is not None:
                use(shard, piece)

    def finish(self, first_hop=1):
        line = self.line
        me, n = line.me, line.n

        @pl.loop(0, self.pieces)
        def _(piece):
            for hop in range(first_hop, n):

                @pl.when((me - (hop - 1) >= 0) & (me < n - 1))
                def _():
                    self.message(True, hop, piece, me - (hop - 1)).wait_send()

                @pl.when((me + (hop - 1) <= n - 1) & (me > 0))
                def _():
                    self.message(False, hop, piece, me + (hop - 1)).wait_send()


class Scatter:
    def __init__(self, line, part, buf, send, recv, pieces):
        self.line, self.part, self.buf, self.pieces = line, part, buf, pieces
        self.send, self.recv = send, recv
        self.size = part.shape[1] // pieces

    def rows(self, piece):
        return piece_rows(piece, self.size)

    def outgoing(self, d, target, piece, from_part=False):
        rows, line = self.rows(piece), self.line
        src = (self.part if from_part else self.buf).at[target, rows]
        slot = target
        if d == 1:
            slot = jnp.where(target == line.me - 1, line.n, target)
        return line.copy(
            src,
            self.buf.at[slot, rows],
            self.send.at[d, target, piece],
            self.recv.at[d, target, piece],
            1 if d == 0 else -1,
        )

    def incoming(self, d, target, slot, piece):
        part = self.buf.at[slot, self.rows(piece)]
        return self.line.copy(
            part, part, self.send.at[d, target, piece], self.recv.at[d, target, piece], 1 if d == 0 else -1
        )

    def start_ends(self, piece):
        line = self.line
        me, n = line.me, line.n

        @pl.when(me == 0)
        def _():
            for target in range(n - 1, 0, -1):
                self.outgoing(0, target, piece, True).start()

        @pl.when(me == n - 1)
        def _():
            for target in range(0, n - 1):
                self.outgoing(1, target, piece, True).start()

    def pass_on(self, d, target, piece):
        buf = self.buf
        self.incoming(d, target, target, piece).wait_recv()
        rows = self.rows(piece)
        total = buf[target, rows].astype(F32) + self.part[target, rows].astype(F32)
        buf[target, rows] = total.astype(BF16)
        self.outgoing(d, target, piece).start()

    def passes(self, piece, right, targets, where):
        line = self.line
        me, n = line.me, line.n
        for target in targets:
            held = (me > 0) & (me < target) if right else (me < n - 1) & (me > target)

            @pl.when(where & held)
            def _():
                self.pass_on(0 if right else 1, target, piece)

    def first(self, piece):
        n, left_half = self.line.n, self.line.me < self.line.n // 2
        self.passes(piece, True, (n - 1,), left_half)
        self.passes(piece, False, (0,), jnp.logical_not(left_half))

    def rest(self, piece):
        n, left_half = self.line.n, self.line.me < self.line.n // 2
        right_half = jnp.logical_not(left_half)
        self.passes(piece, True, range(n - 2, 0, -1), left_half)
        self.passes(piece, False, range(1, n - 1), right_half)
        self.passes(piece, False, range(0, n - 1), left_half)
        self.passes(piece, True, range(n - 1, 0, -1), right_half)

    def middle(self, piece):
        self.first(piece)
        self.rest(piece)

    def result(self, piece, store):
        line = self.line
        me, n = line.me, line.n
        rows = self.rows(piece)

        @pl.when(me > 0)
        def _():
            self.incoming(0, me, me, piece).wait_recv()

        @pl.when(me < n - 1)
        def _():
            self.incoming(1, me, n, piece).wait_recv()

        own = self.part[me, rows].astype(F32)

        @pl.when(me == 0)
        def _():
            store(own + self.buf[n, rows].astype(F32))

        @pl.when(me == n - 1)
        def _():
            store(own + self.buf[me, rows].astype(F32))

        @pl.when((me > 0) & (me < n - 1))
        def _():
            store(own + self.buf[me, rows].astype(F32) + self.buf[n, rows].astype(F32))

    def finish(self):
        line = self.line
        me, n = line.me, line.n

        @pl.loop(0, self.pieces)
        def _(piece):
            for target in range(1, n):

                @pl.when(me < target)
                def _():
                    self.outgoing(0, target, piece).wait_send()

            for target in range(0, n - 1):

                @pl.when(me > target)
                def _():
                    self.outgoing(1, target, piece).wait_send()


def within(piece, pieces):
    return (piece >= 0) & (piece < pieces)


def sems(n, pieces):
    return [pltpu.SemaphoreType.DMA((2, n, pieces)), pltpu.SemaphoreType.DMA((2, n, pieces))]


def comm_params(collective_id):
    return pltpu.CompilerParams(
        collective_id=collective_id, has_side_effects=True, vmem_limit_bytes=56 * 1024 * 1024
    )


def exchange_all(n, dp, send_row, recv_row, send, recv, start_only=False, wait_only=False):
    devices = n * dp
    me = lax.axis_index("dp") * n + lax.axis_index("tensor")

    def message(offset, peer, source):
        return pltpu.make_async_remote_copy(
            src_ref=send_row(peer),
            dst_ref=recv_row(source),
            send_sem=send.at[offset],
            recv_sem=recv.at[offset],
            device_id={"dp": peer // n, "tensor": peer % n},
            device_id_type=MESH,
        )

    if not wait_only:

        @pl.loop(1, devices)
        def _(offset):
            message(offset, lax.rem(me + offset, devices), me).start()

    if not start_only:

        @pl.loop(1, devices)
        def _(offset):
            copy = message(offset, lax.rem(me + offset, devices), me)
            copy.wait_send()
            copy.wait_recv()


def barrier_all(n, dp):
    devices = n * dp
    me = lax.axis_index("dp") * n + lax.axis_index("tensor")
    barrier = pltpu.get_barrier_semaphore()

    @pl.loop(1, devices)
    def _(offset):
        peer = lax.rem(me + offset, devices)
        pl.semaphore_signal(
            barrier, inc=1, device_id={"dp": peer // n, "tensor": peer % n}, device_id_type=MESH
        )

    pl.semaphore_wait(barrier, devices - 1)


def tiles(extent, size):
    return [(start, min(size, extent - start)) for start in range(0, extent, size)]


def mlp_kernel(
    n, pieces, part_ref, x_ref, gain_ref, w_hbm, cot_hbm, near_hbm,
    mid_ref, grad_ref, low_ref, dgain_ref, hid_hbm, wgrad_hbm,
    w, cot, seq, buf, npart, buf_back, hid, dgate, dup, stage, inv_ref,
    ssend, srecv, gsend, grecv, bsend, brecv, csend, crecv, local_sem, stage_sem,
):
    line = Line(n)
    me = line.me
    rows_all, width = part_ref.shape[1:]
    units = hid.shape[2]
    weight_load = pltpu.make_async_copy(w_hbm, w, local_sem.at[0])
    own_load = pltpu.make_async_copy(cot_hbm, cot.at[me], local_sem.at[1])
    inner = (me > 0) & (me < n - 1)

    def near_load(shard):
        return pltpu.make_async_copy(near_hbm.at[shard], cot.at[shard], local_sem.at[5 + shard])

    def each_near(act):
        for shard in range(n):
            here = (me != shard) & (inner | (me - shard == 1) | (shard - me == 1))

            @pl.when(here)
            def _():
                act(near_load(shard))

    each_near(lambda copy: copy.start())
    own_load.start()
    weight_load.start()
    line.barrier()
    scatter = Scatter(line, part_ref, buf, ssend, srecv, pieces)
    gather = Gather(line, seq, gsend, grecv, pieces)
    scatter_back = Scatter(line, npart, buf_back, bsend, brecv, pieces)
    cot_gather = Gather(line, cot, csend, crecv, pieces)
    size = scatter.size
    scatter.start_ends(0)
    dgain_ref[...] = jnp.zeros_like(dgain_ref)

    each_near(lambda copy: copy.wait())

    def each_far(act):
        for hop in range(2, n):

            @pl.when(me == n - 2)
            def _():
                act(True, hop, me - (hop - 1))

            @pl.when(me == 1)
            def _():
                act(False, hop, me + (hop - 1))

    def far_start(piece):
        each_far(lambda right, hop, shard: cot_gather.message(right, hop, piece, shard).start())

    def far_sent(piece):
        each_far(lambda right, hop, shard: cot_gather.message(right, hop, piece, shard).wait_send())

    def far_arrived(piece):
        for hop in range(2, n):

            @pl.when(me == n - 1)
            def _():
                cot_gather.message(True, hop, piece, me - hop).wait_recv()

            @pl.when(me == 0)
            def _():
                cot_gather.message(False, hop, piece, me + hop).wait_recv()

    def norm(piece):
        rows = scatter.rows(piece)

        def store(total):
            mid_ref[rows, :] = x_ref[rows, :].astype(F32) + total

        scatter.result(piece, store)
        mid = mid_ref[rows, :]
        inv = lax.rsqrt(jnp.mean(mid * mid, axis=1, keepdims=True) + EPS)
        inv_ref[rows, :] = jnp.broadcast_to(inv, (size, LANES))
        seq[me, rows, :] = (mid * inv * gain_ref[...]).astype(BF16)

    def back(piece):
        rows = scatter.rows(piece)

        def store(total):
            grad_ref[rows, :] = total

        scatter_back.result(piece, store)
        grad = grad_ref[rows, :]
        mid = mid_ref[rows, :]
        inv = inv_ref[rows, 0:1]
        dgain_ref[...] += jnp.sum(grad * mid * inv, axis=0, keepdims=True)
        scaled = grad * gain_ref[...]
        mean = jnp.mean(scaled * mid, axis=1, keepdims=True)
        out = cot[me, rows, :].astype(F32) + inv * (scaled - mid * (inv * inv * mean))
        grad_ref[rows, :] = out
        low_ref[rows, :] = out.astype(BF16)

    def flat(ref, piece):
        value = ref[:, scatter.rows(piece), :]
        return value.reshape(n * size, value.shape[2])

    def feed(piece):
        rows = scatter.rows(piece)
        for start, count in tiles(units, 512):
            x = flat(seq, piece)
            gate = mm(x, w[:, start : start + count])
            up = mm(x, w[:, units + start : units + start + count])
            dhidden = mm(flat(cot, piece), w[:, 2 * units + start : 2 * units + start + count])
            sigmoid = jax.nn.sigmoid(gate)
            act = gate * sigmoid
            cols = slice(start, start + count)
            shape = (n, size, count)
            hid[:, rows, cols] = (act * up).astype(BF16).reshape(shape)
            dup[:, rows, cols] = (dhidden * act).astype(BF16).reshape(shape)
            dgate[:, rows, cols] = (
                (dhidden * up * sigmoid * (1.0 + gate * (1.0 - sigmoid))).astype(BF16).reshape(shape)
            )
        for start, count in tiles(width, 512):
            cols = slice(start, start + count)
            total = mm(flat(dgate, piece), w[cols, :units], 1, 1)
            total += mm(flat(dup, piece), w[cols, units : 2 * units], 1, 1)
            npart[:, rows, cols] = total.astype(BF16).reshape(n, size, count)

    step_rows = min(LANES, width)
    count = width // step_rows

    def save(index, slot):
        return pltpu.make_async_copy(
            stage.at[slot],
            wgrad_hbm.at[pl.ds(pl.multiple_of(index * step_rows, step_rows), step_rows), :],
            stage_sem.at[slot],
        )

    def weight_grads(events):
        @pl.loop(0, count)
        def _(index):
            for at, event in events:

                @pl.when(index == at)
                def _():
                    event()

            slot = lax.rem(index, 2)
            cols = pl.ds(pl.multiple_of(index * step_rows, step_rows), step_rows)

            @pl.when(index >= 2)
            def _():
                save(index - 2, slot).wait()

            x = seq[:, :, cols].reshape(n * rows_all, step_rows)
            g = cot[:, :, cols].reshape(n * rows_all, step_rows)
            for at, left, right in ((0, x, dgate), (1, x, dup), (2, g, hid)):
                value = right[...].reshape(n * rows_all, units)
                stage[slot, :, at * units : (at + 1) * units] = mm(left, value, 0, 0).astype(BF16)
            save(index, slot).start()

    hid_save = pltpu.make_async_copy(hid, hid_hbm, local_sem.at[2])

    @pl.loop(0, pieces + n - 1)
    def _(step):
        first = step < pieces

        @pl.when(first)
        def _():
            @pl.when(step + 1 < pieces)
            def _():
                scatter.start_ends(step + 1)

            scatter.middle(step)
            far_start(step)

        for hop in range(1, n):
            piece = step - hop

            @pl.when(within(piece, pieces))
            def _():
                gather.receive(hop, piece)

        @pl.when(first)
        def _():
            norm(step)
            gather.start_own(step)

        ready = step - (n - 1)

        @pl.when(ready == 0)
        def _():
            own_load.wait()
            weight_load.wait()

        @pl.when(ready >= 1)
        def _():
            scatter_back.middle(ready - 1)

        @pl.when(ready >= 0)
        def _():
            far_arrived(ready)
            feed(ready)
            scatter_back.start_ends(ready)

        @pl.when(ready >= 1)
        def _():
            back(ready - 1)

    hid_save.start()
    last = pieces - 1
    weight_grads(
        (
            (count * 3 // 8, lambda: scatter_back.first(last)),
            (count * 3 // 4, lambda: scatter_back.rest(last)),
        )
    )
    back(last)
    scatter.finish()
    gather.finish()
    scatter_back.finish()

    @pl.loop(0, pieces)
    def _(piece):
        far_sent(piece)

    hid_save.wait()
    for index in range(max(count - 2, 0), count):
        save(index, index % 2).wait()


def mlp(n, part, x, gain, weights, cotangent, near, pieces=4):
    rows, width = x.shape
    units = weights.shape[1] // 3
    any_spec = pl.BlockSpec(memory_space=pl.ANY)
    return pl.pallas_call(
        functools.partial(mlp_kernel, n, pieces),
        out_shape=(
            jax.ShapeDtypeStruct((rows, width), F32),
            jax.ShapeDtypeStruct((rows, width), F32),
            jax.ShapeDtypeStruct((rows, width), BF16),
            jax.ShapeDtypeStruct((1, width), F32),
            jax.ShapeDtypeStruct((n, rows, units), BF16),
            jax.ShapeDtypeStruct((width, 3 * units), BF16),
        ),
        in_specs=[VMEM_SPEC] * 3 + [any_spec] * 3,
        out_specs=(VMEM_SPEC,) * 4 + (any_spec,) * 2,
        scratch_shapes=[
            pltpu.VMEM((width, 3 * units), BF16),
            pltpu.VMEM((n, rows, width), BF16),
            pltpu.VMEM((n, rows, width), BF16),
            pltpu.VMEM((n + 1, rows, width), BF16),
            pltpu.VMEM((n, rows, width), BF16),
            pltpu.VMEM((n + 1, rows, width), BF16),
            pltpu.VMEM((n, rows, units), BF16),
            pltpu.VMEM((n, rows, units), BF16),
            pltpu.VMEM((n, rows, units), BF16),
            pltpu.VMEM((2, min(LANES, width), 3 * units), BF16),
            pltpu.VMEM((rows, LANES), F32),
        ]
        + sems(n, pieces) * 4
        + [pltpu.SemaphoreType.DMA((5 + n,)), pltpu.SemaphoreType.DMA((2,))],
        compiler_params=pltpu.CompilerParams(
            collective_id=2, has_side_effects=True, vmem_limit_bytes=67043328
        ),
        cost_estimate=pl.CostEstimate(
            flops=18 * n * rows * width * units, bytes_accessed=500 * 1024 * 1024, transcendentals=0
        ),
        name="mlp",
    )(part.reshape(n, rows, width), x, gain, weights, cotangent, near)


def rows_kernel(
    n, pieces, low_ref, mid_ref, hid_hbm, w_hbm, seq_ref, out_ref,
    hid, w, part_ref, buf, ssend, srecv, gsend, grecv, local_sem,
):
    units = hid.shape[2]
    _, width = low_ref.shape
    loads = [
        pltpu.make_async_copy(hid_hbm, hid, local_sem.at[0]),
        pltpu.make_async_copy(w_hbm.at[:, pl.ds(2 * units, units)], w, local_sem.at[1]),
    ]
    for load in loads:
        load.start()
    line = Line(n)
    me = line.me
    line.barrier()
    scatter = Scatter(line, part_ref, buf, ssend, srecv, pieces)
    gather = Gather(line, seq_ref, gsend, grecv, pieces)
    seq_ref[me] = low_ref[...]

    @pl.loop(0, pieces)
    def _(piece):
        gather.start_own(piece)

    def down(piece):
        rows = scatter.rows(piece)
        for start, count in tiles(width, 512):
            cols = slice(start, start + count)
            value = hid[:, rows, :].reshape(n * scatter.size, units)
            value = mm(value, w[cols, :], 1, 1).astype(BF16)
            part_ref[:, rows, cols] = value.reshape(n, scatter.size, count)

    for load in loads:
        load.wait()
    down(0)
    scatter.start_ends(0)

    @pl.loop(0, pieces + n - 2)
    def _(step):
        for hop in range(1, n):
            piece = step + 1 - hop

            @pl.when(within(piece, pieces))
            def _():
                gather.receive(hop, piece)

        @pl.when(step < pieces)
        def _():
            @pl.when(step + 1 < pieces)
            def _():
                down(step + 1)
                scatter.start_ends(step + 1)

            scatter.middle(step)
            rows = scatter.rows(step)

            def store(total):
                out_ref[rows, :] = (mid_ref[rows, :] + total).astype(BF16)

            scatter.result(step, store)

    scatter.finish()
    gather.finish()


def gather_and_sum(n, low, mid, hidden, weights, pieces=4):
    rows, width = low.shape
    units = hidden.shape[2]
    any_spec = pl.BlockSpec(memory_space=pl.ANY)
    return pl.pallas_call(
        functools.partial(rows_kernel, n, pieces),
        out_shape=(
            jax.ShapeDtypeStruct((n, rows, width), BF16),
            jax.ShapeDtypeStruct((rows, width), BF16),
        ),
        in_specs=[VMEM_SPEC] * 2 + [any_spec] * 2,
        out_specs=(VMEM_SPEC,) * 2,
        scratch_shapes=[
            pltpu.VMEM((n, rows, units), BF16),
            pltpu.VMEM((width, units), BF16),
            pltpu.VMEM((n, rows, width), BF16),
            pltpu.VMEM((n + 1, rows, width), BF16),
        ]
        + sems(n, pieces) * 2
        + [pltpu.SemaphoreType.DMA((2,))],
        compiler_params=comm_params(3),
        cost_estimate=pl.CostEstimate(flops=0, bytes_accessed=300 * 1024 * 1024, transcendentals=0),
        name="gather_and_sum",
    )(low, mid, hidden, weights)


def last_kernel(
    n, dp, pieces, part_ref, x_ref, gain_ref, grad_mid_ref, dgain_mlp_ref, out_ref, gains_ref,
    total_ref, dgain_ref, packed, held, buf, ssend, srecv, gsend, grecv,
):
    line = Line(n)
    all_me = lax.axis_index("dp") * n + line.me
    barrier_all(n, dp)
    scatter = Scatter(line, part_ref, buf, ssend, srecv, pieces)
    scatter.start_ends(0)
    dgain_ref[...] = jnp.zeros_like(dgain_ref)
    packed[...] = jnp.zeros_like(packed)

    @pl.loop(0, pieces)
    def _(piece):
        @pl.when(piece + 1 < pieces)
        def _():
            scatter.start_ends(piece + 1)

        scatter.middle(piece)
        rows = scatter.rows(piece)

        def store(total):
            total_ref[...] = total

        scatter.result(piece, store)
        grad = total_ref[...]
        x = x_ref[rows, :].astype(F32)
        inv = lax.rsqrt(jnp.mean(x * x, axis=1, keepdims=True) + EPS)
        dgain_ref[...] += jnp.sum(grad * x * inv, axis=0, keepdims=True)
        scaled = grad * gain_ref[...]
        mean = jnp.mean(scaled * x, axis=1, keepdims=True)
        out = grad_mid_ref[rows, :] + inv * (scaled - x * (inv * inv * mean))
        out_ref[rows, :] = out.astype(BF16)

    per = x_ref.shape[1] // (n * dp)
    for device in range(n * dp):
        cols = slice(device * per, (device + 1) * per)
        packed[device, :, :per] = dgain_ref[:, cols]
        packed[device, :, per : 2 * per] = dgain_mlp_ref[:, cols]
    held[all_me] = packed[all_me]
    exchange_all(n, dp, lambda peer: packed.at[peer], lambda source: held.at[source], gsend, grecv)
    gains_ref[...] = jnp.sum(held[...], axis=0)
    scatter.finish()


def sum_input_grad(n, dp, part, x, gain, grad_mid, dgain_mlp, packed, pieces=4):
    rows, width = x.shape
    return pl.pallas_call(
        functools.partial(last_kernel, n, dp, pieces),
        out_shape=(
            jax.ShapeDtypeStruct((rows, width), BF16),
            jax.ShapeDtypeStruct((1, packed), F32),
        ),
        in_specs=[VMEM_SPEC] * 5,
        out_specs=(VMEM_SPEC,) * 2,
        scratch_shapes=[
            pltpu.VMEM((rows // pieces, width), F32),
            pltpu.VMEM((1, width), F32),
            pltpu.VMEM((n * dp, 1, packed), F32),
            pltpu.VMEM((n * dp, 1, packed), F32),
            pltpu.VMEM((n + 1, rows, width), BF16),
        ]
        + sems(n, pieces)
        + [pltpu.SemaphoreType.DMA((n * dp,)), pltpu.SemaphoreType.DMA((n * dp,))],
        compiler_params=comm_params(4),
        cost_estimate=pl.CostEstimate(flops=0, bytes_accessed=250 * 1024 * 1024, transcendentals=0),
        name="sum_input_grad",
    )(part.reshape(n, rows, width), x, gain, grad_mid, dgain_mlp)


def widen_kernel(mlp_ref, attn_ref, gate_ref, up_ref, down_ref, query_ref, key_ref, value_ref, out_ref):
    units = gate_ref.shape[1]
    gate_ref[...] = mlp_ref[:, :units].astype(F32)
    up_ref[...] = mlp_ref[:, units : 2 * units].astype(F32)
    down_ref[...] = mlp_ref[:, 2 * units :].astype(F32).T
    q_cols, k_cols = query_ref.shape[1], key_ref.shape[1]
    query_ref[...] = attn_ref[:, :q_cols].astype(F32)
    key_ref[...] = attn_ref[:, q_cols : q_cols + k_cols].astype(F32)
    value_ref[...] = attn_ref[:, q_cols + k_cols : q_cols + 2 * k_cols].astype(F32)
    out_ref[...] = attn_ref[:, q_cols + 2 * k_cols :].astype(F32).T


def widen(mlp_grad, attn_grad, q_cols, k_cols):
    rows, units = mlp_grad.shape[0], mlp_grad.shape[1] // 3
    shapes = [(rows, units)] * 2 + [(units, rows), (rows, q_cols)] + [(rows, k_cols)] * 2 + [(q_cols, rows)]
    return pl.pallas_call(
        widen_kernel,
        out_shape=tuple(jax.ShapeDtypeStruct(shape, F32) for shape in shapes),
        in_specs=[VMEM_SPEC] * 2,
        out_specs=(VMEM_SPEC,) * 7,
        compiler_params=pltpu.CompilerParams(vmem_limit_bytes=56 * 1024 * 1024),
        name="widen",
    )(mlp_grad, attn_grad)


def rotate(half_a, half_b, cos, sin):
    return half_a * cos - half_b * sin, half_b * cos + half_a * sin


def unrotate(half_a, half_b, cos, sin):
    return half_a * cos + half_b * sin, half_b * cos - half_a * sin


def mask_block(size, scores):
    key = lax.broadcasted_iota(jnp.int32, (size, size), 0)
    row = lax.broadcasted_iota(jnp.int32, (size, size), 1)
    return jnp.where(key <= row, scores, NEG_LARGE)


def attend_kernel(
    n, dp, heads, block, pieces, x_ref, gain_ref, cos_ref, sin_ref, cot_hbm, wq_hbm, wk_hbm, wv_hbm, wo_hbm,
    norm_ref, attn_gain_ref, mlp_gain_ref, qkv_ref, kv_ref, out_ref, log_ref, part_ref, w_ref, wo_ref, near_hbm,
    seq, act_ref, gains, wq, wk, wv, wo, send, recv, gsend, grecv, wsend, wrecv, own_sem, csend, crecv,
):
    half = HEAD_SIZE // 2
    rows_all, width = x_ref.shape
    length = n * rows_all
    line = Line(n)
    me = line.me
    mine = lax.axis_index("dp")
    barrier_all(n, dp)
    seq[me] = x_ref[...]
    gains[mine * n + me] = gain_ref[...]
    gather = Gather(line, seq, send, recv, pieces)

    @pl.loop(0, pieces)
    def _(piece):
        gather.start_own(piece)

    def gain_rows(**kind):
        exchange_all(
            n, dp, lambda peer: gain_ref, lambda source: gains.at[source], gsend, grecv, **kind
        )

    gain_rows(start_only=True)

    shards = ((wq_hbm, wq), (wk_hbm, wk), (wv_hbm, wv), (wo_hbm, wo))
    own = [pltpu.make_async_copy(src, dst.at[mine], own_sem.at[i]) for i, (src, dst) in enumerate(shards)]
    pair = mine + 1 - 2 * lax.rem(mine, 2)

    def even_copy(i, offset):
        src, dst = shards[i]
        return pltpu.make_async_remote_copy(
            src_ref=src,
            dst_ref=dst.at[mine],
            send_sem=wsend.at[0, i, offset],
            recv_sem=wrecv.at[0, i, offset],
            device_id={"dp": lax.rem(mine + 2 * offset, dp)},
            device_id_type=MESH,
        )

    def pair_copy(i, offset):
        dst = shards[i][1].at[lax.rem(mine + 2 * offset, dp)]
        return pltpu.make_async_remote_copy(
            src_ref=dst,
            dst_ref=dst,
            send_sem=wsend.at[1, i, offset],
            recv_sem=wrecv.at[1, i, offset],
            device_id={"dp": pair},
            device_id_type=MESH,
        )

    for i in range(4):
        own[i].start()

    @pl.loop(1, dp // 2)
    def _(offset):
        for i in range(4):
            even_copy(i, offset).start()

    def cot_copy(right, hop):
        d = 0 if right else 1
        shard = me - (hop - 1) if right else me + (hop - 1)
        src = cot_hbm if hop == 1 else near_hbm.at[shard]
        return line.copy(src, near_hbm.at[shard], csend.at[d, hop - 1], crecv.at[d, hop - 1], 1 if right else -1)

    inner = (me > 0) & (me < n - 1)

    @pl.when(me == 0)
    def _():
        cot_copy(True, 1).start()

    @pl.when(me == n - 1)
    def _():
        cot_copy(False, 1).start()

    q_cols, k_cols = wq.shape[2], wk.shape[2]
    w_rows, w_cols = wq.shape[1], wo.shape[2]

    def project(shard):
        x = seq[shard].astype(F32)
        inv = lax.rsqrt(jnp.mean(x * x, axis=1, keepdims=True) + EPS)
        norm = (x * inv * attn_gain_ref[...]).astype(BF16)
        rows = piece_rows(shard, rows_all)
        norm_ref[rows, :] = norm
        act_ref[:, rows] = mm(w_ref[...], norm, 0, 1)

    def project_at(hop):
        @pl.when(me - hop >= 0)
        def _():
            project(me - hop)

        @pl.when(me + hop <= n - 1)
        def _():
            project(me + hop)

    def prepare():
        gain_rows(wait_only=True)
        per = width // (n * dp)
        for device in range(n * dp):
            attn_gain_ref[:, device * per : (device + 1) * per] = gains[device, :, :per]
            mlp_gain_ref[:, device * per : (device + 1) * per] = gains[device, :, per : 2 * per]

        @pl.loop(0, dp // 2)
        def _(offset):
            for i in range(4):
                pair_copy(i, offset).wait_recv()

        for d in range(dp):
            rows = slice(d * w_rows, (d + 1) * w_rows)
            w_ref[rows, :q_cols] = wq[d]
            w_ref[rows, q_cols : q_cols + k_cols] = wk[d]
            w_ref[rows, q_cols + k_cols :] = wv[d]
            wo_ref[:, d * w_cols : (d + 1) * w_cols] = wo[d]
        project(me)

    def start_pair():
        for i in range(4):
            own[i].wait()

        @pl.loop(1, dp // 2)
        def _(offset):
            for i in range(4):
                even_copy(i, offset).wait_recv()

        @pl.loop(0, dp // 2)
        def _(offset):
            for i in range(4):
                pair_copy(i, offset).start()

    ready = min(2, n - 1)
    for hop in range(1, n):

        @pl.loop(0, pieces)
        def _(piece):
            gather.receive(hop, piece)
            if hop == ready:

                @pl.when(piece == pieces // 2)
                def _():
                    start_pair()

        @pl.when((me == hop) & (me < n - 1))
        def _():
            cot_copy(True, 1).start()

        @pl.when((n - 1 - me == hop) & (me > 0))
        def _():
            cot_copy(False, 1).start()

        if hop == ready:
            if n == 4:

                @pl.when(me == 1)
                def _():
                    cot_copy_in(line, near_hbm, me - 1, crecv.at[0, 0], csend.at[0, 0], -1).wait_recv()
                    cot_copy(True, 2).start()

                @pl.when(me == 2)
                def _():
                    cot_copy_in(line, near_hbm, me + 1, crecv.at[1, 0], csend.at[1, 0], 1).wait_recv()
                    cot_copy(False, 2).start()

            prepare()
            for earlier in range(1, hop + 1):
                project_at(earlier)
        elif hop > ready:
            project_at(hop)

    cos, sin = cos_ref[...], sin_ref[...]

    @pl.loop(0, heads + 1)
    def _(h):
        base = pl.multiple_of(h * HEAD_SIZE, HEAD_SIZE)
        a, b = rotate(act_ref[pl.ds(base, half), :], act_ref[pl.ds(base + half, half), :], cos, sin)
        qkv_ref[pl.ds(base, half), :] = a.astype(BF16)
        qkv_ref[pl.ds(base + half, half), :] = b.astype(BF16)

    values = pl.ds((heads + 1) * HEAD_SIZE, HEAD_SIZE)
    qkv_ref[values, :] = act_ref[values, :].astype(BF16)
    scale = 1.0 / math.sqrt(HEAD_SIZE)
    kv_ref[...] = qkv_ref[pl.ds(heads * HEAD_SIZE, 2 * HEAD_SIZE), :].T

    @pl.loop(0, heads)
    def _(h):
        base = pl.multiple_of(h * HEAD_SIZE, HEAD_SIZE)
        for i in range(length // block):
            cols = pl.ds(i * block, block)
            query = qkv_ref[pl.ds(base, HEAD_SIZE), cols]
            scores = []
            peak = None
            for j in range(i + 1):
                s = mm(kv_ref[pl.ds(j * block, block), :HEAD_SIZE], query) * scale
                if i == j:
                    s = mask_block(block, s)
                top = jnp.max(s, axis=0, keepdims=True)
                peak = top if peak is None else jnp.maximum(peak, top)
                scores.append(s)
            weights = [jnp.exp(s - peak) for s in scores]
            total = sum(jnp.sum(w, axis=0, keepdims=True) for w in weights)
            log_ref[pl.ds(h, 1), cols] = peak + jnp.log(total)
            inverse = 1.0 / total
            mixed = None
            for j in range(i + 1):
                w = (weights[j] * inverse).astype(BF16)
                v = qkv_ref[values, pl.ds(j * block, block)]
                term = mm(v, w)
                mixed = term if mixed is None else mixed + term
            out_ref[pl.ds(base, HEAD_SIZE), cols] = mixed.astype(BF16)

    for start, count in tiles(width, 512):
        cols = slice(start, start + count)
        part_ref[:, cols] = mm(out_ref[...], wo_ref[:, cols], 0, 0).astype(BF16)

    gather.finish()

    @pl.loop(1, dp // 2)
    def _(offset):
        for i in range(4):
            even_copy(i, offset).wait_send()

    @pl.loop(0, dp // 2)
    def _(offset):
        for i in range(4):
            pair_copy(i, offset).wait_send()

    def arrived(d, hop, shard):
        cot_copy_in(
            line, near_hbm, shard, crecv.at[d, hop - 1], csend.at[d, hop - 1], 1 if d == 1 else -1
        ).wait_recv()

    if n == 4:

        @pl.when(me == 1)
        def _():
            arrived(1, 1, me + 1)
            arrived(1, 2, me + 2)
            cot_copy(True, 2).wait_send()

        @pl.when(me == 2)
        def _():
            arrived(0, 1, me - 1)
            arrived(0, 2, me - 2)
            cot_copy(False, 2).wait_send()

    else:

        @pl.when(inner)
        def _():
            arrived(0, 1, me - 1)
            arrived(1, 1, me + 1)

    @pl.when(me == 0)
    def _():
        arrived(1, 1, me + 1)

    @pl.when(me == n - 1)
    def _():
        arrived(0, 1, me - 1)

    @pl.when(me < n - 1)
    def _():
        cot_copy(True, 1).wait_send()

    @pl.when(me > 0)
    def _():
        cot_copy(False, 1).wait_send()


def cot_copy_in(line, near_hbm, shard, recv, send, step):
    part = near_hbm.at[shard]
    return line.copy(part, part, send, recv, step)


def attend(n, dp, x, gains, weights, cos, sin, cotangent, block=256, pieces=4):
    assert n <= 4 and dp % 2 == 0
    rows, width = x.shape
    length = n * rows
    q_cols, k_cols = weights[0].shape[1], weights[1].shape[1]
    cols_in = q_cols + 2 * k_cols
    heads = cols_in // HEAD_SIZE - 2
    any_spec = pl.BlockSpec(memory_space=pl.ANY)
    dma = pltpu.SemaphoreType.DMA
    return pl.pallas_call(
        functools.partial(attend_kernel, n, dp, heads, block, pieces),
        out_shape=(
            jax.ShapeDtypeStruct((length, width), BF16),
            jax.ShapeDtypeStruct((1, width), F32),
            jax.ShapeDtypeStruct((1, width), F32),
            jax.ShapeDtypeStruct((cols_in, length), BF16),
            jax.ShapeDtypeStruct((length, 2 * HEAD_SIZE), BF16),
            jax.ShapeDtypeStruct((heads * HEAD_SIZE, length), BF16),
            jax.ShapeDtypeStruct((heads, length), F32),
            jax.ShapeDtypeStruct((length, width), BF16),
            jax.ShapeDtypeStruct((width, cols_in), BF16),
            jax.ShapeDtypeStruct((q_cols, width), BF16),
            jax.ShapeDtypeStruct((n,) + cotangent.shape, BF16),
        ),
        in_specs=[VMEM_SPEC] * 4 + [any_spec] * 5,
        out_specs=(VMEM_SPEC,) * 10 + (any_spec,),
        scratch_shapes=[
            pltpu.VMEM((n, rows, width), BF16),
            pltpu.VMEM((cols_in, length), F32),
            pltpu.VMEM((n * dp, 1, gains.shape[1]), F32),
        ]
        + [pltpu.VMEM((dp,) + w.shape, BF16) for w in weights]
        + sems(n, pieces)
        + [dma((n * dp,)), dma((n * dp,)), dma((2, 4, dp // 2)), dma((2, 4, dp // 2)), dma((4,))]
        + [dma((2, 2)), dma((2, 2))],
        compiler_params=comm_params(1),
        cost_estimate=pl.CostEstimate(
            flops=2 * length * width * (cols_in + q_cols),
            bytes_accessed=350 * 1024 * 1024,
            transcendentals=heads * length * length,
        ),
        name="attend",
    )(x, gains, cos, sin, cotangent, *weights)


def attend_back_kernel(
    heads, block, seq_ref, w_ref, wo_ref, qkv_ref, kv_ref, out_ref, log_ref, norm_ref, cos_ref, sin_ref,
    part_ref, wgrad_ref, dkv, grad_ref, dqkv_ref,
):
    half = HEAD_SIZE // 2
    length, width = seq_ref.shape
    cols_in = qkv_ref.shape[0]
    scale = 1.0 / math.sqrt(HEAD_SIZE)
    dkv[...] = jnp.zeros_like(dkv)
    keys = pl.ds(heads * HEAD_SIZE, HEAD_SIZE)
    for first in range(0, length, block):
        rows = pl.ds(first, block)
        grad_ref[:, rows] = mm(wo_ref[...], seq_ref[rows, :], 1, 1).astype(BF16)

    @pl.loop(0, heads)
    def _(h):
        base = pl.multiple_of(h * HEAD_SIZE, HEAD_SIZE)
        mine = pl.ds(base, HEAD_SIZE)
        for i in range(length // block):
            cols = pl.ds(i * block, block)
            query = qkv_ref[mine, cols]
            grad = grad_ref[mine, cols]
            delta = jnp.sum(
                grad.astype(F32) * out_ref[mine, cols].astype(F32), axis=0, keepdims=True
            )
            log_total = log_ref[pl.ds(h, 1), cols]
            dquery = None
            for j in range(i + 1):
                rows = pl.ds(j * block, block)
                s = mm(kv_ref[rows, :HEAD_SIZE], query) * scale
                if i == j:
                    s = mask_block(block, s)
                probs = jnp.exp(s - log_total)
                dprobs = mm(kv_ref[rows, HEAD_SIZE:], grad)
                dscores = (probs * (dprobs - delta) * scale).astype(BF16)
                dkv[0, rows, :] += mm(dscores, query, 1, 1)
                dkv[1, rows, :] += mm(probs.astype(BF16), grad, 1, 1)
                term = mm(qkv_ref[keys, rows], dscores)
                dquery = term if dquery is None else dquery + term
            cos, sin = cos_ref[:, cols], sin_ref[:, cols]
            a, b = unrotate(dquery[:half], dquery[half:], cos, sin)
            dqkv_ref[pl.ds(base, half), cols] = a.astype(BF16)
            dqkv_ref[pl.ds(base + half, half), cols] = b.astype(BF16)

    dkeys = dkv[0].T
    a, b = unrotate(dkeys[:half], dkeys[half:], cos_ref[...], sin_ref[...])
    dqkv_ref[pl.ds(heads * HEAD_SIZE, half), :] = a.astype(BF16)
    dqkv_ref[pl.ds(heads * HEAD_SIZE + half, half), :] = b.astype(BF16)
    dqkv_ref[pl.ds((heads + 1) * HEAD_SIZE, HEAD_SIZE), :] = dkv[1].T.astype(BF16)
    for start, count in tiles(width, 512):
        cols = slice(start, start + count)
        part_ref[:, cols] = mm(dqkv_ref[...], w_ref[cols, :], 0, 1).astype(BF16)
        wgrad_ref[cols, :cols_in] = mm(norm_ref[:, cols], dqkv_ref[...], 0, 1).astype(BF16)
        wgrad_ref[cols, cols_in:] = mm(seq_ref[:, cols], out_ref[...], 0, 1).astype(BF16)


def attend_back(seq, weights, w_out, qkv, kv, out, log_total, norm, cos, sin, block=256):
    length, width = seq.shape
    cols_in = qkv.shape[0]
    heads = cols_in // HEAD_SIZE - 2
    return pl.pallas_call(
        functools.partial(attend_back_kernel, heads, block),
        out_shape=(
            jax.ShapeDtypeStruct((length, width), BF16),
            jax.ShapeDtypeStruct((width, cols_in + w_out.shape[0]), BF16),
        ),
        in_specs=[VMEM_SPEC] * 10,
        out_specs=(VMEM_SPEC,) * 2,
        scratch_shapes=[
            pltpu.VMEM((2, length, HEAD_SIZE), F32),
            pltpu.VMEM((heads * HEAD_SIZE, length), BF16),
            pltpu.VMEM((cols_in, length), BF16),
        ],
        compiler_params=pltpu.CompilerParams(vmem_limit_bytes=56 * 1024 * 1024),
        cost_estimate=pl.CostEstimate(
            flops=6 * length * width * (cols_in + w_out.shape[0]),
            bytes_accessed=120 * 1024 * 1024,
            transcendentals=heads * length * length,
        ),
        name="attend_back",
    )(seq, weights, w_out, qkv, kv, out, log_total, norm, cos, sin)


def local(
    n, dp, x, gain_attn, gain_mlp, w_query, w_key, w_value, w_out, w_gate, w_up, w_down, cotangent
):
    rows, width = x.shape
    length = n * rows
    per = gain_attn.shape[0]
    packed = 2 * per + (-2 * per) % LANES

    mlp_all = lax.all_gather(
        jnp.concatenate([w_gate, w_up, w_down.T], axis=1), "dp", axis=0, tiled=True
    )
    gains = [gain_attn, gain_mlp]
    if packed > 2 * per:
        gains.append(jnp.zeros((packed - 2 * per,), F32))
    cos, sin = tables(length)
    norm_attn, full_attn, full_mlp, qkv, kv, attended, log_total, out_part, w_qkv, w_out_all, near = attend(
        n,
        dp,
        x,
        jnp.concatenate(gains).reshape(1, packed),
        (w_query, w_key, w_value, w_out),
        cos,
        sin,
        cotangent,
    )
    mid, grad_mid, grad_low, dgain_mlp, hidden, mlp_grad = mlp(
        n, out_part, x, full_mlp, mlp_all, cotangent, near
    )
    mlp_grad = lax.psum_scatter(mlp_grad, "dp", scatter_dimension=0, tiled=True)
    grad_mid_seq, block_output = gather_and_sum(n, grad_low, mid, hidden, mlp_all)
    attn_part, attn_grad = attend_back(
        grad_mid_seq.reshape(length, width),
        w_qkv,
        w_out_all,
        qkv,
        kv,
        attended,
        log_total,
        norm_attn,
        cos,
        sin,
    )
    attn_grad = lax.psum_scatter(attn_grad, "dp", scatter_dimension=0, tiled=True)
    input_grad, dgains = sum_input_grad(n, dp, attn_part, x, full_attn, grad_mid, dgain_mlp, packed)
    gate, up, down, query, key, value, out = widen(
        mlp_grad, attn_grad, w_query.shape[1], w_key.shape[1]
    )
    return (
        block_output,
        input_grad,
        dgains[0, :per],
        dgains[0, per : 2 * per],
        query,
        key,
        value,
        out,
        gate,
        up,
        down,
    )


def solution(mesh):
    rows = P(("dp", "tensor"), None)
    gain = P(("dp", "tensor"))
    into = P("dp", "tensor")
    back = P("tensor", "dp")
    in_specs = (rows, gain, gain, into, into, into, back, into, into, back, rows)
    out_specs = (rows, rows, gain, gain, into, into, into, back, into, into, back)

    def body(*args):
        return local(mesh.shape["tensor"], mesh.shape["dp"], *args)

    return jax.shard_map(body, mesh=mesh, in_specs=in_specs, out_specs=out_specs, check_vma=False)
```

```python
import functools
import math

import jax
import jax.numpy as jnp
from jax import lax
from jax.experimental import pallas as pl
from jax.experimental.pallas import tpu as pltpu
from jax.sharding import PartitionSpec as P


HEAD_SIZE = 64
EPS = 1e-05
ROPE_BASE = 10000.0
NEG_LARGE = -1e30
LANES = 128
MESH = pl.DeviceIdType.MESH
F32 = jnp.float32
BF16 = jnp.bfloat16
VMEM_SPEC = pl.BlockSpec(memory_space=pltpu.VMEM)
EARLY = 0


def tables(sequence_length):
    half = HEAD_SIZE // 2
    frequency = ROPE_BASE ** (-(jnp.arange(half, dtype=F32) * 2.0) / HEAD_SIZE)
    angles = frequency[:, None] * jnp.arange(sequence_length, dtype=F32)[None, :]
    return jnp.cos(angles), jnp.sin(angles)


def dims(contract_left, contract_right):
    return (((contract_left,), (contract_right,)), ((), ()))


def mm(left, right, contract_left=1, contract_right=0):
    return lax.dot_general(
        left, right, dims(contract_left, contract_right), preferred_element_type=F32
    )


def piece_rows(piece, size):
    return pl.ds(pl.multiple_of(piece * size, size), size)


class Line:
    def __init__(self, n):
        self.n = n
        self.me = lax.axis_index("tensor")

    def barrier(self):
        barrier = pltpu.get_barrier_semaphore()
        n, me = self.n, self.me

        @pl.when(me > 0)
        def _():
            pl.semaphore_signal(barrier, inc=1, device_id={"tensor": me - 1}, device_id_type=MESH)

        @pl.when(me < n - 1)
        def _():
            pl.semaphore_signal(barrier, inc=1, device_id={"tensor": me + 1}, device_id_type=MESH)

        inner = (me > 0) & (me < n - 1)

        @pl.when(inner)
        def _():
            pl.semaphore_wait(barrier, 2)

        @pl.when(jnp.logical_not(inner))
        def _():
            pl.semaphore_wait(barrier, 1)

    def copy(self, src, dst, send, recv, step):
        return pltpu.make_async_remote_copy(
            src_ref=src,
            dst_ref=dst,
            send_sem=send,
            recv_sem=recv,
            device_id={"tensor": self.me + step},
            device_id_type=MESH,
        )


class Gather:
    def __init__(self, line, buf, send, recv, pieces):
        self.line, self.buf, self.send, self.recv, self.pieces = line, buf, send, recv, pieces
        self.size = buf.shape[1] // pieces

    def message(self, right, hop, piece, shard):
        d = 0 if right else 1
        part = self.buf.at[shard, piece_rows(piece, self.size)]
        return self.line.copy(
            part, part, self.send.at[d, hop - 1, piece], self.recv.at[d, hop - 1, piece], 1 if right else -1
        )

    def start_own(self, piece):
        line = self.line
        me, n = line.me, line.n

        @pl.when(me < n - 1)
        def _():
            self.message(True, 1, piece, me).start()

        @pl.when(me > 0)
        def _():
            self.message(False, 1, piece, me).start()

    def start_hop(self, hop, piece):
        line = self.line
        me, n = line.me, line.n

        @pl.when((me - (hop - 1) >= 0) & (me < n - 1))
        def _():
            self.message(True, hop, piece, me - (hop - 1)).start()

        @pl.when((me + (hop - 1) <= n - 1) & (me > 0))
        def _():
            self.message(False, hop, piece, me + (hop - 1)).start()

    def receive(self, hop, piece, use=None):
        line = self.line
        me, n = line.me, line.n

        @pl.when(me - hop >= 0)
        def _():
            shard = me - hop
            self.message(True, hop, piece, shard).wait_recv()
            if not isinstance(hop, int) or hop < n - 1:

                @pl.when((me < n - 1) & (hop < n - 1))
                def _():
                    self.message(True, hop + 1, piece, shard).start()

            if use is not None:
                use(shard, piece)

        @pl.when(me + hop <= n - 1)
        def _():
            shard = me + hop
            self.message(False, hop, piece, shard).wait_recv()
            if not isinstance(hop, int) or hop < n - 1:

                @pl.when((me > 0) & (hop < n - 1))
                def _():
                    self.message(False, hop + 1, piece, shard).start()

            if use is not None:
                use(shard, piece)

    def finish(self, first_piece=0, end_piece=None):
        line = self.line
        me, n = line.me, line.n

        @pl.loop(first_piece, self.pieces if end_piece is None else end_piece)
        def _(piece):
            for hop in range(1, n):

                @pl.when((me - (hop - 1) >= 0) & (me < n - 1))
                def _():
                    self.message(True, hop, piece, me - (hop - 1)).wait_send()

                @pl.when((me + (hop - 1) <= n - 1) & (me > 0))
                def _():
                    self.message(False, hop, piece, me + (hop - 1)).wait_send()


class Scatter:
    def __init__(self, line, part, buf, send, recv, pieces):
        self.line, self.part, self.buf, self.pieces = line, part, buf, pieces
        self.send, self.recv = send, recv
        self.size = part.shape[1] // pieces

    def rows(self, piece):
        return piece_rows(piece, self.size)

    def outgoing(self, d, target, piece, from_part=False):
        rows, line = self.rows(piece), self.line
        src = (self.part if from_part else self.buf).at[target, rows]
        slot = target
        if d == 1:
            slot = jnp.where(target == line.me - 1, line.n, target)
        return line.copy(
            src,
            self.buf.at[slot, rows],
            self.send.at[d, target, piece],
            self.recv.at[d, target, piece],
            1 if d == 0 else -1,
        )

    def incoming(self, d, target, slot, piece):
        part = self.buf.at[slot, self.rows(piece)]
        return self.line.copy(
            part, part, self.send.at[d, target, piece], self.recv.at[d, target, piece], 1 if d == 0 else -1
        )

    def start_ends(self, piece):
        line = self.line
        me, n = line.me, line.n

        @pl.when(me == 0)
        def _():
            for target in range(n - 1, 0, -1):
                self.outgoing(0, target, piece, True).start()

        @pl.when(me == n - 1)
        def _():
            for target in range(0, n - 1):
                self.outgoing(1, target, piece, True).start()

    def pass_on(self, d, target, piece):
        buf = self.buf
        self.incoming(d, target, target, piece).wait_recv()
        rows = self.rows(piece)
        total = buf[target, rows].astype(F32) + self.part[target, rows].astype(F32)
        buf[target, rows] = total.astype(BF16)
        self.outgoing(d, target, piece).start()

    def passes(self, piece, right, targets, where):
        line = self.line
        me, n = line.me, line.n
        for target in targets:
            held = (me > 0) & (me < target) if right else (me < n - 1) & (me > target)

            @pl.when(where & held)
            def _():
                self.pass_on(0 if right else 1, target, piece)

    def first(self, piece):
        n, left_half = self.line.n, self.line.me < self.line.n // 2
        self.passes(piece, True, (n - 1,), left_half)
        self.passes(piece, False, (0,), jnp.logical_not(left_half))

    def rest(self, piece):
        n, left_half = self.line.n, self.line.me < self.line.n // 2
        right_half = jnp.logical_not(left_half)
        self.passes(piece, True, range(n - 2, 0, -1), left_half)
        self.passes(piece, False, range(1, n - 1), right_half)
        self.passes(piece, False, range(0, n - 1), left_half)
        self.passes(piece, True, range(n - 1, 0, -1), right_half)

    def middle(self, piece):
        self.first(piece)
        self.rest(piece)

    def result(self, piece, store):
        line = self.line
        me, n = line.me, line.n
        rows = self.rows(piece)

        @pl.when(me > 0)
        def _():
            self.incoming(0, me, me, piece).wait_recv()

        @pl.when(me < n - 1)
        def _():
            self.incoming(1, me, n, piece).wait_recv()

        own = self.part[me, rows].astype(F32)

        @pl.when(me == 0)
        def _():
            store(own + self.buf[n, rows].astype(F32))

        @pl.when(me == n - 1)
        def _():
            store(own + self.buf[me, rows].astype(F32))

        @pl.when((me > 0) & (me < n - 1))
        def _():
            store(own + self.buf[me, rows].astype(F32) + self.buf[n, rows].astype(F32))

    def finish(self, ends=True, middles=True):
        line = self.line
        me, n = line.me, line.n
        inner = (me > 0) & (me < n - 1)

        @pl.when((inner & middles) | (jnp.logical_not(inner) & ends))
        def _():
            @pl.loop(0, self.pieces)
            def _(piece):
                for target in range(1, n):

                    @pl.when(me < target)
                    def _():
                        self.outgoing(0, target, piece).wait_send()

                for target in range(0, n - 1):

                    @pl.when(me > target)
                    def _():
                        self.outgoing(1, target, piece).wait_send()


def within(piece, pieces):
    return (piece >= 0) & (piece < pieces)


def sems(n, pieces):
    return [pltpu.SemaphoreType.DMA((2, n, pieces)), pltpu.SemaphoreType.DMA((2, n, pieces))]


def comm_params(collective_id):
    return pltpu.CompilerParams(
        collective_id=collective_id, has_side_effects=True, vmem_limit_bytes=60 * 1024 * 1024
    )


def exchange_all(n, dp, send_row, recv_row, send, recv, start_only=False, wait_only=False):
    devices = n * dp
    me = lax.axis_index("dp") * n + lax.axis_index("tensor")

    def message(offset, peer, source):
        return pltpu.make_async_remote_copy(
            src_ref=send_row(peer),
            dst_ref=recv_row(source),
            send_sem=send.at[offset],
            recv_sem=recv.at[offset],
            device_id={"dp": peer // n, "tensor": peer % n},
            device_id_type=MESH,
        )

    if not wait_only:

        @pl.loop(1, devices)
        def _(offset):
            message(offset, lax.rem(me + offset, devices), me).start()

    if not start_only:

        @pl.loop(1, devices)
        def _(offset):
            copy = message(offset, lax.rem(me + offset, devices), me)
            copy.wait_send()
            copy.wait_recv()


def barrier_all(n, dp):
    devices = n * dp
    me = lax.axis_index("dp") * n + lax.axis_index("tensor")
    barrier = pltpu.get_barrier_semaphore()

    @pl.loop(1, devices)
    def _(offset):
        peer = lax.rem(me + offset, devices)
        pl.semaphore_signal(
            barrier, inc=1, device_id={"dp": peer // n, "tensor": peer % n}, device_id_type=MESH
        )

    pl.semaphore_wait(barrier, devices - 1)


def tiles(extent, size):
    return [(start, min(size, extent - start)) for start in range(0, extent, size)]


def mlp_kernel(
    n, pieces, part_ref, x_ref, gain_ref, w_hbm, cot_hbm, near_hbm,
    mid_ref, grad_ref, dgain_ref, hid_hbm, wgrad_hbm, low_hbm,
    w, cot, seq, buf, npart, buf_back, hid, dgate, dup, stage, inv_ref,
    ssend, srecv, gsend, grecv, bsend, brecv, csend, crecv, lsend, lrecv, local_sem, stage_sem,
):
    line = Line(n)
    me = line.me
    rows_all, width = part_ref.shape[1:]
    units = hid.shape[2]
    weight_load = pltpu.make_async_copy(w_hbm, w, local_sem.at[0])
    own_load = pltpu.make_async_copy(cot_hbm, cot.at[me], local_sem.at[1])
    inner = (me > 0) & (me < n - 1)

    def near_load(shard):
        return pltpu.make_async_copy(near_hbm.at[shard], cot.at[shard], local_sem.at[5 + shard])

    def each_near(act):
        for shard in range(n):
            here = (me != shard) & (inner | (me - shard == 1) | (shard - me == 1))

            @pl.when(here)
            def _():
                act(near_load(shard))

    each_near(lambda copy: copy.start())
    own_load.start()
    weight_load.start()
    line.barrier()
    scatter = Scatter(line, part_ref, buf, ssend, srecv, pieces)
    gather = Gather(line, seq, gsend, grecv, pieces)
    scatter_back = Scatter(line, npart, buf_back, bsend, brecv, pieces)
    cot_gather = Gather(line, cot, csend, crecv, pieces)
    low_gather = Gather(line, buf, lsend, lrecv, pieces)
    size = scatter.size
    scatter.start_ends(0)
    dgain_ref[...] = jnp.zeros_like(dgain_ref)

    each_near(lambda copy: copy.wait())

    def each_far(act):
        for hop in range(2, n):

            @pl.when(me == n - 2)
            def _():
                act(True, hop, me - (hop - 1))

            @pl.when(me == 1)
            def _():
                act(False, hop, me + (hop - 1))

    def far_start(piece):
        each_far(lambda right, hop, shard: cot_gather.message(right, hop, piece, shard).start())

    def far_sent(piece):
        each_far(lambda right, hop, shard: cot_gather.message(right, hop, piece, shard).wait_send())

    def far_arrived(piece):
        for hop in range(2, n):

            @pl.when(me == n - 1)
            def _():
                cot_gather.message(True, hop, piece, me - hop).wait_recv()

            @pl.when(me == 0)
            def _():
                cot_gather.message(False, hop, piece, me + hop).wait_recv()

    for piece in range(min(2, pieces)):
        far_start(piece)

    def norm(piece):
        rows = scatter.rows(piece)

        def store(total):
            mid_ref[rows, :] = x_ref[rows, :].astype(F32) + total

        scatter.result(piece, store)
        mid = mid_ref[rows, :]
        inv = lax.rsqrt(jnp.mean(mid * mid, axis=1, keepdims=True) + EPS)
        inv_ref[rows, :] = jnp.broadcast_to(inv, (size, LANES))
        seq[me, rows, :] = (mid * inv * gain_ref[...]).astype(BF16)

    def back(piece):
        rows = scatter.rows(piece)

        def store(total):
            grad_ref[rows, :] = total

        scatter_back.result(piece, store)
        grad = grad_ref[rows, :]
        mid = mid_ref[rows, :]
        inv = inv_ref[rows, 0:1]
        dgain_ref[...] += jnp.sum(grad * mid * inv, axis=0, keepdims=True)
        scaled = grad * gain_ref[...]
        mean = jnp.mean(scaled * mid, axis=1, keepdims=True)
        out = cot[me, rows, :].astype(F32) + inv * (scaled - mid * (inv * inv * mean))
        grad_ref[rows, :] = out
        buf[me, rows, :] = out.astype(BF16)

    def flat(ref, piece):
        value = ref[:, scatter.rows(piece), :]
        return value.reshape(n * size, value.shape[2])

    def feed(piece):
        rows = scatter.rows(piece)
        for start, count in tiles(units, 512):
            x = flat(seq, piece)
            gate = mm(x, w[:, start : start + count])
            up = mm(x, w[:, units + start : units + start + count])
            dhidden = mm(flat(cot, piece), w[:, 2 * units + start : 2 * units + start + count])
            sigmoid = jax.nn.sigmoid(gate)
            act = gate * sigmoid
            cols = slice(start, start + count)
            shape = (n, size, count)
            hid[:, rows, cols] = (act * up).astype(BF16).reshape(shape)
            dup[:, rows, cols] = (dhidden * act).astype(BF16).reshape(shape)
            dgate[:, rows, cols] = (
                (dhidden * up * sigmoid * (1.0 + gate * (1.0 - sigmoid))).astype(BF16).reshape(shape)
            )
        for start, count in tiles(width, 512):
            cols = slice(start, start + count)
            total = mm(flat(dgate, piece), w[cols, :units], 1, 1)
            total += mm(flat(dup, piece), w[cols, units : 2 * units], 1, 1)
            npart[:, rows, cols] = total.astype(BF16).reshape(n, size, count)

    step_rows = min(LANES, width)
    count = width // step_rows

    def save(index, slot):
        return pltpu.make_async_copy(
            stage.at[slot],
            wgrad_hbm.at[pl.ds(pl.multiple_of(index * step_rows, step_rows), step_rows), :],
            stage_sem.at[slot],
        )

    def weight_grads(events):
        @pl.loop(0, count)
        def _(index):
            for at, event in events:

                @pl.when(index == at)
                def _():
                    event()

            slot = lax.rem(index, 2)
            cols = pl.ds(pl.multiple_of(index * step_rows, step_rows), step_rows)

            @pl.when(index >= 2)
            def _():
                save(index - 2, slot).wait()

            x = seq[:, :, cols].reshape(n * rows_all, step_rows)
            g = cot[:, :, cols].reshape(n * rows_all, step_rows)
            for at, left, right in ((0, x, dgate), (1, x, dup), (2, g, hid)):
                value = right[...].reshape(n * rows_all, units)
                stage[slot, :, at * units : (at + 1) * units] = mm(left, value, 0, 0).astype(BF16)
            save(index, slot).start()

    hid_save = pltpu.make_async_copy(hid, hid_hbm, local_sem.at[2])

    @pl.loop(0, pieces + n - 1)
    def _(step):
        first = step < pieces

        @pl.when(first)
        def _():
            @pl.when(step + 1 < pieces)
            def _():
                scatter.start_ends(step + 1)

            scatter.middle(step)

            @pl.when(step + 2 < pieces)
            def _():
                far_start(step + 2)

        for hop in range(1, n):
            piece = step - hop

            @pl.when(within(piece, pieces))
            def _():
                gather.receive(hop, piece)

        @pl.when(first)
        def _():
            norm(step)
            gather.start_own(step)

        ready = step - (n - 1)

        @pl.when(ready == 0)
        def _():
            own_load.wait()
            weight_load.wait()

        @pl.when(ready == 1)
        def _():
            scatter.finish(ends=False)

        for hop in range(1, n):
            piece = ready - 1 - hop

            @pl.when(within(piece, EARLY))
            def _():
                low_gather.receive(hop, piece)

        @pl.when(ready >= 1)
        def _():
            scatter_back.middle(ready - 1)

        @pl.when(ready >= 0)
        def _():
            far_arrived(ready)
            feed(ready)
            scatter_back.start_ends(ready)

        @pl.when(ready >= 1)
        def _():
            back(ready - 1)

            @pl.when(ready - 1 < EARLY)
            def _():
                low_gather.start_own(ready - 1)

    hid_save.start()
    last = pieces - 1

    def low_arrivals(step):
        for hop in range(1, n):
            piece = step - hop
            if 0 <= piece < EARLY:
                low_gather.receive(hop, piece)

    late = [
        (lambda step: lambda: low_arrivals(step))(step) for step in range(pieces - 1, pieces + n - 2)
    ]
    events = [
        (count * 3 // 8, lambda: scatter_back.first(last)),
        (count * 3 // 4, lambda: scatter_back.rest(last)),
    ]
    if EARLY:
        events += [(count * (2 * i + 1) // (2 * len(late)), event) for i, event in enumerate(late)]
    weight_grads(events)
    back(last)
    own_rows, early_rows = pl.ds(EARLY * size, rows_all - EARLY * size), pl.ds(0, EARLY * size)
    low_saves = [
        pltpu.make_async_copy(buf.at[me, own_rows], low_hbm.at[me, own_rows], local_sem.at[4])
    ]
    if EARLY:
        low_saves.append(
            pltpu.make_async_copy(
                buf.at[pl.ds(0, n), early_rows], low_hbm.at[:, early_rows], local_sem.at[3]
            )
        )
    for save_low in low_saves:
        save_low.start()
    scatter.finish(middles=False)
    gather.finish()
    scatter_back.finish()
    low_gather.finish(0, EARLY)

    @pl.loop(0, pieces)
    def _(piece):
        far_sent(piece)

    for save_low in low_saves:
        save_low.wait()
    hid_save.wait()
    for index in range(max(count - 2, 0), count):
        save(index, index % 2).wait()


def mlp(n, part, x, gain, weights, cotangent, near, pieces=4):
    rows, width = x.shape
    units = weights.shape[1] // 3
    any_spec = pl.BlockSpec(memory_space=pl.ANY)
    return pl.pallas_call(
        functools.partial(mlp_kernel, n, pieces),
        out_shape=(
            jax.ShapeDtypeStruct((rows, width), F32),
            jax.ShapeDtypeStruct((rows, width), F32),
            jax.ShapeDtypeStruct((1, width), F32),
            jax.ShapeDtypeStruct((n, rows, units), BF16),
            jax.ShapeDtypeStruct((width, 3 * units), BF16),
            jax.ShapeDtypeStruct((n, rows, width), BF16),
        ),
        in_specs=[VMEM_SPEC] * 3 + [any_spec] * 3,
        out_specs=(VMEM_SPEC,) * 3 + (any_spec,) * 3,
        scratch_shapes=[
            pltpu.VMEM((width, 3 * units), BF16),
            pltpu.VMEM((n, rows, width), BF16),
            pltpu.VMEM((n, rows, width), BF16),
            pltpu.VMEM((n + 1, rows, width), BF16),
            pltpu.VMEM((n, rows, width), BF16),
            pltpu.VMEM((n + 1, rows, width), BF16),
            pltpu.VMEM((n, rows, units), BF16),
            pltpu.VMEM((n, rows, units), BF16),
            pltpu.VMEM((n, rows, units), BF16),
            pltpu.VMEM((2, min(LANES, width), 3 * units), BF16),
            pltpu.VMEM((rows, LANES), F32),
        ]
        + sems(n, pieces) * 5
        + [pltpu.SemaphoreType.DMA((5 + n,)), pltpu.SemaphoreType.DMA((2,))],
        compiler_params=pltpu.CompilerParams(
            collective_id=2, has_side_effects=True, vmem_limit_bytes=67043328
        ),
        cost_estimate=pl.CostEstimate(
            flops=18 * n * rows * width * units, bytes_accessed=500 * 1024 * 1024, transcendentals=0
        ),
        name="mlp",
    )(part.reshape(n, rows, width), x, gain, weights, cotangent, near)


def last_kernel(
    n, dp, pieces, part_ref, x_ref, gain_ref, grad_mid_ref, dgain_mlp_ref, out_ref, gains_ref,
    total_ref, dgain_ref, packed, held, buf, ssend, srecv, gsend, grecv,
):
    line = Line(n)
    all_me = lax.axis_index("dp") * n + line.me
    barrier_all(n, dp)
    scatter = Scatter(line, part_ref, buf, ssend, srecv, pieces)
    scatter.start_ends(0)
    dgain_ref[...] = jnp.zeros_like(dgain_ref)
    packed[...] = jnp.zeros_like(packed)

    @pl.loop(0, pieces)
    def _(piece):
        @pl.when(piece + 1 < pieces)
        def _():
            scatter.start_ends(piece + 1)

        scatter.middle(piece)
        rows = scatter.rows(piece)

        def store(total):
            total_ref[...] = total

        scatter.result(piece, store)
        grad = total_ref[...]
        x = x_ref[rows, :].astype(F32)
        inv = lax.rsqrt(jnp.mean(x * x, axis=1, keepdims=True) + EPS)
        dgain_ref[...] += jnp.sum(grad * x * inv, axis=0, keepdims=True)
        scaled = grad * gain_ref[...]
        mean = jnp.mean(scaled * x, axis=1, keepdims=True)
        out = grad_mid_ref[rows, :] + inv * (scaled - x * (inv * inv * mean))
        out_ref[rows, :] = out.astype(BF16)

    per = x_ref.shape[1] // (n * dp)
    for device in range(n * dp):
        cols = slice(device * per, (device + 1) * per)
        packed[device, :, :per] = dgain_ref[:, cols]
        packed[device, :, per : 2 * per] = dgain_mlp_ref[:, cols]
    held[all_me] = packed[all_me]
    exchange_all(n, dp, lambda peer: packed.at[peer], lambda source: held.at[source], gsend, grecv)
    gains_ref[...] = jnp.sum(held[...], axis=0)
    scatter.finish()


def sum_input_grad(n, dp, part, x, gain, grad_mid, dgain_mlp, packed, pieces=4):
    rows, width = x.shape
    return pl.pallas_call(
        functools.partial(last_kernel, n, dp, pieces),
        out_shape=(
            jax.ShapeDtypeStruct((rows, width), BF16),
            jax.ShapeDtypeStruct((1, packed), F32),
        ),
        in_specs=[VMEM_SPEC] * 5,
        out_specs=(VMEM_SPEC,) * 2,
        scratch_shapes=[
            pltpu.VMEM((rows // pieces, width), F32),
            pltpu.VMEM((1, width), F32),
            pltpu.VMEM((n * dp, 1, packed), F32),
            pltpu.VMEM((n * dp, 1, packed), F32),
            pltpu.VMEM((n + 1, rows, width), BF16),
        ]
        + sems(n, pieces)
        + [pltpu.SemaphoreType.DMA((n * dp,)), pltpu.SemaphoreType.DMA((n * dp,))],
        compiler_params=comm_params(4),
        cost_estimate=pl.CostEstimate(flops=0, bytes_accessed=250 * 1024 * 1024, transcendentals=0),
        name="sum_input_grad",
    )(part.reshape(n, rows, width), x, gain, grad_mid, dgain_mlp)


def widen_kernel(mlp_ref, attn_ref, gate_ref, up_ref, down_ref, query_ref, key_ref, value_ref, out_ref):
    units = gate_ref.shape[1]
    gate_ref[...] = mlp_ref[:, :units].astype(F32)
    up_ref[...] = mlp_ref[:, units : 2 * units].astype(F32)
    down_ref[...] = mlp_ref[:, 2 * units :].astype(F32).T
    q_cols, k_cols = query_ref.shape[1], key_ref.shape[0]
    query_ref[...] = attn_ref[:, :q_cols].astype(F32)
    key_ref[...] = attn_ref[:, q_cols : q_cols + k_cols].astype(F32).T
    value_ref[...] = attn_ref[:, q_cols + k_cols : q_cols + 2 * k_cols].astype(F32).T
    out_ref[...] = attn_ref[:, q_cols + 2 * k_cols :].astype(F32).T


def widen(mlp_grad, attn_grad, q_cols, k_cols):
    rows, units = mlp_grad.shape[0], mlp_grad.shape[1] // 3
    shapes = [(rows, units)] * 2 + [(units, rows), (rows, q_cols)] + [(k_cols, rows)] * 2 + [(q_cols, rows)]
    return pl.pallas_call(
        widen_kernel,
        out_shape=tuple(jax.ShapeDtypeStruct(shape, F32) for shape in shapes),
        in_specs=[VMEM_SPEC] * 2,
        out_specs=(VMEM_SPEC,) * 7,
        compiler_params=pltpu.CompilerParams(vmem_limit_bytes=56 * 1024 * 1024),
        name="widen",
    )(mlp_grad, attn_grad)


def rotate(half_a, half_b, cos, sin):
    return half_a * cos - half_b * sin, half_b * cos + half_a * sin


def unrotate(half_a, half_b, cos, sin):
    return half_a * cos + half_b * sin, half_b * cos - half_a * sin


def mask_block(size):
    key = lax.broadcasted_iota(jnp.int32, (size, size), 0)
    row = lax.broadcasted_iota(jnp.int32, (size, size), 1)
    return jnp.where(key <= row, 0.0, NEG_LARGE)


def attend_kernel(
    n, dp, heads, block, pieces, x_ref, gain_ref, cos_ref, sin_ref, cot_hbm, wq_hbm, wk_hbm, wv_hbm, wo_hbm,
    norm_ref, attn_gain_ref, mlp_gain_ref, qkv_ref, kv_ref, out_ref, log_ref, part_ref, w_ref, wo_ref, near_hbm,
    seq, act_ref, mask_ref, gains, wq, wk, wv, wo, send, recv, gsend, grecv, wsend, wrecv, own_sem, csend, crecv,
):
    half = HEAD_SIZE // 2
    rows_all, width = x_ref.shape
    length = n * rows_all
    line = Line(n)
    me = line.me
    mine = lax.axis_index("dp")
    barrier_all(n, dp)
    seq[me] = x_ref[...]
    gains[mine * n + me] = gain_ref[...]
    gather = Gather(line, seq, send, recv, pieces)

    @pl.loop(0, pieces)
    def _(piece):
        gather.start_own(piece)

    def gain_rows(**kind):
        exchange_all(
            n, dp, lambda peer: gain_ref, lambda source: gains.at[source], gsend, grecv, **kind
        )

    gain_rows(start_only=True)

    shards = ((wq_hbm, wq), (wk_hbm, wk), (wv_hbm, wv), (wo_hbm, wo))
    own = [pltpu.make_async_copy(src, dst.at[mine], own_sem.at[i]) for i, (src, dst) in enumerate(shards)]
    pair = mine + 1 - 2 * lax.rem(mine, 2)

    def even_copy(i, offset):
        src, dst = shards[i]
        return pltpu.make_async_remote_copy(
            src_ref=src,
            dst_ref=dst.at[mine],
            send_sem=wsend.at[0, i, offset],
            recv_sem=wrecv.at[0, i, offset],
            device_id={"dp": lax.rem(mine + 2 * offset, dp)},
            device_id_type=MESH,
        )

    def pair_copy(i, offset):
        dst = shards[i][1].at[lax.rem(mine + 2 * offset, dp)]
        return pltpu.make_async_remote_copy(
            src_ref=dst,
            dst_ref=dst,
            send_sem=wsend.at[1, i, offset],
            recv_sem=wrecv.at[1, i, offset],
            device_id={"dp": pair},
            device_id_type=MESH,
        )

    for i in range(4):
        own[i].start()

    @pl.loop(1, dp // 2)
    def _(offset):
        for i in range(4):
            even_copy(i, offset).start()

    def cot_copy(right, hop):
        d = 0 if right else 1
        shard = me - (hop - 1) if right else me + (hop - 1)
        src = cot_hbm if hop == 1 else near_hbm.at[shard]
        return line.copy(src, near_hbm.at[shard], csend.at[d, hop - 1], crecv.at[d, hop - 1], 1 if right else -1)

    inner = (me > 0) & (me < n - 1)

    @pl.when(me == 0)
    def _():
        cot_copy(True, 1).start()

    @pl.when(me == n - 1)
    def _():
        cot_copy(False, 1).start()

    q_cols, k_cols = wq.shape[2], wk.shape[1]
    w_rows, w_cols = wq.shape[1], wo.shape[2]

    def project(shard):
        x = seq[shard].astype(F32)
        inv = lax.rsqrt(jnp.mean(x * x, axis=1, keepdims=True) + EPS)
        norm = (x * inv * attn_gain_ref[...]).astype(BF16)
        rows = piece_rows(shard, rows_all)
        norm_ref[rows, :] = norm
        act_ref[:, rows] = mm(w_ref[...], norm, 0, 1)

    def project_at(hop):
        @pl.when(me - hop >= 0)
        def _():
            project(me - hop)

        @pl.when(me + hop <= n - 1)
        def _():
            project(me + hop)

    def prepare():
        gain_rows(wait_only=True)
        per = width // (n * dp)
        for device in range(n * dp):
            attn_gain_ref[:, device * per : (device + 1) * per] = gains[device, :, :per]
            mlp_gain_ref[:, device * per : (device + 1) * per] = gains[device, :, per : 2 * per]

        @pl.loop(0, dp // 2)
        def _(offset):
            for i in range(4):
                pair_copy(i, offset).wait_recv()

        for d in range(dp):
            rows = slice(d * w_rows, (d + 1) * w_rows)
            w_ref[rows, :q_cols] = wq[d]
            w_ref[rows, q_cols : q_cols + k_cols] = wk[d].T
            w_ref[rows, q_cols + k_cols :] = wv[d].T
            wo_ref[:, d * w_cols : (d + 1) * w_cols] = wo[d]
        project(me)

    def start_pair():
        for i in range(4):
            own[i].wait()

        @pl.loop(1, dp // 2)
        def _(offset):
            for i in range(4):
                even_copy(i, offset).wait_recv()

        @pl.loop(0, dp // 2)
        def _(offset):
            for i in range(4):
                pair_copy(i, offset).start()

    ready = min(2, n - 1)
    for hop in range(1, n):

        @pl.loop(0, pieces)
        def _(piece):
            gather.receive(hop, piece)
            if hop == ready:

                @pl.when(piece == pieces // 2)
                def _():
                    start_pair()

        @pl.when((me == hop) & (me < n - 1))
        def _():
            cot_copy(True, 1).start()

        @pl.when((n - 1 - me == hop) & (me > 0))
        def _():
            cot_copy(False, 1).start()

        if hop == ready:
            if n == 4:

                @pl.when(me == 1)
                def _():
                    cot_copy_in(line, near_hbm, me - 1, crecv.at[0, 0], csend.at[0, 0], -1).wait_recv()
                    cot_copy(True, 2).start()

                @pl.when(me == 2)
                def _():
                    cot_copy_in(line, near_hbm, me + 1, crecv.at[1, 0], csend.at[1, 0], 1).wait_recv()
                    cot_copy(False, 2).start()

            prepare()
            for earlier in range(1, hop + 1):
                project_at(earlier)
        elif hop > ready:
            project_at(hop)

    cos, sin = cos_ref[...], sin_ref[...]

    scale = 1.0 / math.sqrt(HEAD_SIZE)

    @pl.loop(0, heads + 1)
    def _(h):
        base = pl.multiple_of(h * HEAD_SIZE, HEAD_SIZE)
        a, b = rotate(act_ref[pl.ds(base, half), :], act_ref[pl.ds(base + half, half), :], cos, sin)
        factor = jnp.where(h < heads, scale, 1.0)
        a, b = a * factor, b * factor
        qkv_ref[pl.ds(base, half), :] = a.astype(BF16)
        qkv_ref[pl.ds(base + half, half), :] = b.astype(BF16)

    values = pl.ds((heads + 1) * HEAD_SIZE, HEAD_SIZE)
    qkv_ref[values, :] = act_ref[values, :].astype(BF16)
    mask_ref[...] = mask_block(block)
    kv_ref[...] = qkv_ref[pl.ds(heads * HEAD_SIZE, 2 * HEAD_SIZE), :].T

    @pl.loop(0, heads)
    def _(h):
        base = pl.multiple_of(h * HEAD_SIZE, HEAD_SIZE)
        for i in range(length // block):
            cols = pl.ds(i * block, block)
            query = qkv_ref[pl.ds(base, HEAD_SIZE), cols]
            scores = []
            peak = None
            for j in range(i + 1):
                s = mm(kv_ref[pl.ds(j * block, block), :HEAD_SIZE], query)
                if i == j:
                    s = s + mask_ref[...]
                top = jnp.max(s, axis=0, keepdims=True)
                peak = top if peak is None else jnp.maximum(peak, top)
                scores.append(s)
            weights = [jnp.exp(s - peak) for s in scores]
            total = sum(jnp.sum(w, axis=0, keepdims=True) for w in weights)
            log_ref[pl.ds(h, 1), cols] = peak + jnp.log(total)
            inverse = 1.0 / total
            mixed = None
            for j in range(i + 1):
                w = (weights[j] * inverse).astype(BF16)
                v = qkv_ref[values, pl.ds(j * block, block)]
                term = mm(v, w)
                mixed = term if mixed is None else mixed + term
            out_ref[pl.ds(base, HEAD_SIZE), cols] = mixed.astype(BF16)

    for start, count in tiles(width, 512):
        cols = slice(start, start + count)
        part_ref[:, cols] = mm(out_ref[...], wo_ref[:, cols], 0, 0).astype(BF16)

    gather.finish()

    @pl.loop(1, dp // 2)
    def _(offset):
        for i in range(4):
            even_copy(i, offset).wait_send()

    @pl.loop(0, dp // 2)
    def _(offset):
        for i in range(4):
            pair_copy(i, offset).wait_send()

    def arrived(d, hop, shard):
        cot_copy_in(
            line, near_hbm, shard, crecv.at[d, hop - 1], csend.at[d, hop - 1], 1 if d == 1 else -1
        ).wait_recv()

    if n == 4:

        @pl.when(me == 1)
        def _():
            arrived(1, 1, me + 1)
            arrived(1, 2, me + 2)
            cot_copy(True, 2).wait_send()

        @pl.when(me == 2)
        def _():
            arrived(0, 1, me - 1)
            arrived(0, 2, me - 2)
            cot_copy(False, 2).wait_send()

    else:

        @pl.when(inner)
        def _():
            arrived(0, 1, me - 1)
            arrived(1, 1, me + 1)

    @pl.when(me == 0)
    def _():
        arrived(1, 1, me + 1)

    @pl.when(me == n - 1)
    def _():
        arrived(0, 1, me - 1)

    @pl.when(me < n - 1)
    def _():
        cot_copy(True, 1).wait_send()

    @pl.when(me > 0)
    def _():
        cot_copy(False, 1).wait_send()


def cot_copy_in(line, near_hbm, shard, recv, send, step):
    part = near_hbm.at[shard]
    return line.copy(part, part, send, recv, step)


def attend(n, dp, x, gains, weights, cos, sin, cotangent, block=256, pieces=4):
    assert n <= 4 and dp % 2 == 0
    rows, width = x.shape
    length = n * rows
    q_cols, k_cols = weights[0].shape[1], weights[1].shape[0]
    cols_in = q_cols + 2 * k_cols
    heads = cols_in // HEAD_SIZE - 2
    any_spec = pl.BlockSpec(memory_space=pl.ANY)
    dma = pltpu.SemaphoreType.DMA
    return pl.pallas_call(
        functools.partial(attend_kernel, n, dp, heads, block, pieces),
        out_shape=(
            jax.ShapeDtypeStruct((length, width), BF16),
            jax.ShapeDtypeStruct((1, width), F32),
            jax.ShapeDtypeStruct((1, width), F32),
            jax.ShapeDtypeStruct((cols_in, length), BF16),
            jax.ShapeDtypeStruct((length, 2 * HEAD_SIZE), BF16),
            jax.ShapeDtypeStruct((heads * HEAD_SIZE, length), BF16),
            jax.ShapeDtypeStruct((heads, length), F32),
            jax.ShapeDtypeStruct((length, width), BF16),
            jax.ShapeDtypeStruct((width, cols_in), BF16),
            jax.ShapeDtypeStruct((q_cols, width), BF16),
            jax.ShapeDtypeStruct((n,) + cotangent.shape, BF16),
        ),
        in_specs=[VMEM_SPEC] * 4 + [any_spec] * 5,
        out_specs=(VMEM_SPEC,) * 10 + (any_spec,),
        scratch_shapes=[
            pltpu.VMEM((n, rows, width), BF16),
            pltpu.VMEM((cols_in, length), F32),
            pltpu.VMEM((block, block), F32),
            pltpu.VMEM((n * dp, 1, gains.shape[1]), F32),
        ]
        + [pltpu.VMEM((dp,) + w.shape, BF16) for w in weights]
        + sems(n, pieces)
        + [dma((n * dp,)), dma((n * dp,)), dma((2, 4, dp // 2)), dma((2, 4, dp // 2)), dma((4,))]
        + [dma((2, 2)), dma((2, 2))],
        compiler_params=comm_params(1),
        cost_estimate=pl.CostEstimate(
            flops=2 * length * width * (cols_in + q_cols),
            bytes_accessed=350 * 1024 * 1024,
            transcendentals=heads * length * length,
        ),
        name="attend",
    )(x, gains, cos, sin, cotangent, *weights)


def attend_back_kernel(
    n, heads, block, pieces, mid_ref, kv_ref, log_ref, cos_ref, sin_ref,
    low_hbm, hid_hbm, w_mlp_hbm, wo_hbm, w_hbm, qkv_hbm, out_hbm, norm_hbm,
    rows_ref, part_ref, wgrad_hbm,
    seq, hid, w_down, down_ref, buf, wo_ref, w_ref, qkv_ref, out_ref, norm_ref,
    dkv, mask_ref, grad_ref, dqkv_ref, wgrad, ssend, srecv, gsend, grecv, load_sem, save_sem,
):
    half = HEAD_SIZE // 2
    rows_all, width = mid_ref.shape
    units = hid.shape[2]
    cols_in = qkv_ref.shape[0]
    scale = 1.0 / math.sqrt(HEAD_SIZE)
    me = lax.axis_index("tensor")
    size = rows_all // pieces
    own_rows, early_rows = pl.ds(EARLY * size, rows_all - EARLY * size), pl.ds(0, EARLY * size)
    pairs = (
        (low_hbm.at[me, own_rows], seq.at[me, own_rows]),
        (hid_hbm, hid),
        (w_mlp_hbm.at[:, pl.ds(2 * units, units)], w_down),
        (wo_hbm, wo_ref),
        (qkv_hbm, qkv_ref),
        (out_hbm, out_ref),
        (w_hbm, w_ref),
        (norm_hbm, norm_ref),
    )
    if EARLY:
        pairs += ((low_hbm.at[:, early_rows], seq.at[:, early_rows]),)
    loads = [pltpu.make_async_copy(src, dst, load_sem.at[i]) for i, (src, dst) in enumerate(pairs)]
    for load in loads:
        load.start()
    line = Line(n)
    line.barrier()
    scatter = Scatter(line, down_ref, buf, ssend, srecv, pieces)
    gather = Gather(line, seq, gsend, grecv, pieces)
    loads[0].wait()

    @pl.loop(EARLY, pieces)
    def _(piece):
        gather.start_own(piece)

    dkv[...] = jnp.zeros_like(dkv)
    mask_ref[...] = mask_block(block)
    keys = pl.ds(heads * HEAD_SIZE, HEAD_SIZE)

    def project(shard):
        grad_ref[:, piece_rows(shard, rows_all)] = mm(wo_ref[...], seq[shard], 1, 1).astype(BF16)

    def start_sums():
        loads[1].wait()
        loads[2].wait()

        @pl.loop(0, pieces)
        def _(piece):
            rows = scatter.rows(piece)
            for start, count in tiles(width, 512):
                cols = slice(start, start + count)
                value = hid[:, rows, :].reshape(n * scatter.size, units)
                value = mm(value, w_down[cols, :], 1, 1).astype(BF16)
                down_ref[:, rows, cols] = value.reshape(n, scatter.size, count)
            scatter.start_ends(piece)

    def sum_piece(piece):
        scatter.middle(piece)
        rows = scatter.rows(piece)

        def store(total):
            rows_ref[rows, :] = (mid_ref[rows, :] + total).astype(BF16)

        scatter.result(piece, store)

    start_sums()
    for load in loads[3:]:
        load.wait()

    def attention_rows(i):
        cols = pl.ds(i * block, block)
        cos, sin = cos_ref[:, cols], sin_ref[:, cols]

        @pl.loop(0, heads)
        def _(h):
            base = pl.multiple_of(h * HEAD_SIZE, HEAD_SIZE)
            mine = pl.ds(base, HEAD_SIZE)
            query = qkv_ref[mine, cols]
            grad = grad_ref[mine, cols]
            delta = jnp.sum(
                grad.astype(F32) * out_ref[mine, cols].astype(F32), axis=0, keepdims=True
            )
            log_total = log_ref[pl.ds(h, 1), cols]
            dquery = None
            for j in range(i + 1):
                rows = pl.ds(j * block, block)
                s = mm(kv_ref[rows, :HEAD_SIZE], query)
                if i == j:
                    s = s + mask_ref[...]
                probs = jnp.exp(s - log_total)
                dprobs = mm(kv_ref[rows, HEAD_SIZE:], grad)
                dscores = (probs * (dprobs - delta)).astype(BF16)
                dkv[0, rows, :] += mm(dscores, query, 1, 1)
                dkv[1, rows, :] += mm(probs.astype(BF16), grad, 1, 1)
                term = mm(qkv_ref[keys, rows], dscores)
                dquery = term if dquery is None else dquery + term
            dquery = dquery * scale
            a, b = unrotate(dquery[:half], dquery[half:], cos, sin)
            dqkv_ref[pl.ds(base, half), cols] = a.astype(BF16)
            dqkv_ref[pl.ds(base + half, half), cols] = b.astype(BF16)

    @pl.loop(0, 2 * n - 1)
    def _(turn):
        hop = (turn + 1) // 2
        leftward = lax.rem(turn, 2) == 1
        shard = jnp.where(leftward, me - hop, me + hop)

        @pl.when(leftward)
        def _():
            @pl.loop(EARLY, pieces)
            def _(piece):
                gather.receive(hop, piece)

        @pl.when(within(shard, n))
        def _():
            project(shard)
            for i in range(n):

                @pl.when(shard == i)
                def _():
                    attention_rows(i)

        @pl.when(jnp.logical_not(leftward) & within(hop - 1, min(n, pieces) - 1))
        def _():
            sum_piece(hop - 1)

    dkeys = dkv[0].T
    a, b = unrotate(dkeys[:half], dkeys[half:], cos_ref[...], sin_ref[...])
    dqkv_ref[pl.ds(heads * HEAD_SIZE, half), :] = a.astype(BF16)
    dqkv_ref[pl.ds(heads * HEAD_SIZE + half, half), :] = b.astype(BF16)
    dqkv_ref[pl.ds((heads + 1) * HEAD_SIZE, HEAD_SIZE), :] = dkv[1].T.astype(BF16)
    saves = []
    for index, (start, count) in enumerate(tiles(width, 512)):
        cols = slice(start, start + count)
        wgrad[cols, :cols_in] = mm(norm_ref[:, cols], dqkv_ref[...], 0, 1).astype(BF16)
        for shard in range(n):
            term = mm(seq[shard, :, cols], out_ref[:, shard * rows_all : (shard + 1) * rows_all], 0, 1)
            total = term if shard == 0 else total + term
        wgrad[cols, cols_in:] = total.astype(BF16)
        save = pltpu.make_async_copy(
            wgrad.at[pl.ds(start, count), :], wgrad_hbm.at[pl.ds(start, count), :], save_sem.at[index]
        )
        save.start()
        saves.append(save)
    for start, count in tiles(width, 512):
        cols = slice(start, start + count)
        part_ref[:, cols] = mm(dqkv_ref[...], w_ref[cols, :], 0, 1).astype(BF16)
    for piece in range(min(n, pieces) - 1, pieces):
        sum_piece(piece)
    scatter.finish()
    gather.finish(EARLY, pieces)
    for save in saves:
        save.wait()


def attend_back(
    n, mid, kv, log_total, cos, sin, low, hidden, w_mlp, w_out, w_qkv, qkv, out, norm, pieces=4
):
    rows, width = mid.shape
    block = rows
    length = n * rows
    cols_in = qkv.shape[0]
    heads = cols_in // HEAD_SIZE - 2
    units = hidden.shape[2]
    any_spec = pl.BlockSpec(memory_space=pl.ANY)
    wgrad_shape = (width, cols_in + w_out.shape[0])
    return pl.pallas_call(
        functools.partial(attend_back_kernel, n, heads, block, pieces),
        out_shape=(
            jax.ShapeDtypeStruct((rows, width), BF16),
            jax.ShapeDtypeStruct((length, width), BF16),
            jax.ShapeDtypeStruct(wgrad_shape, BF16),
        ),
        in_specs=[VMEM_SPEC] * 5 + [any_spec] * 8,
        out_specs=(VMEM_SPEC,) * 2 + (any_spec,),
        scratch_shapes=[
            pltpu.VMEM((n, rows, width), BF16),
            pltpu.VMEM((n, rows, units), BF16),
            pltpu.VMEM((width, units), BF16),
            pltpu.VMEM((n, rows, width), BF16),
            pltpu.VMEM((n + 1, rows, width), BF16),
            pltpu.VMEM(w_out.shape, BF16),
            pltpu.VMEM(w_qkv.shape, BF16),
            pltpu.VMEM(qkv.shape, BF16),
            pltpu.VMEM(out.shape, BF16),
            pltpu.VMEM(norm.shape, BF16),
            pltpu.VMEM((2, length, HEAD_SIZE), F32),
            pltpu.VMEM((block, block), F32),
            pltpu.VMEM((heads * HEAD_SIZE, length), BF16),
            pltpu.VMEM((cols_in, length), BF16),
            pltpu.VMEM(wgrad_shape, BF16),
        ]
        + sems(n, pieces) * 2
        + [pltpu.SemaphoreType.DMA((9,)), pltpu.SemaphoreType.DMA((len(tiles(width, 512)),))],
        compiler_params=comm_params(3),
        cost_estimate=pl.CostEstimate(
            flops=6 * length * width * wgrad_shape[1],
            bytes_accessed=350 * 1024 * 1024,
            transcendentals=heads * length * length,
        ),
        name="attend_back",
    )(mid, kv, log_total, cos, sin, low, hidden, w_mlp, w_out, w_qkv, qkv, out, norm)


def local(
    n, dp, x, gain_attn, gain_mlp, w_query, w_key, w_value, w_out, w_gate, w_up, w_down, cotangent
):
    rows, _ = x.shape
    length = n * rows
    per = gain_attn.shape[0]
    packed = 2 * per + (-2 * per) % LANES

    mlp_all = lax.all_gather(
        jnp.concatenate([w_gate, w_up, w_down.T], axis=1), "dp", axis=0, tiled=True
    )
    gains = [gain_attn, gain_mlp]
    if packed > 2 * per:
        gains.append(jnp.zeros((packed - 2 * per,), F32))
    cos, sin = tables(length)
    norm_attn, full_attn, full_mlp, qkv, kv, attended, log_total, out_part, w_qkv, w_out_all, near = attend(
        n,
        dp,
        x,
        jnp.concatenate(gains).reshape(1, packed),
        (w_query, w_key.T, w_value.T, w_out),
        cos,
        sin,
        cotangent,
    )
    mid, grad_mid, dgain_mlp, hidden, mlp_grad, grad_low = mlp(
        n, out_part, x, full_mlp, mlp_all, cotangent, near
    )
    mlp_grad = lax.psum_scatter(mlp_grad, "dp", scatter_dimension=0, tiled=True)
    block_output, attn_part, attn_grad = attend_back(
        n, mid, kv, log_total, cos, sin, grad_low, hidden, mlp_all, w_out_all, w_qkv, qkv, attended, norm_attn
    )
    attn_grad = lax.psum_scatter(attn_grad, "dp", scatter_dimension=0, tiled=True)
    input_grad, dgains = sum_input_grad(n, dp, attn_part, x, full_attn, grad_mid, dgain_mlp, packed)
    gate, up, down, query, key, value, out = widen(
        mlp_grad, attn_grad, w_query.shape[1], w_key.shape[1]
    )
    return (
        block_output,
        input_grad,
        dgains[0, :per],
        dgains[0, per : 2 * per],
        query,
        key.T,
        value.T,
        out,
        gate,
        up,
        down,
    )


def solution(mesh):
    rows = P(("dp", "tensor"), None)
    gain = P(("dp", "tensor"))
    into = P("dp", "tensor")
    back = P("tensor", "dp")
    in_specs = (rows, gain, gain, into, into, into, back, into, into, back, rows)
    out_specs = (rows, rows, gain, gain, into, into, into, back, into, into, back)

    def body(*args):
        return local(mesh.shape["tensor"], mesh.shape["dp"], *args)

    return jax.shard_map(body, mesh=mesh, in_specs=in_specs, out_specs=out_specs, check_vma=False)
```

```python
import functools
import math

import jax
import jax.numpy as jnp
from jax import lax
from jax.experimental import pallas as pl
from jax.experimental.pallas import tpu as pltpu
from jax.sharding import PartitionSpec as P


HEAD_SIZE = 64
EPS = 1e-05
ROPE_BASE = 10000.0
NEG_LARGE = -1e30
LANES = 128
MESH = pl.DeviceIdType.MESH
F32 = jnp.float32
BF16 = jnp.bfloat16
VMEM_SPEC = pl.BlockSpec(memory_space=pltpu.VMEM)
EARLY = 0
FAR_DONE = 3


def tables(sequence_length):
    half = HEAD_SIZE // 2
    frequency = ROPE_BASE ** (-(jnp.arange(half, dtype=F32) * 2.0) / HEAD_SIZE)
    angles = frequency[:, None] * jnp.arange(sequence_length, dtype=F32)[None, :]
    return jnp.cos(angles), jnp.sin(angles)


def dims(contract_left, contract_right):
    return (((contract_left,), (contract_right,)), ((), ()))


def mm(left, right, contract_left=1, contract_right=0):
    return lax.dot_general(
        left, right, dims(contract_left, contract_right), preferred_element_type=F32
    )


def piece_rows(piece, size):
    return pl.ds(pl.multiple_of(piece * size, size), size)


class Line:
    def __init__(self, n):
        self.n = n
        self.me = lax.axis_index("tensor")

    def barrier(self):
        barrier = pltpu.get_barrier_semaphore()
        n, me = self.n, self.me

        @pl.when(me > 0)
        def _():
            pl.semaphore_signal(barrier, inc=1, device_id={"tensor": me - 1}, device_id_type=MESH)

        @pl.when(me < n - 1)
        def _():
            pl.semaphore_signal(barrier, inc=1, device_id={"tensor": me + 1}, device_id_type=MESH)

        inner = (me > 0) & (me < n - 1)

        @pl.when(inner)
        def _():
            pl.semaphore_wait(barrier, 2)

        @pl.when(jnp.logical_not(inner))
        def _():
            pl.semaphore_wait(barrier, 1)

    def copy(self, src, dst, send, recv, step):
        return pltpu.make_async_remote_copy(
            src_ref=src,
            dst_ref=dst,
            send_sem=send,
            recv_sem=recv,
            device_id={"tensor": self.me + step},
            device_id_type=MESH,
        )


class Gather:
    def __init__(self, line, buf, send, recv, pieces):
        self.line, self.buf, self.send, self.recv, self.pieces = line, buf, send, recv, pieces
        self.size = buf.shape[1] // pieces

    def message(self, right, hop, piece, shard):
        d = 0 if right else 1
        part = self.buf.at[shard, piece_rows(piece, self.size)]
        return self.line.copy(
            part, part, self.send.at[d, hop - 1, piece], self.recv.at[d, hop - 1, piece], 1 if right else -1
        )

    def start_own(self, piece):
        line = self.line
        me, n = line.me, line.n

        @pl.when(me < n - 1)
        def _():
            self.message(True, 1, piece, me).start()

        @pl.when(me > 0)
        def _():
            self.message(False, 1, piece, me).start()

    def start_hop(self, hop, piece):
        line = self.line
        me, n = line.me, line.n

        @pl.when((me - (hop - 1) >= 0) & (me < n - 1))
        def _():
            self.message(True, hop, piece, me - (hop - 1)).start()

        @pl.when((me + (hop - 1) <= n - 1) & (me > 0))
        def _():
            self.message(False, hop, piece, me + (hop - 1)).start()

    def receive(self, hop, piece, use=None):
        line = self.line
        me, n = line.me, line.n

        @pl.when(me - hop >= 0)
        def _():
            shard = me - hop
            self.message(True, hop, piece, shard).wait_recv()
            if not isinstance(hop, int) or hop < n - 1:

                @pl.when((me < n - 1) & (hop < n - 1))
                def _():
                    self.message(True, hop + 1, piece, shard).start()

            if use is not None:
                use(shard, piece)

        @pl.when(me + hop <= n - 1)
        def _():
            shard = me + hop
            self.message(False, hop, piece, shard).wait_recv()
            if not isinstance(hop, int) or hop < n - 1:

                @pl.when((me > 0) & (hop < n - 1))
                def _():
                    self.message(False, hop + 1, piece, shard).start()

            if use is not None:
                use(shard, piece)

    def finish(self, first_piece=0, end_piece=None):
        line = self.line
        me, n = line.me, line.n

        @pl.loop(first_piece, self.pieces if end_piece is None else end_piece)
        def _(piece):
            for hop in range(1, n):

                @pl.when((me - (hop - 1) >= 0) & (me < n - 1))
                def _():
                    self.message(True, hop, piece, me - (hop - 1)).wait_send()

                @pl.when((me + (hop - 1) <= n - 1) & (me > 0))
                def _():
                    self.message(False, hop, piece, me + (hop - 1)).wait_send()


class Scatter:
    def __init__(self, line, part, buf, send, recv, pieces):
        self.line, self.part, self.buf, self.pieces = line, part, buf, pieces
        self.send, self.recv = send, recv
        self.size = part.shape[1] // pieces

    def rows(self, piece):
        return piece_rows(piece, self.size)

    def outgoing(self, d, target, piece, from_part=False):
        rows, line = self.rows(piece), self.line
        src = (self.part if from_part else self.buf).at[target, rows]
        slot = target
        if d == 1:
            slot = jnp.where(target == line.me - 1, line.n, target)
        return line.copy(
            src,
            self.buf.at[slot, rows],
            self.send.at[d, target, piece],
            self.recv.at[d, target, piece],
            1 if d == 0 else -1,
        )

    def incoming(self, d, target, slot, piece):
        part = self.buf.at[slot, self.rows(piece)]
        return self.line.copy(
            part, part, self.send.at[d, target, piece], self.recv.at[d, target, piece], 1 if d == 0 else -1
        )

    def start_ends(self, piece):
        line = self.line
        me, n = line.me, line.n

        @pl.when(me == 0)
        def _():
            for target in range(n - 1, 0, -1):
                self.outgoing(0, target, piece, True).start()

        @pl.when(me == n - 1)
        def _():
            for target in range(0, n - 1):
                self.outgoing(1, target, piece, True).start()

    def pass_on(self, d, target, piece):
        buf = self.buf
        self.incoming(d, target, target, piece).wait_recv()
        rows = self.rows(piece)
        total = buf[target, rows].astype(F32) + self.part[target, rows].astype(F32)
        buf[target, rows] = total.astype(BF16)
        self.outgoing(d, target, piece).start()

    def passes(self, piece, right, targets, where):
        line = self.line
        me, n = line.me, line.n
        for target in targets:
            held = (me > 0) & (me < target) if right else (me < n - 1) & (me > target)

            @pl.when(where & held)
            def _():
                self.pass_on(0 if right else 1, target, piece)

    def first(self, piece):
        n, left_half = self.line.n, self.line.me < self.line.n // 2
        self.passes(piece, True, (n - 1,), left_half)
        self.passes(piece, False, (0,), jnp.logical_not(left_half))

    def rest(self, piece):
        n, left_half = self.line.n, self.line.me < self.line.n // 2
        right_half = jnp.logical_not(left_half)
        self.passes(piece, True, range(n - 2, 0, -1), left_half)
        self.passes(piece, False, range(1, n - 1), right_half)
        self.passes(piece, False, range(0, n - 1), left_half)
        self.passes(piece, True, range(n - 1, 0, -1), right_half)

    def middle(self, piece):
        self.first(piece)
        self.rest(piece)

    def result(self, piece, store):
        line = self.line
        me, n = line.me, line.n
        rows = self.rows(piece)

        @pl.when(me > 0)
        def _():
            self.incoming(0, me, me, piece).wait_recv()

        @pl.when(me < n - 1)
        def _():
            self.incoming(1, me, n, piece).wait_recv()

        own = self.part[me, rows].astype(F32)

        @pl.when(me == 0)
        def _():
            store(own + self.buf[n, rows].astype(F32))

        @pl.when(me == n - 1)
        def _():
            store(own + self.buf[me, rows].astype(F32))

        @pl.when((me > 0) & (me < n - 1))
        def _():
            store(own + self.buf[me, rows].astype(F32) + self.buf[n, rows].astype(F32))

    def finish(self, ends=True, middles=True):
        line = self.line
        me, n = line.me, line.n
        inner = (me > 0) & (me < n - 1)

        @pl.when((inner & middles) | (jnp.logical_not(inner) & ends))
        def _():
            @pl.loop(0, self.pieces)
            def _(piece):
                for target in range(1, n):

                    @pl.when(me < target)
                    def _():
                        self.outgoing(0, target, piece).wait_send()

                for target in range(0, n - 1):

                    @pl.when(me > target)
                    def _():
                        self.outgoing(1, target, piece).wait_send()


def within(piece, pieces):
    return (piece >= 0) & (piece < pieces)


def sems(n, pieces):
    return [pltpu.SemaphoreType.DMA((2, n, pieces)), pltpu.SemaphoreType.DMA((2, n, pieces))]


def comm_params(collective_id):
    return pltpu.CompilerParams(
        collective_id=collective_id, has_side_effects=True, vmem_limit_bytes=60 * 1024 * 1024
    )


def exchange_all(n, dp, send_row, recv_row, send, recv, start_only=False, wait_only=False):
    devices = n * dp
    me = lax.axis_index("dp") * n + lax.axis_index("tensor")

    def message(offset, peer, source):
        return pltpu.make_async_remote_copy(
            src_ref=send_row(peer),
            dst_ref=recv_row(source),
            send_sem=send.at[offset],
            recv_sem=recv.at[offset],
            device_id={"dp": peer // n, "tensor": peer % n},
            device_id_type=MESH,
        )

    if not wait_only:

        @pl.loop(1, devices)
        def _(offset):
            message(offset, lax.rem(me + offset, devices), me).start()

    if not start_only:

        @pl.loop(1, devices)
        def _(offset):
            copy = message(offset, lax.rem(me + offset, devices), me)
            copy.wait_send()
            copy.wait_recv()


def barrier_all(n, dp):
    devices = n * dp
    me = lax.axis_index("dp") * n + lax.axis_index("tensor")
    barrier = pltpu.get_barrier_semaphore()

    @pl.loop(1, devices)
    def _(offset):
        peer = lax.rem(me + offset, devices)
        pl.semaphore_signal(
            barrier, inc=1, device_id={"dp": peer // n, "tensor": peer % n}, device_id_type=MESH
        )

    pl.semaphore_wait(barrier, devices - 1)


def tiles(extent, size):
    return [(start, min(size, extent - start)) for start in range(0, extent, size)]


def mlp_kernel(
    n, pieces, gain_ref, part_hbm, x_hbm, w_hbm, cot_hbm, near_hbm,
    dgain_ref, mid_hbm, grad_hbm, hid_hbm, wgrad_hbm, low_hbm,
    part_ref, x_ref, mid_ref, grad_ref, w, cot, seq, buf, npart, buf_back, hid, dgate, dup, stage, inv_ref,
    ssend, srecv, gsend, grecv, bsend, brecv, csend, crecv, lsend, lrecv, local_sem, stage_sem, part_sem,
):
    line = Line(n)
    me = line.me
    rows_all, width = part_ref.shape[1:]

    def part_load(piece):
        rows = piece_rows(piece, rows_all // pieces)
        return pltpu.make_async_copy(part_hbm.at[:, rows], part_ref.at[:, rows], part_sem.at[0, piece])

    def piece_save(which, ref, hbm, piece):
        rows = piece_rows(piece, rows_all // pieces)
        return pltpu.make_async_copy(ref.at[rows], hbm.at[rows], part_sem.at[which, piece])

    x_load = pltpu.make_async_copy(x_hbm, x_ref, local_sem.at[3])
    for piece in range(pieces):
        part_load(piece).start()
    x_load.start()

    units = hid.shape[2]
    weight_load = pltpu.make_async_copy(w_hbm, w, local_sem.at[0])
    own_load = pltpu.make_async_copy(cot_hbm, cot.at[me], local_sem.at[1])
    inner = (me > 0) & (me < n - 1)

    def near_load(shard, count):
        rows = pl.ds(0, count)
        return pltpu.make_async_copy(near_hbm.at[shard, rows], cot.at[shard, rows], local_sem.at[5 + shard])

    def each_near(act):
        for shard in range(n):
            here = (me != shard) & (inner | (me - shard == 1) | (shard - me == 1))

            @pl.when(here)
            def _():
                act(near_load(shard, rows_all))

            if n == 4:

                @pl.when(jnp.logical_not(inner) & ((me - shard == 2) | (shard - me == 2)))
                def _():
                    act(near_load(shard, rows_all // pieces * FAR_DONE))

    each_near(lambda copy: copy.start())
    own_load.start()
    weight_load.start()
    line.barrier()
    scatter = Scatter(line, part_ref, buf, ssend, srecv, pieces)
    gather = Gather(line, seq, gsend, grecv, pieces)
    scatter_back = Scatter(line, npart, buf_back, bsend, brecv, pieces)
    cot_gather = Gather(line, cot, csend, crecv, pieces)
    low_gather = Gather(line, buf, lsend, lrecv, pieces)
    size = scatter.size
    part_load(0).wait()
    scatter.start_ends(0)
    for piece in range(1, pieces):
        part_load(piece).wait()
    x_load.wait()
    dgain_ref[...] = jnp.zeros_like(dgain_ref)

    each_near(lambda copy: copy.wait())

    def still_far(hop, piece):
        return (piece >= FAR_DONE) if hop == 2 and n == 4 else (piece >= 0)

    def each_far(piece, act):
        for hop in range(2, n):

            @pl.when((me == n - 2) & still_far(hop, piece))
            def _():
                act(True, hop, me - (hop - 1))

            @pl.when((me == 1) & still_far(hop, piece))
            def _():
                act(False, hop, me + (hop - 1))

    def far_start(piece):
        each_far(piece, lambda right, hop, shard: cot_gather.message(right, hop, piece, shard).start())

    def far_sent(piece):
        each_far(piece, lambda right, hop, shard: cot_gather.message(right, hop, piece, shard).wait_send())

    def far_arrived(piece):
        for hop in range(2, n):

            @pl.when((me == n - 1) & still_far(hop, piece))
            def _():
                cot_gather.message(True, hop, piece, me - hop).wait_recv()

            @pl.when((me == 0) & still_far(hop, piece))
            def _():
                cot_gather.message(False, hop, piece, me + hop).wait_recv()

    for piece in range(min(3, pieces)):
        far_start(jnp.int32(piece))

    def norm(piece):
        rows = scatter.rows(piece)

        def store(total):
            mid_ref[rows, :] = x_ref[rows, :].astype(F32) + total

        scatter.result(piece, store)
        mid = mid_ref[rows, :]
        inv = lax.rsqrt(jnp.mean(mid * mid, axis=1, keepdims=True) + EPS)
        inv_ref[rows, :] = jnp.broadcast_to(inv, (size, LANES))
        seq[me, rows, :] = (mid * inv * gain_ref[...]).astype(BF16)
        piece_save(1, mid_ref, mid_hbm, piece).start()

    def back(piece):
        rows = scatter.rows(piece)

        def store(total):
            grad_ref[rows, :] = total

        scatter_back.result(piece, store)
        grad = grad_ref[rows, :]
        mid = mid_ref[rows, :]
        inv = inv_ref[rows, 0:1]
        dgain_ref[...] += jnp.sum(grad * mid * inv, axis=0, keepdims=True)
        scaled = grad * gain_ref[...]
        mean = jnp.mean(scaled * mid, axis=1, keepdims=True)
        out = cot[me, rows, :].astype(F32) + inv * (scaled - mid * (inv * inv * mean))
        grad_ref[rows, :] = out
        buf[me, rows, :] = out.astype(BF16)
        piece_save(2, grad_ref, grad_hbm, piece).start()

    def flat(ref, piece):
        value = ref[:, scatter.rows(piece), :]
        return value.reshape(n * size, value.shape[2])

    def feed(piece):
        rows = scatter.rows(piece)
        for start, count in tiles(units, 512):
            x = flat(seq, piece)
            gate = mm(x, w[:, start : start + count])
            up = mm(x, w[:, units + start : units + start + count])
            dhidden = mm(flat(cot, piece), w[:, 2 * units + start : 2 * units + start + count])
            sigmoid = jax.nn.sigmoid(gate)
            act = gate * sigmoid
            cols = slice(start, start + count)
            shape = (n, size, count)
            hid[:, rows, cols] = (act * up).astype(BF16).reshape(shape)
            dup[:, rows, cols] = (dhidden * act).astype(BF16).reshape(shape)
            dgate[:, rows, cols] = (
                (dhidden * up * sigmoid * (1.0 + gate * (1.0 - sigmoid))).astype(BF16).reshape(shape)
            )
        for start, count in tiles(width, 512):
            cols = slice(start, start + count)
            total = mm(flat(dgate, piece), w[cols, :units], 1, 1)
            total += mm(flat(dup, piece), w[cols, units : 2 * units], 1, 1)
            npart[:, rows, cols] = total.astype(BF16).reshape(n, size, count)

    step_rows = min(LANES, width)
    count = width // step_rows

    def save(index, slot):
        return pltpu.make_async_copy(
            stage.at[slot],
            wgrad_hbm.at[pl.ds(pl.multiple_of(index * step_rows, step_rows), step_rows), :],
            stage_sem.at[slot],
        )

    def weight_grads(events):
        @pl.loop(0, count)
        def _(index):
            for at, event in events:

                @pl.when(index == at)
                def _():
                    event()

            slot = lax.rem(index, 2)
            cols = pl.ds(pl.multiple_of(index * step_rows, step_rows), step_rows)

            @pl.when(index >= 2)
            def _():
                save(index - 2, slot).wait()

            x = seq[:, :, cols].reshape(n * rows_all, step_rows)
            g = cot[:, :, cols].reshape(n * rows_all, step_rows)
            for at, left, right in ((0, x, dgate), (1, x, dup), (2, g, hid)):
                value = right[...].reshape(n * rows_all, units)
                stage[slot, :, at * units : (at + 1) * units] = mm(left, value, 0, 0).astype(BF16)
            save(index, slot).start()

    hid_save = pltpu.make_async_copy(hid, hid_hbm, local_sem.at[2])

    @pl.loop(0, pieces + n - 1)
    def _(step):
        first = step < pieces

        @pl.when(first)
        def _():
            @pl.when(step + 1 < pieces)
            def _():
                scatter.start_ends(step + 1)

            scatter.middle(step)

            @pl.when(step + 3 < pieces)
            def _():
                far_start(step + 3)

        for hop in range(1, n):
            piece = step - hop

            @pl.when(within(piece, pieces))
            def _():
                gather.receive(hop, piece)

        @pl.when(first)
        def _():
            norm(step)
            gather.start_own(step)

        ready = step - (n - 1)

        @pl.when(ready == 0)
        def _():
            own_load.wait()
            weight_load.wait()

        @pl.when(ready == 1)
        def _():
            scatter.finish(ends=False)

        for hop in range(1, n):
            piece = ready - 1 - hop

            @pl.when(within(piece, EARLY))
            def _():
                low_gather.receive(hop, piece)

        @pl.when(ready >= 1)
        def _():
            scatter_back.middle(ready - 1)

        @pl.when(ready >= 0)
        def _():
            far_arrived(ready)
            feed(ready)
            scatter_back.start_ends(ready)

        @pl.when(ready >= 1)
        def _():
            back(ready - 1)

            @pl.when(ready - 1 < EARLY)
            def _():
                low_gather.start_own(ready - 1)

    hid_save.start()
    last = pieces - 1

    def low_arrivals(step):
        for hop in range(1, n):
            piece = step - hop
            if 0 <= piece < EARLY:
                low_gather.receive(hop, piece)

    late = [
        (lambda step: lambda: low_arrivals(step))(step) for step in range(pieces - 1, pieces + n - 2)
    ]
    events = [
        (count // 4, lambda: scatter_back.first(last)),
        (count * 5 // 8, lambda: scatter_back.rest(last)),
    ]
    if EARLY:
        events += [(count * (2 * i + 1) // (2 * len(late)), event) for i, event in enumerate(late)]
    weight_grads(events)
    back(last)
    own_rows, early_rows = pl.ds(EARLY * size, rows_all - EARLY * size), pl.ds(0, EARLY * size)
    low_saves = [
        pltpu.make_async_copy(buf.at[me, own_rows], low_hbm.at[me, own_rows], local_sem.at[4])
    ]
    if EARLY:
        low_saves.append(
            pltpu.make_async_copy(
                buf.at[pl.ds(0, n), early_rows], low_hbm.at[:, early_rows], local_sem.at[0]
            )
        )
    for save_low in low_saves:
        save_low.start()
    scatter.finish(middles=False)
    gather.finish()
    scatter_back.finish()
    low_gather.finish(0, EARLY)

    @pl.loop(0, pieces)
    def _(piece):
        far_sent(piece)
        piece_save(1, mid_ref, mid_hbm, piece).wait()
        piece_save(2, grad_ref, grad_hbm, piece).wait()

    for save_low in low_saves:
        save_low.wait()
    hid_save.wait()
    for index in range(max(count - 2, 0), count):
        save(index, index % 2).wait()


def mlp(n, part, x, gain, weights, cotangent, near, pieces=4):
    rows, width = x.shape
    units = weights.shape[1] // 3
    any_spec = pl.BlockSpec(memory_space=pl.ANY)
    return pl.pallas_call(
        functools.partial(mlp_kernel, n, pieces),
        out_shape=(
            jax.ShapeDtypeStruct((1, width), F32),
            jax.ShapeDtypeStruct((rows, width), F32),
            jax.ShapeDtypeStruct((rows, width), F32),
            jax.ShapeDtypeStruct((n, rows, units), BF16),
            jax.ShapeDtypeStruct((width, 3 * units), BF16),
            jax.ShapeDtypeStruct((n, rows, width), BF16),
        ),
        in_specs=[VMEM_SPEC] + [any_spec] * 5,
        out_specs=(VMEM_SPEC,) + (any_spec,) * 5,
        scratch_shapes=[
            pltpu.VMEM((n, rows, width), BF16),
            pltpu.VMEM((rows, width), BF16),
            pltpu.VMEM((rows, width), F32),
            pltpu.VMEM((rows, width), F32),
            pltpu.VMEM((width, 3 * units), BF16),
            pltpu.VMEM((n, rows, width), BF16),
            pltpu.VMEM((n, rows, width), BF16),
            pltpu.VMEM((n + 1, rows, width), BF16),
            pltpu.VMEM((n, rows, width), BF16),
            pltpu.VMEM((n + 1, rows, width), BF16),
            pltpu.VMEM((n, rows, units), BF16),
            pltpu.VMEM((n, rows, units), BF16),
            pltpu.VMEM((n, rows, units), BF16),
            pltpu.VMEM((2, min(LANES, width), 3 * units), BF16),
            pltpu.VMEM((rows, LANES), F32),
        ]
        + sems(n, pieces) * 5
        + [pltpu.SemaphoreType.DMA((5 + n,)), pltpu.SemaphoreType.DMA((2,)), pltpu.SemaphoreType.DMA((3, pieces))],
        compiler_params=pltpu.CompilerParams(
            collective_id=2, has_side_effects=True, vmem_limit_bytes=67043328
        ),
        cost_estimate=pl.CostEstimate(
            flops=18 * n * rows * width * units, bytes_accessed=500 * 1024 * 1024, transcendentals=0
        ),
        name="mlp",
    )(gain, part.reshape(n, rows, width), x, weights, cotangent, near)


def last_kernel(
    n, dp, pieces, gain_ref, dgain_mlp_ref, part_hbm, x_hbm, grad_mid_hbm, out_ref, gains_ref,
    part_ref, x_ref, grad_mid_ref, total_ref, dgain_ref, packed, held, buf, ssend, srecv, gsend, grecv, load_sem,
):
    def part_load(piece):
        rows = piece_rows(piece, part_ref.shape[1] // pieces)
        return pltpu.make_async_copy(part_hbm.at[:, rows], part_ref.at[:, rows], load_sem.at[2 + piece])

    others = [
        pltpu.make_async_copy(x_hbm, x_ref, load_sem.at[0]),
        pltpu.make_async_copy(grad_mid_hbm, grad_mid_ref, load_sem.at[1]),
    ]
    for piece in range(pieces):
        part_load(piece).start()
    for load in others:
        load.start()
    line = Line(n)
    all_me = lax.axis_index("dp") * n + line.me
    barrier_all(n, dp)
    scatter = Scatter(line, part_ref, buf, ssend, srecv, pieces)
    part_load(0).wait()
    scatter.start_ends(0)
    for piece in range(1, pieces):
        part_load(piece).wait()
    for load in others:
        load.wait()
    dgain_ref[...] = jnp.zeros_like(dgain_ref)
    packed[...] = jnp.zeros_like(packed)

    @pl.loop(0, pieces)
    def _(piece):
        @pl.when(piece + 1 < pieces)
        def _():
            scatter.start_ends(piece + 1)

        scatter.middle(piece)
        rows = scatter.rows(piece)

        def store(total):
            total_ref[...] = total

        scatter.result(piece, store)
        grad = total_ref[...]
        x = x_ref[rows, :].astype(F32)
        inv = lax.rsqrt(jnp.mean(x * x, axis=1, keepdims=True) + EPS)
        dgain_ref[...] += jnp.sum(grad * x * inv, axis=0, keepdims=True)
        scaled = grad * gain_ref[...]
        mean = jnp.mean(scaled * x, axis=1, keepdims=True)
        out = grad_mid_ref[rows, :] + inv * (scaled - x * (inv * inv * mean))
        out_ref[rows, :] = out.astype(BF16)

    per = x_ref.shape[1] // (n * dp)
    for device in range(n * dp):
        cols = slice(device * per, (device + 1) * per)
        packed[device, :, :per] = dgain_ref[:, cols]
        packed[device, :, per : 2 * per] = dgain_mlp_ref[:, cols]
    held[all_me] = packed[all_me]
    exchange_all(n, dp, lambda peer: packed.at[peer], lambda source: held.at[source], gsend, grecv)
    gains_ref[...] = jnp.sum(held[...], axis=0)
    scatter.finish()


def sum_input_grad(n, dp, part, x, gain, grad_mid, dgain_mlp, packed, pieces=8):
    rows, width = x.shape
    any_spec = pl.BlockSpec(memory_space=pl.ANY)
    return pl.pallas_call(
        functools.partial(last_kernel, n, dp, pieces),
        out_shape=(
            jax.ShapeDtypeStruct((rows, width), BF16),
            jax.ShapeDtypeStruct((1, packed), F32),
        ),
        in_specs=[VMEM_SPEC] * 2 + [any_spec] * 3,
        out_specs=(VMEM_SPEC,) * 2,
        scratch_shapes=[
            pltpu.VMEM((n, rows, width), BF16),
            pltpu.VMEM((rows, width), BF16),
            pltpu.VMEM((rows, width), F32),
            pltpu.VMEM((rows // pieces, width), F32),
            pltpu.VMEM((1, width), F32),
            pltpu.VMEM((n * dp, 1, packed), F32),
            pltpu.VMEM((n * dp, 1, packed), F32),
            pltpu.VMEM((n + 1, rows, width), BF16),
        ]
        + sems(n, pieces)
        + [pltpu.SemaphoreType.DMA((n * dp,)), pltpu.SemaphoreType.DMA((n * dp,))]
        + [pltpu.SemaphoreType.DMA((2 + pieces,))],
        compiler_params=comm_params(4),
        cost_estimate=pl.CostEstimate(flops=0, bytes_accessed=250 * 1024 * 1024, transcendentals=0),
        name="sum_input_grad",
    )(gain, dgain_mlp, part.reshape(n, rows, width), x, grad_mid)


def widen_kernel(
    mlp_ref, attn_ref, gains_ref, rows_ref, input_ref,
    gate_ref, up_ref, down_ref, query_ref, key_ref, value_ref, out_ref,
    attn_gain_ref, mlp_gain_ref, rows_out_ref, input_out_ref,
):
    units = gate_ref.shape[1]
    per = attn_gain_ref.shape[1]
    attn_gain_ref[...] = gains_ref[:, :per]
    mlp_gain_ref[...] = gains_ref[:, per : 2 * per]
    rows_out_ref[...] = rows_ref[...]
    input_out_ref[...] = input_ref[...]
    gate_ref[...] = mlp_ref[:, :units].astype(F32)
    up_ref[...] = mlp_ref[:, units : 2 * units].astype(F32)
    down_ref[...] = mlp_ref[:, 2 * units :].astype(F32).T
    q_cols, k_cols = query_ref.shape[1], key_ref.shape[0]
    query_ref[...] = attn_ref[:, :q_cols].astype(F32)
    key_ref[...] = attn_ref[:, q_cols : q_cols + k_cols].astype(F32).T
    value_ref[...] = attn_ref[:, q_cols + k_cols : q_cols + 2 * k_cols].astype(F32).T
    out_ref[...] = attn_ref[:, q_cols + 2 * k_cols :].astype(F32).T


def widen(mlp_grad, attn_grad, gains, rows_out, input_out, per, q_cols, k_cols):
    rows, units = mlp_grad.shape[0], mlp_grad.shape[1] // 3
    shapes = [(rows, units)] * 2 + [(units, rows), (rows, q_cols)] + [(k_cols, rows)] * 2 + [(q_cols, rows)]
    return pl.pallas_call(
        widen_kernel,
        out_shape=tuple(jax.ShapeDtypeStruct(shape, F32) for shape in shapes + [(1, per)] * 2)
        + (jax.ShapeDtypeStruct(rows_out.shape, BF16),) * 2,
        in_specs=[VMEM_SPEC] * 5,
        out_specs=(VMEM_SPEC,) * 11,
        compiler_params=pltpu.CompilerParams(vmem_limit_bytes=56 * 1024 * 1024),
        name="widen",
    )(mlp_grad, attn_grad, gains, rows_out, input_out)


def rotate(half_a, half_b, cos, sin):
    return half_a * cos - half_b * sin, half_b * cos + half_a * sin


def unrotate(half_a, half_b, cos, sin):
    return half_a * cos + half_b * sin, half_b * cos - half_a * sin


def mask_block(size):
    key = lax.broadcasted_iota(jnp.int32, (size, size), 0)
    row = lax.broadcasted_iota(jnp.int32, (size, size), 1)
    return jnp.where(key <= row, 0.0, NEG_LARGE)


def attend_kernel(
    n, dp, heads, block, pieces, x_ref, gain_ref, cos_ref, sin_ref, cot_hbm, wq_hbm, wk_hbm, wv_hbm, wo_hbm,
    attn_gain_ref, mlp_gain_ref, kv_ref, out_ref, log_ref, norm_hbm, qkv_hbm, part_hbm, w_out_hbm, wo_out_hbm, near_hbm,
    norm_ref, qkv_ref, part_ref, w_ref, wo_ref, seq, act_ref, mask_ref, gains, wq, wk, wv, wo, send, recv, gsend, grecv, wsend, wrecv, own_sem, csend, crecv, fsend, frecv, save_sem,
):
    half = HEAD_SIZE // 2
    rows_all, width = x_ref.shape
    length = n * rows_all
    line = Line(n)
    me = line.me
    mine = lax.axis_index("dp")
    barrier_all(n, dp)
    seq[me] = x_ref[...]
    gains[mine * n + me] = gain_ref[...]
    gather = Gather(line, seq, send, recv, pieces)

    @pl.loop(0, pieces)
    def _(piece):
        gather.start_own(piece)

    def gain_rows(**kind):
        exchange_all(
            n, dp, lambda peer: gain_ref, lambda source: gains.at[source], gsend, grecv, **kind
        )

    gain_rows(start_only=True)

    shards = ((wq_hbm, wq), (wk_hbm, wk), (wv_hbm, wv), (wo_hbm, wo))
    own = [pltpu.make_async_copy(src, dst.at[mine], own_sem.at[i]) for i, (src, dst) in enumerate(shards)]
    pair = mine + 1 - 2 * lax.rem(mine, 2)

    def even_copy(i, offset):
        src, dst = shards[i]
        return pltpu.make_async_remote_copy(
            src_ref=src,
            dst_ref=dst.at[mine],
            send_sem=wsend.at[0, i, offset],
            recv_sem=wrecv.at[0, i, offset],
            device_id={"dp": lax.rem(mine + 2 * offset, dp)},
            device_id_type=MESH,
        )

    def pair_copy(i, offset):
        dst = shards[i][1].at[lax.rem(mine + 2 * offset, dp)]
        return pltpu.make_async_remote_copy(
            src_ref=dst,
            dst_ref=dst,
            send_sem=wsend.at[1, i, offset],
            recv_sem=wrecv.at[1, i, offset],
            device_id={"dp": pair},
            device_id_type=MESH,
        )

    for i in range(4):
        own[i].start()

    @pl.loop(1, dp // 2)
    def _(offset):
        for i in range(4):
            even_copy(i, offset).start()

    def cot_copy(right, hop):
        d = 0 if right else 1
        shard = me - (hop - 1) if right else me + (hop - 1)
        src = cot_hbm if hop == 1 else near_hbm.at[shard]
        return line.copy(src, near_hbm.at[shard], csend.at[d, hop - 1], crecv.at[d, hop - 1], 1 if right else -1)

    inner = (me > 0) & (me < n - 1)

    @pl.when(me == 0)
    def _():
        cot_copy(True, 1).start()

    @pl.when(me == n - 1)
    def _():
        cot_copy(False, 1).start()

    q_cols, k_cols = wq.shape[2], wk.shape[1]
    w_rows, w_cols = wq.shape[1], wo.shape[2]

    saves = [
        pltpu.make_async_copy(src, dst, save_sem.at[i])
        for i, (src, dst) in enumerate(
            ((w_ref, w_out_hbm), (wo_ref, wo_out_hbm), (norm_ref, norm_hbm), (qkv_ref, qkv_hbm))
        )
    ]

    def project(shard):
        x = seq[shard].astype(F32)
        inv = lax.rsqrt(jnp.mean(x * x, axis=1, keepdims=True) + EPS)
        norm = (x * inv * attn_gain_ref[...]).astype(BF16)
        rows = piece_rows(shard, rows_all)
        norm_ref[rows, :] = norm
        act_ref[:, rows] = mm(w_ref[...], norm, 0, 1)

    def project_at(hop):
        @pl.when(me - hop >= 0)
        def _():
            project(me - hop)

        @pl.when(me + hop <= n - 1)
        def _():
            project(me + hop)

    def prepare():
        gain_rows(wait_only=True)
        per = width // (n * dp)
        for device in range(n * dp):
            attn_gain_ref[:, device * per : (device + 1) * per] = gains[device, :, :per]
            mlp_gain_ref[:, device * per : (device + 1) * per] = gains[device, :, per : 2 * per]

        @pl.loop(0, dp // 2)
        def _(offset):
            for i in range(4):
                pair_copy(i, offset).wait_recv()

        for d in range(dp):
            rows = slice(d * w_rows, (d + 1) * w_rows)
            w_ref[rows, :q_cols] = wq[d]
            w_ref[rows, q_cols : q_cols + k_cols] = wk[d].T
            w_ref[rows, q_cols + k_cols :] = wv[d].T
            wo_ref[:, d * w_cols : (d + 1) * w_cols] = wo[d]
        saves[0].start()
        saves[1].start()
        project(me)

    def start_pair():
        for i in range(4):
            own[i].wait()

        @pl.loop(1, dp // 2)
        def _(offset):
            for i in range(4):
                even_copy(i, offset).wait_recv()

        @pl.loop(0, dp // 2)
        def _(offset):
            for i in range(4):
                pair_copy(i, offset).start()

    def arrived(d, hop, shard):
        cot_copy_in(
            line, near_hbm, shard, crecv.at[d, hop - 1], csend.at[d, hop - 1], 1 if d == 1 else -1
        ).wait_recv()

    ready = min(2, n - 1)
    for hop in range(1, n):

        @pl.loop(0, pieces)
        def _(piece):
            gather.receive(hop, piece)
            if hop == ready:

                @pl.when(piece == pieces // 2)
                def _():
                    start_pair()

        @pl.when((me == hop) & (me < n - 1))
        def _():
            cot_copy(True, 1).start()

        @pl.when((n - 1 - me == hop) & (me > 0))
        def _():
            cot_copy(False, 1).start()

        if hop == ready:
            if n == 4:

                @pl.when(me == 1)
                def _():
                    cot_copy_in(line, near_hbm, me - 1, crecv.at[0, 0], csend.at[0, 0], -1).wait_recv()
                    cot_copy(True, 2).start()

                @pl.when(me == 2)
                def _():
                    cot_copy_in(line, near_hbm, me + 1, crecv.at[1, 0], csend.at[1, 0], 1).wait_recv()
                    cot_copy(False, 2).start()

            prepare()
            for earlier in range(1, hop + 1):
                project_at(earlier)
        elif hop > ready:
            project_at(hop)

    def far_copy(right, shard):
        part = near_hbm.at[shard, pl.ds(0, rows_all // pieces * FAR_DONE)]
        d = 0 if right else 1
        return line.copy(part, part, fsend.at[d], frecv.at[d], jnp.where(inner, 1 if right else -1, jnp.where(me == 0, 1, -1)))

    if n == 4:

        @pl.when(me == 1)
        def _():
            arrived(1, 1, me + 1)
            far_copy(False, me + 1).start()

        @pl.when(me == 2)
        def _():
            arrived(0, 1, me - 1)
            far_copy(True, me - 1).start()

    cos, sin = cos_ref[...], sin_ref[...]

    scale = 1.0 / math.sqrt(HEAD_SIZE)

    @pl.loop(0, heads + 1)
    def _(h):
        base = pl.multiple_of(h * HEAD_SIZE, HEAD_SIZE)
        a, b = rotate(act_ref[pl.ds(base, half), :], act_ref[pl.ds(base + half, half), :], cos, sin)
        factor = jnp.where(h < heads, scale, 1.0)
        a, b = a * factor, b * factor
        qkv_ref[pl.ds(base, half), :] = a.astype(BF16)
        qkv_ref[pl.ds(base + half, half), :] = b.astype(BF16)

    values = pl.ds((heads + 1) * HEAD_SIZE, HEAD_SIZE)
    qkv_ref[values, :] = act_ref[values, :].astype(BF16)
    saves[2].start()
    saves[3].start()
    mask_ref[...] = mask_block(block)
    kv_ref[...] = qkv_ref[pl.ds(heads * HEAD_SIZE, 2 * HEAD_SIZE), :].T

    @pl.loop(0, heads)
    def _(h):
        base = pl.multiple_of(h * HEAD_SIZE, HEAD_SIZE)
        for i in range(length // block):
            cols = pl.ds(i * block, block)
            query = qkv_ref[pl.ds(base, HEAD_SIZE), cols]
            scores = []
            peak = None
            for j in range(i + 1):
                s = mm(kv_ref[pl.ds(j * block, block), :HEAD_SIZE], query)
                if i == j:
                    s = s + mask_ref[...]
                top = jnp.max(s, axis=0, keepdims=True)
                peak = top if peak is None else jnp.maximum(peak, top)
                scores.append(s)
            weights = [jnp.exp(s - peak) for s in scores]
            total = sum(jnp.sum(w, axis=0, keepdims=True) for w in weights)
            log_ref[pl.ds(h, 1), cols] = peak + jnp.log(total)
            inverse = 1.0 / total
            mixed = None
            for j in range(i + 1):
                w = (weights[j] * inverse).astype(BF16)
                v = qkv_ref[values, pl.ds(j * block, block)]
                term = mm(v, w)
                mixed = term if mixed is None else mixed + term
            out_ref[pl.ds(base, HEAD_SIZE), cols] = mixed.astype(BF16)

    for start, count in tiles(width, 512):
        cols = slice(start, start + count)
        part_ref[:, cols] = mm(out_ref[...], wo_ref[:, cols], 0, 0).astype(BF16)
        save = pltpu.make_async_copy(
            part_ref.at[:, pl.ds(start, count)], part_hbm.at[:, pl.ds(start, count)], save_sem.at[len(saves)]
        )
        save.start()
        saves.append(save)

    gather.finish()
    for save in saves:
        save.wait()

    @pl.loop(1, dp // 2)
    def _(offset):
        for i in range(4):
            even_copy(i, offset).wait_send()

    @pl.loop(0, dp // 2)
    def _(offset):
        for i in range(4):
            pair_copy(i, offset).wait_send()

    if n == 4:

        @pl.when(me == 1)
        def _():
            arrived(1, 2, me + 2)
            cot_copy(True, 2).wait_send()
            far_copy(False, me + 1).wait_send()

        @pl.when(me == 2)
        def _():
            arrived(0, 2, me - 2)
            cot_copy(False, 2).wait_send()
            far_copy(True, me - 1).wait_send()

        @pl.when(me == 0)
        def _():
            far_copy(False, me + 2).wait_recv()

        @pl.when(me == n - 1)
        def _():
            far_copy(True, me - 2).wait_recv()

    else:

        @pl.when(inner)
        def _():
            arrived(0, 1, me - 1)
            arrived(1, 1, me + 1)

    @pl.when(me == 0)
    def _():
        arrived(1, 1, me + 1)

    @pl.when(me == n - 1)
    def _():
        arrived(0, 1, me - 1)

    @pl.when(me < n - 1)
    def _():
        cot_copy(True, 1).wait_send()

    @pl.when(me > 0)
    def _():
        cot_copy(False, 1).wait_send()


def cot_copy_in(line, near_hbm, shard, recv, send, step):
    part = near_hbm.at[shard]
    return line.copy(part, part, send, recv, step)


def attend(n, dp, x, gains, weights, cos, sin, cotangent, block=256, pieces=4):
    assert n <= 4 and dp % 2 == 0
    rows, width = x.shape
    length = n * rows
    q_cols, k_cols = weights[0].shape[1], weights[1].shape[0]
    cols_in = q_cols + 2 * k_cols
    heads = cols_in // HEAD_SIZE - 2
    any_spec = pl.BlockSpec(memory_space=pl.ANY)
    dma = pltpu.SemaphoreType.DMA
    return pl.pallas_call(
        functools.partial(attend_kernel, n, dp, heads, block, pieces),
        out_shape=(
            jax.ShapeDtypeStruct((1, width), F32),
            jax.ShapeDtypeStruct((1, width), F32),
            jax.ShapeDtypeStruct((length, 2 * HEAD_SIZE), BF16),
            jax.ShapeDtypeStruct((heads * HEAD_SIZE, length), BF16),
            jax.ShapeDtypeStruct((heads, length), F32),
            jax.ShapeDtypeStruct((length, width), BF16),
            jax.ShapeDtypeStruct((cols_in, length), BF16),
            jax.ShapeDtypeStruct((length, width), BF16),
            jax.ShapeDtypeStruct((width, cols_in), BF16),
            jax.ShapeDtypeStruct((q_cols, width), BF16),
            jax.ShapeDtypeStruct((n,) + cotangent.shape, BF16),
        ),
        in_specs=[VMEM_SPEC] * 4 + [any_spec] * 5,
        out_specs=(VMEM_SPEC,) * 5 + (any_spec,) * 6,
        scratch_shapes=[
            pltpu.VMEM((length, width), BF16),
            pltpu.VMEM((cols_in, length), BF16),
            pltpu.VMEM((length, width), BF16),
            pltpu.VMEM((width, cols_in), BF16),
            pltpu.VMEM((q_cols, width), BF16),
            pltpu.VMEM((n, rows, width), BF16),
            pltpu.VMEM((cols_in, length), F32),
            pltpu.VMEM((block, block), F32),
            pltpu.VMEM((n * dp, 1, gains.shape[1]), F32),
        ]
        + [pltpu.VMEM((dp,) + w.shape, BF16) for w in weights]
        + sems(n, pieces)
        + [dma((n * dp,)), dma((n * dp,)), dma((2, 4, dp // 2)), dma((2, 4, dp // 2)), dma((4,))]
        + [dma((2, 2)), dma((2, 2)), dma((2,)), dma((2,)), dma((4 + len(tiles(width, 512)),))],
        compiler_params=comm_params(1),
        cost_estimate=pl.CostEstimate(
            flops=2 * length * width * (cols_in + q_cols),
            bytes_accessed=350 * 1024 * 1024,
            transcendentals=heads * length * length,
        ),
        name="attend",
    )(x, gains, cos, sin, cotangent, *weights)


def attend_back_kernel(
    n, heads, block, pieces, kv_ref, log_ref, cos_ref, sin_ref,
    mid_hbm, low_hbm, hid_hbm, w_mlp_hbm, wo_hbm, w_hbm, qkv_hbm, out_hbm, norm_hbm,
    rows_ref, part_hbm, wgrad_hbm,
    mid_ref, part_ref, seq, hid, w_down, down_ref, buf, wo_ref, w_ref, qkv_ref, out_ref, norm_ref,
    dkv, mask_ref, grad_ref, dqkv_ref, wgrad, ssend, srecv, gsend, grecv, load_sem, save_sem,
):
    half = HEAD_SIZE // 2
    rows_all, width = mid_ref.shape
    units = hid.shape[2]
    cols_in = qkv_ref.shape[0]
    scale = 1.0 / math.sqrt(HEAD_SIZE)
    me = lax.axis_index("tensor")
    size = rows_all // pieces
    own_rows, early_rows = pl.ds(EARLY * size, rows_all - EARLY * size), pl.ds(0, EARLY * size)
    pairs = (
        (low_hbm.at[me, own_rows], seq.at[me, own_rows]),
        (hid_hbm, hid),
        (w_mlp_hbm.at[:, pl.ds(2 * units, units)], w_down),
        (wo_hbm, wo_ref),
        (qkv_hbm, qkv_ref),
        (out_hbm, out_ref),
        (w_hbm, w_ref),
        (norm_hbm, norm_ref),
        (mid_hbm, mid_ref),
    )
    if EARLY:
        pairs += ((low_hbm.at[:, early_rows], seq.at[:, early_rows]),)
    loads = [pltpu.make_async_copy(src, dst, load_sem.at[i]) for i, (src, dst) in enumerate(pairs)]
    for load in loads:
        load.start()
    line = Line(n)
    line.barrier()
    scatter = Scatter(line, down_ref, buf, ssend, srecv, pieces)
    gather = Gather(line, seq, gsend, grecv, pieces)
    loads[0].wait()

    @pl.loop(EARLY, pieces)
    def _(piece):
        gather.start_own(piece)

    dkv[...] = jnp.zeros_like(dkv)
    mask_ref[...] = mask_block(block)
    keys = pl.ds(heads * HEAD_SIZE, HEAD_SIZE)

    def project(shard):
        grad_ref[:, piece_rows(shard, rows_all)] = mm(wo_ref[...], seq[shard], 1, 1).astype(BF16)

    def start_sums():
        loads[1].wait()
        loads[2].wait()

        @pl.loop(0, pieces)
        def _(piece):
            rows = scatter.rows(piece)
            for start, count in tiles(width, 512):
                cols = slice(start, start + count)
                value = hid[:, rows, :].reshape(n * scatter.size, units)
                value = mm(value, w_down[cols, :], 1, 1).astype(BF16)
                down_ref[:, rows, cols] = value.reshape(n, scatter.size, count)
            scatter.start_ends(piece)

    def sum_piece(piece):
        scatter.middle(piece)
        rows = scatter.rows(piece)

        def store(total):
            rows_ref[rows, :] = (mid_ref[rows, :] + total).astype(BF16)

        scatter.result(piece, store)

    start_sums()
    for load in loads[3:]:
        load.wait()

    def attention_rows(i):
        cols = pl.ds(i * block, block)
        cos, sin = cos_ref[:, cols], sin_ref[:, cols]

        @pl.loop(0, heads)
        def _(h):
            base = pl.multiple_of(h * HEAD_SIZE, HEAD_SIZE)
            mine = pl.ds(base, HEAD_SIZE)
            query = qkv_ref[mine, cols]
            grad = grad_ref[mine, cols]
            delta = jnp.sum(
                grad.astype(F32) * out_ref[mine, cols].astype(F32), axis=0, keepdims=True
            )
            log_total = log_ref[pl.ds(h, 1), cols]
            dquery = None
            for j in range(i + 1):
                rows = pl.ds(j * block, block)
                s = mm(kv_ref[rows, :HEAD_SIZE], query)
                if i == j:
                    s = s + mask_ref[...]
                probs = jnp.exp(s - log_total)
                dprobs = mm(kv_ref[rows, HEAD_SIZE:], grad)
                dscores = (probs * (dprobs - delta)).astype(BF16)
                dkv[0, rows, :] += mm(dscores, query, 1, 1)
                dkv[1, rows, :] += mm(probs.astype(BF16), grad, 1, 1)
                term = mm(qkv_ref[keys, rows], dscores)
                dquery = term if dquery is None else dquery + term
            dquery = dquery * scale
            a, b = unrotate(dquery[:half], dquery[half:], cos, sin)
            dqkv_ref[pl.ds(base, half), cols] = a.astype(BF16)
            dqkv_ref[pl.ds(base + half, half), cols] = b.astype(BF16)

    @pl.loop(0, 2 * n - 1)
    def _(turn):
        hop = (turn + 1) // 2
        leftward = lax.rem(turn, 2) == 1
        shard = jnp.where(leftward, me - hop, me + hop)

        @pl.when(leftward)
        def _():
            @pl.loop(EARLY, pieces)
            def _(piece):
                gather.receive(hop, piece)

        @pl.when(within(shard, n))
        def _():
            project(shard)
            for i in range(n):

                @pl.when(shard == i)
                def _():
                    attention_rows(i)

        @pl.when(jnp.logical_not(leftward) & within(hop - 1, min(n, pieces) - 1))
        def _():
            sum_piece(hop - 1)

    dkeys = dkv[0].T
    a, b = unrotate(dkeys[:half], dkeys[half:], cos_ref[...], sin_ref[...])
    dqkv_ref[pl.ds(heads * HEAD_SIZE, half), :] = a.astype(BF16)
    dqkv_ref[pl.ds(heads * HEAD_SIZE + half, half), :] = b.astype(BF16)
    dqkv_ref[pl.ds((heads + 1) * HEAD_SIZE, HEAD_SIZE), :] = dkv[1].T.astype(BF16)
    saves = []
    count_tiles = len(tiles(width, 512))
    for index, (start, count) in enumerate(tiles(width, 512)):
        cols = slice(start, start + count)
        part_ref[:, cols] = mm(dqkv_ref[...], w_ref[cols, :], 0, 1).astype(BF16)
        save = pltpu.make_async_copy(
            part_ref.at[:, pl.ds(start, count)],
            part_hbm.at[:, pl.ds(start, count)],
            save_sem.at[count_tiles + index],
        )
        save.start()
        saves.append(save)
    for index, (start, count) in enumerate(tiles(width, 512)):
        cols = slice(start, start + count)
        wgrad[cols, :cols_in] = mm(norm_ref[:, cols], dqkv_ref[...], 0, 1).astype(BF16)
        for shard in range(n):
            term = mm(seq[shard, :, cols], out_ref[:, shard * rows_all : (shard + 1) * rows_all], 0, 1)
            total = term if shard == 0 else total + term
        wgrad[cols, cols_in:] = total.astype(BF16)
        save = pltpu.make_async_copy(
            wgrad.at[pl.ds(start, count), :], wgrad_hbm.at[pl.ds(start, count), :], save_sem.at[index]
        )
        save.start()
        saves.append(save)
    for piece in range(min(n, pieces) - 1, pieces):
        sum_piece(piece)
    scatter.finish()
    gather.finish(EARLY, pieces)
    for save in saves:
        save.wait()


def attend_back(
    n, mid, kv, log_total, cos, sin, low, hidden, w_mlp, w_out, w_qkv, qkv, out, norm, pieces=4
):
    rows, width = mid.shape
    block = rows
    length = n * rows
    cols_in = qkv.shape[0]
    heads = cols_in // HEAD_SIZE - 2
    units = hidden.shape[2]
    any_spec = pl.BlockSpec(memory_space=pl.ANY)
    wgrad_shape = (width, cols_in + w_out.shape[0])
    return pl.pallas_call(
        functools.partial(attend_back_kernel, n, heads, block, pieces),
        out_shape=(
            jax.ShapeDtypeStruct((rows, width), BF16),
            jax.ShapeDtypeStruct((length, width), BF16),
            jax.ShapeDtypeStruct(wgrad_shape, BF16),
        ),
        in_specs=[VMEM_SPEC] * 4 + [any_spec] * 9,
        out_specs=(VMEM_SPEC,) + (any_spec,) * 2,
        scratch_shapes=[
            pltpu.VMEM(mid.shape, F32),
            pltpu.VMEM((length, width), BF16),
            pltpu.VMEM((n, rows, width), BF16),
            pltpu.VMEM((n, rows, units), BF16),
            pltpu.VMEM((width, units), BF16),
            pltpu.VMEM((n, rows, width), BF16),
            pltpu.VMEM((n + 1, rows, width), BF16),
            pltpu.VMEM(w_out.shape, BF16),
            pltpu.VMEM(w_qkv.shape, BF16),
            pltpu.VMEM(qkv.shape, BF16),
            pltpu.VMEM(out.shape, BF16),
            pltpu.VMEM(norm.shape, BF16),
            pltpu.VMEM((2, length, HEAD_SIZE), F32),
            pltpu.VMEM((block, block), F32),
            pltpu.VMEM((heads * HEAD_SIZE, length), BF16),
            pltpu.VMEM((cols_in, length), BF16),
            pltpu.VMEM(wgrad_shape, BF16),
        ]
        + sems(n, pieces) * 2
        + [pltpu.SemaphoreType.DMA((9,)), pltpu.SemaphoreType.DMA((2 * len(tiles(width, 512)),))],
        compiler_params=comm_params(3),
        cost_estimate=pl.CostEstimate(
            flops=6 * length * width * wgrad_shape[1],
            bytes_accessed=350 * 1024 * 1024,
            transcendentals=heads * length * length,
        ),
        name="attend_back",
    )(kv, log_total, cos, sin, mid, low, hidden, w_mlp, w_out, w_qkv, qkv, out, norm)


def local(
    n, dp, x, gain_attn, gain_mlp, w_query, w_key, w_value, w_out, w_gate, w_up, w_down, cotangent
):
    rows, _ = x.shape
    length = n * rows
    per = gain_attn.shape[0]
    packed = 2 * per + (-2 * per) % LANES

    mlp_all = lax.all_gather(
        jnp.concatenate([w_gate, w_up, w_down.T], axis=1), "dp", axis=0, tiled=True
    )
    gains = [gain_attn, gain_mlp]
    if packed > 2 * per:
        gains.append(jnp.zeros((packed - 2 * per,), F32))
    cos, sin = tables(length)
    full_attn, full_mlp, kv, attended, log_total, norm_attn, qkv, out_part, w_qkv, w_out_all, near = attend(
        n,
        dp,
        x,
        jnp.concatenate(gains).reshape(1, packed),
        (w_query, w_key.T, w_value.T, w_out),
        cos,
        sin,
        cotangent,
    )
    dgain_mlp, mid, grad_mid, hidden, mlp_grad, grad_low = mlp(
        n, out_part, x, full_mlp, mlp_all, cotangent, near
    )
    mlp_grad = lax.psum_scatter(mlp_grad, "dp", scatter_dimension=0, tiled=True)
    block_output, attn_part, attn_grad = attend_back(
        n, mid, kv, log_total, cos, sin, grad_low, hidden, mlp_all, w_out_all, w_qkv, qkv, attended, norm_attn
    )
    attn_grad = lax.psum_scatter(attn_grad, "dp", scatter_dimension=0, tiled=True)
    input_grad, dgains = sum_input_grad(
        n, dp, attn_part, x, full_attn, grad_mid, dgain_mlp, packed
    )
    gate, up, down, query, key, value, out, dgain_attn, dgain_mlp, block_output, input_grad = widen(
        mlp_grad, attn_grad, dgains, block_output, input_grad, per, w_query.shape[1], w_key.shape[1]
    )
    return (
        block_output,
        input_grad,
        dgain_attn.reshape(per),
        dgain_mlp.reshape(per),
        query,
        key.T,
        value.T,
        out,
        gate,
        up,
        down,
    )


def solution(mesh):
    rows = P(("dp", "tensor"), None)
    gain = P(("dp", "tensor"))
    into = P("dp", "tensor")
    back = P("tensor", "dp")
    in_specs = (rows, gain, gain, into, into, into, back, into, into, back, rows)
    out_specs = (rows, rows, gain, gain, into, into, into, back, into, into, back)

    def body(*args):
        return local(mesh.shape["tensor"], mesh.shape["dp"], *args)

    return jax.shard_map(body, mesh=mesh, in_specs=in_specs, out_specs=out_specs, check_vma=False)
```

```python
import functools
import math

import jax
import jax.numpy as jnp
from jax import lax
from jax.experimental import pallas as pl
from jax.experimental.pallas import tpu as pltpu
from jax.sharding import PartitionSpec as P


HEAD_SIZE = 64
EPS = 1e-05
ROPE_BASE = 10000.0
NEG_LARGE = -1e30
LANES = 128
MESH = pl.DeviceIdType.MESH
F32 = jnp.float32
BF16 = jnp.bfloat16
VMEM_SPEC = pl.BlockSpec(memory_space=pltpu.VMEM)
EARLY = 0
FAR_DONE = 3


def tables(sequence_length):
    half = HEAD_SIZE // 2
    frequency = ROPE_BASE ** (-(jnp.arange(half, dtype=F32) * 2.0) / HEAD_SIZE)
    angles = frequency[:, None] * jnp.arange(sequence_length, dtype=F32)[None, :]
    return jnp.cos(angles), jnp.sin(angles)


def dims(contract_left, contract_right):
    return (((contract_left,), (contract_right,)), ((), ()))


def mm(left, right, contract_left=1, contract_right=0):
    return lax.dot_general(
        left, right, dims(contract_left, contract_right), preferred_element_type=F32
    )


def piece_rows(piece, size):
    return pl.ds(pl.multiple_of(piece * size, size), size)


class Line:
    def __init__(self, n):
        self.n = n
        self.me = lax.axis_index("tensor")

    def barrier(self):
        barrier = pltpu.get_barrier_semaphore()
        n, me = self.n, self.me

        @pl.when(me > 0)
        def _():
            pl.semaphore_signal(barrier, inc=1, device_id={"tensor": me - 1}, device_id_type=MESH)

        @pl.when(me < n - 1)
        def _():
            pl.semaphore_signal(barrier, inc=1, device_id={"tensor": me + 1}, device_id_type=MESH)

        inner = (me > 0) & (me < n - 1)

        @pl.when(inner)
        def _():
            pl.semaphore_wait(barrier, 2)

        @pl.when(jnp.logical_not(inner))
        def _():
            pl.semaphore_wait(barrier, 1)

    def copy(self, src, dst, send, recv, step):
        return pltpu.make_async_remote_copy(
            src_ref=src,
            dst_ref=dst,
            send_sem=send,
            recv_sem=recv,
            device_id={"tensor": self.me + step},
            device_id_type=MESH,
        )


class Gather:
    def __init__(self, line, buf, send, recv, pieces):
        self.line, self.buf, self.send, self.recv, self.pieces = line, buf, send, recv, pieces
        self.size = buf.shape[1] // pieces

    def message(self, right, hop, piece, shard):
        d = 0 if right else 1
        part = self.buf.at[shard, piece_rows(piece, self.size)]
        return self.line.copy(
            part, part, self.send.at[d, hop - 1, piece], self.recv.at[d, hop - 1, piece], 1 if right else -1
        )

    def start_own(self, piece):
        line = self.line
        me, n = line.me, line.n

        @pl.when(me < n - 1)
        def _():
            self.message(True, 1, piece, me).start()

        @pl.when(me > 0)
        def _():
            self.message(False, 1, piece, me).start()

    def start_hop(self, hop, piece):
        line = self.line
        me, n = line.me, line.n

        @pl.when((me - (hop - 1) >= 0) & (me < n - 1))
        def _():
            self.message(True, hop, piece, me - (hop - 1)).start()

        @pl.when((me + (hop - 1) <= n - 1) & (me > 0))
        def _():
            self.message(False, hop, piece, me + (hop - 1)).start()

    def receive(self, hop, piece, use=None):
        line = self.line
        me, n = line.me, line.n

        @pl.when(me - hop >= 0)
        def _():
            shard = me - hop
            self.message(True, hop, piece, shard).wait_recv()
            if not isinstance(hop, int) or hop < n - 1:

                @pl.when((me < n - 1) & (hop < n - 1))
                def _():
                    self.message(True, hop + 1, piece, shard).start()

            if use is not None:
                use(shard, piece)

        @pl.when(me + hop <= n - 1)
        def _():
            shard = me + hop
            self.message(False, hop, piece, shard).wait_recv()
            if not isinstance(hop, int) or hop < n - 1:

                @pl.when((me > 0) & (hop < n - 1))
                def _():
                    self.message(False, hop + 1, piece, shard).start()

            if use is not None:
                use(shard, piece)

    def finish(self, first_piece=0, end_piece=None):
        line = self.line
        me, n = line.me, line.n

        @pl.loop(first_piece, self.pieces if end_piece is None else end_piece)
        def _(piece):
            for hop in range(1, n):

                @pl.when((me - (hop - 1) >= 0) & (me < n - 1))
                def _():
                    self.message(True, hop, piece, me - (hop - 1)).wait_send()

                @pl.when((me + (hop - 1) <= n - 1) & (me > 0))
                def _():
                    self.message(False, hop, piece, me + (hop - 1)).wait_send()


class Scatter:
    def __init__(self, line, part, buf, send, recv, pieces):
        self.line, self.part, self.buf, self.pieces = line, part, buf, pieces
        self.send, self.recv = send, recv
        self.size = part.shape[1] // pieces

    def rows(self, piece):
        return piece_rows(piece, self.size)

    def outgoing(self, d, target, piece, from_part=False):
        rows, line = self.rows(piece), self.line
        src = (self.part if from_part else self.buf).at[target, rows]
        slot = target
        if d == 1:
            slot = jnp.where(target == line.me - 1, line.n, target)
        return line.copy(
            src,
            self.buf.at[slot, rows],
            self.send.at[d, target, piece],
            self.recv.at[d, target, piece],
            1 if d == 0 else -1,
        )

    def incoming(self, d, target, slot, piece):
        part = self.buf.at[slot, self.rows(piece)]
        return self.line.copy(
            part, part, self.send.at[d, target, piece], self.recv.at[d, target, piece], 1 if d == 0 else -1
        )

    def start_ends(self, piece):
        line = self.line
        me, n = line.me, line.n

        @pl.when(me == 0)
        def _():
            for target in range(n - 1, 0, -1):
                self.outgoing(0, target, piece, True).start()

        @pl.when(me == n - 1)
        def _():
            for target in range(0, n - 1):
                self.outgoing(1, target, piece, True).start()

    def pass_on(self, d, target, piece):
        buf = self.buf
        self.incoming(d, target, target, piece).wait_recv()
        rows = self.rows(piece)
        total = buf[target, rows].astype(F32) + self.part[target, rows].astype(F32)
        buf[target, rows] = total.astype(BF16)
        self.outgoing(d, target, piece).start()

    def passes(self, piece, right, targets, where):
        line = self.line
        me, n = line.me, line.n
        for target in targets:
            held = (me > 0) & (me < target) if right else (me < n - 1) & (me > target)

            @pl.when(where & held)
            def _():
                self.pass_on(0 if right else 1, target, piece)

    def first(self, piece):
        n, left_half = self.line.n, self.line.me < self.line.n // 2
        self.passes(piece, True, (n - 1,), left_half)
        self.passes(piece, False, (0,), jnp.logical_not(left_half))

    def rest(self, piece):
        n, left_half = self.line.n, self.line.me < self.line.n // 2
        right_half = jnp.logical_not(left_half)
        self.passes(piece, True, range(n - 2, 0, -1), left_half)
        self.passes(piece, False, range(1, n - 1), right_half)
        self.passes(piece, False, range(0, n - 1), left_half)
        self.passes(piece, True, range(n - 1, 0, -1), right_half)

    def middle(self, piece):
        self.first(piece)
        self.rest(piece)

    def result(self, piece, store):
        line = self.line
        me, n = line.me, line.n
        rows = self.rows(piece)

        @pl.when(me > 0)
        def _():
            self.incoming(0, me, me, piece).wait_recv()

        @pl.when(me < n - 1)
        def _():
            self.incoming(1, me, n, piece).wait_recv()

        own = self.part[me, rows].astype(F32)

        @pl.when(me == 0)
        def _():
            store(own + self.buf[n, rows].astype(F32))

        @pl.when(me == n - 1)
        def _():
            store(own + self.buf[me, rows].astype(F32))

        @pl.when((me > 0) & (me < n - 1))
        def _():
            store(own + self.buf[me, rows].astype(F32) + self.buf[n, rows].astype(F32))

    def finish(self, ends=True, middles=True):
        line = self.line
        me, n = line.me, line.n
        inner = (me > 0) & (me < n - 1)

        @pl.when((inner & middles) | (jnp.logical_not(inner) & ends))
        def _():
            @pl.loop(0, self.pieces)
            def _(piece):
                for target in range(1, n):

                    @pl.when(me < target)
                    def _():
                        self.outgoing(0, target, piece).wait_send()

                for target in range(0, n - 1):

                    @pl.when(me > target)
                    def _():
                        self.outgoing(1, target, piece).wait_send()


def within(piece, pieces):
    return (piece >= 0) & (piece < pieces)


def sems(n, pieces):
    return [pltpu.SemaphoreType.DMA((2, n, pieces)), pltpu.SemaphoreType.DMA((2, n, pieces))]


def comm_params(collective_id):
    return pltpu.CompilerParams(
        collective_id=collective_id, has_side_effects=True, vmem_limit_bytes=60 * 1024 * 1024
    )


def exchange_all(n, dp, send_row, recv_row, send, recv, start_only=False, wait_only=False):
    devices = n * dp
    me = lax.axis_index("dp") * n + lax.axis_index("tensor")

    def message(offset, peer, source):
        return pltpu.make_async_remote_copy(
            src_ref=send_row(peer),
            dst_ref=recv_row(source),
            send_sem=send.at[offset],
            recv_sem=recv.at[offset],
            device_id={"dp": peer // n, "tensor": peer % n},
            device_id_type=MESH,
        )

    if not wait_only:

        @pl.loop(1, devices)
        def _(offset):
            message(offset, lax.rem(me + offset, devices), me).start()

    if not start_only:

        @pl.loop(1, devices)
        def _(offset):
            copy = message(offset, lax.rem(me + offset, devices), me)
            copy.wait_send()
            copy.wait_recv()


def barrier_all(n, dp):
    devices = n * dp
    me = lax.axis_index("dp") * n + lax.axis_index("tensor")
    barrier = pltpu.get_barrier_semaphore()

    @pl.loop(1, devices)
    def _(offset):
        peer = lax.rem(me + offset, devices)
        pl.semaphore_signal(
            barrier, inc=1, device_id={"dp": peer // n, "tensor": peer % n}, device_id_type=MESH
        )

    pl.semaphore_wait(barrier, devices - 1)


def even_tile(extent):
    return 512 if extent % 512 == 0 else extent


def tiles(extent, size):
    return [(start, min(size, extent - start)) for start in range(0, extent, size)]


def mlp_kernel(
    n, pieces, gain_ref, part_hbm, x_hbm, w_hbm, cot_hbm, near_hbm,
    dgain_ref, mid_hbm, grad_hbm, hid_hbm, wgrad_hbm, low_hbm,
    part_ref, x_ref, mid_ref, grad_ref, w, cot, seq, buf, npart, buf_back, hid, dgate, dup, stage, inv_ref,
    ssend, srecv, gsend, grecv, bsend, brecv, csend, crecv, lsend, lrecv, local_sem, stage_sem, part_sem,
):
    line = Line(n)
    me = line.me
    rows_all, width = part_ref.shape[1:]

    def part_load(piece):
        rows = piece_rows(piece, rows_all // pieces)
        return pltpu.make_async_copy(part_hbm.at[:, rows], part_ref.at[:, rows], part_sem.at[0, piece])

    def piece_save(which, ref, hbm, piece):
        rows = piece_rows(piece, rows_all // pieces)
        return pltpu.make_async_copy(ref.at[rows], hbm.at[rows], part_sem.at[which, piece])

    x_load = pltpu.make_async_copy(x_hbm, x_ref, local_sem.at[3])
    for piece in range(pieces):
        part_load(piece).start()
    x_load.start()

    units = hid.shape[2]
    weight_load = pltpu.make_async_copy(w_hbm, w, local_sem.at[0])
    own_load = pltpu.make_async_copy(cot_hbm, cot.at[me], local_sem.at[1])
    inner = (me > 0) & (me < n - 1)

    def near_load(shard, count):
        rows = pl.ds(0, count)
        return pltpu.make_async_copy(near_hbm.at[shard, rows], cot.at[shard, rows], local_sem.at[5 + shard])

    def each_near(act):
        for shard in range(n):
            here = (me != shard) & (inner | (me - shard == 1) | (shard - me == 1))

            @pl.when(here)
            def _():
                act(near_load(shard, rows_all))

            if n == 4:

                @pl.when(jnp.logical_not(inner) & ((me - shard == 2) | (shard - me == 2)))
                def _():
                    act(near_load(shard, rows_all // pieces * FAR_DONE))

    each_near(lambda copy: copy.start())
    own_load.start()
    weight_load.start()
    line.barrier()
    scatter = Scatter(line, part_ref, buf, ssend, srecv, pieces)
    gather = Gather(line, seq, gsend, grecv, pieces)
    scatter_back = Scatter(line, npart, buf_back, bsend, brecv, pieces)
    cot_gather = Gather(line, cot, csend, crecv, pieces)
    low_gather = Gather(line, buf, lsend, lrecv, pieces)
    size = scatter.size
    part_load(0).wait()
    scatter.start_ends(0)
    for piece in range(1, pieces):
        part_load(piece).wait()
    x_load.wait()
    dgain_ref[...] = jnp.zeros_like(dgain_ref)

    each_near(lambda copy: copy.wait())

    def still_far(hop, piece):
        return (piece >= FAR_DONE) if hop == 2 and n == 4 else (piece >= 0)

    def each_far(piece, act):
        for hop in range(2, n):

            @pl.when((me == n - 2) & still_far(hop, piece))
            def _():
                act(True, hop, me - (hop - 1))

            @pl.when((me == 1) & still_far(hop, piece))
            def _():
                act(False, hop, me + (hop - 1))

    def far_start(piece):
        each_far(piece, lambda right, hop, shard: cot_gather.message(right, hop, piece, shard).start())

    def far_sent(piece):
        each_far(piece, lambda right, hop, shard: cot_gather.message(right, hop, piece, shard).wait_send())

    def far_arrived(piece):
        for hop in range(2, n):

            @pl.when((me == n - 1) & still_far(hop, piece))
            def _():
                cot_gather.message(True, hop, piece, me - hop).wait_recv()

            @pl.when((me == 0) & still_far(hop, piece))
            def _():
                cot_gather.message(False, hop, piece, me + hop).wait_recv()

    for piece in range(min(3, pieces)):
        far_start(jnp.int32(piece))

    def norm(piece):
        rows = scatter.rows(piece)

        def store(total):
            mid_ref[rows, :] = x_ref[rows, :].astype(F32) + total

        scatter.result(piece, store)
        mid = mid_ref[rows, :]
        inv = lax.rsqrt(jnp.mean(mid * mid, axis=1, keepdims=True) + EPS)
        inv_ref[rows, :] = jnp.broadcast_to(inv, (size, LANES))
        seq[me, rows, :] = (mid * inv * gain_ref[...]).astype(BF16)
        piece_save(1, mid_ref, mid_hbm, piece).start()

    def back(piece):
        rows = scatter.rows(piece)

        def store(total):
            grad_ref[rows, :] = total

        scatter_back.result(piece, store)
        grad = grad_ref[rows, :]
        mid = mid_ref[rows, :]
        inv = inv_ref[rows, 0:1]
        dgain_ref[...] += jnp.sum(grad * mid * inv, axis=0, keepdims=True)
        scaled = grad * gain_ref[...]
        mean = jnp.mean(scaled * mid, axis=1, keepdims=True)
        out = cot[me, rows, :].astype(F32) + inv * (scaled - mid * (inv * inv * mean))
        grad_ref[rows, :] = out
        buf[me, rows, :] = out.astype(BF16)
        piece_save(2, grad_ref, grad_hbm, piece).start()

    def flat(ref, piece):
        value = ref[:, scatter.rows(piece), :]
        return value.reshape(n * size, value.shape[2])

    def feed(piece):
        rows = scatter.rows(piece)
        for start, count in tiles(units, 512):
            x = flat(seq, piece)
            gate = mm(x, w[:, start : start + count])
            up = mm(x, w[:, units + start : units + start + count])
            dhidden = mm(flat(cot, piece), w[:, 2 * units + start : 2 * units + start + count])
            sigmoid = jax.nn.sigmoid(gate)
            act = gate * sigmoid
            cols = slice(start, start + count)
            shape = (n, size, count)
            hid[:, rows, cols] = (act * up).astype(BF16).reshape(shape)
            dup[:, rows, cols] = (dhidden * act).astype(BF16).reshape(shape)
            dgate[:, rows, cols] = (
                (dhidden * up * sigmoid * (1.0 + gate * (1.0 - sigmoid))).astype(BF16).reshape(shape)
            )
        tile = even_tile(width)

        @pl.loop(0, width // tile)
        def _(index):
            cols = piece_rows(index, tile)
            total = mm(flat(dgate, piece), w[cols, :units], 1, 1)
            total += mm(flat(dup, piece), w[cols, units : 2 * units], 1, 1)
            npart[:, rows, cols] = total.astype(BF16).reshape(n, size, tile)

    step_rows = min(LANES, width)
    count = width // step_rows

    def save(index, slot):
        return pltpu.make_async_copy(
            stage.at[slot],
            wgrad_hbm.at[pl.ds(pl.multiple_of(index * step_rows, step_rows), step_rows), :],
            stage_sem.at[slot],
        )

    def weight_grads(events):
        @pl.loop(0, count)
        def _(index):
            for at, event in events:

                @pl.when(index == at)
                def _():
                    event()

            slot = lax.rem(index, 2)
            cols = pl.ds(pl.multiple_of(index * step_rows, step_rows), step_rows)

            @pl.when(index >= 2)
            def _():
                save(index - 2, slot).wait()

            x = seq[:, :, cols].reshape(n * rows_all, step_rows)
            g = cot[:, :, cols].reshape(n * rows_all, step_rows)
            for at, left, right in ((0, x, dgate), (1, x, dup), (2, g, hid)):
                value = right[...].reshape(n * rows_all, units)
                stage[slot, :, at * units : (at + 1) * units] = mm(left, value, 0, 0).astype(BF16)
            save(index, slot).start()

    hid_save = pltpu.make_async_copy(hid, hid_hbm, local_sem.at[2])

    @pl.loop(0, pieces + n - 1)
    def _(step):
        first = step < pieces

        @pl.when(first)
        def _():
            @pl.when(step + 1 < pieces)
            def _():
                scatter.start_ends(step + 1)

            scatter.middle(step)

            @pl.when(step + 3 < pieces)
            def _():
                far_start(step + 3)

        for hop in range(1, n):
            piece = step - hop

            @pl.when(within(piece, pieces))
            def _():
                gather.receive(hop, piece)

        @pl.when(first)
        def _():
            norm(step)
            gather.start_own(step)

        ready = step - (n - 1)

        @pl.when(ready == 0)
        def _():
            own_load.wait()
            weight_load.wait()

        @pl.when(ready == 1)
        def _():
            scatter.finish(ends=False)

        for hop in range(1, n):
            piece = ready - 1 - hop

            @pl.when(within(piece, EARLY))
            def _():
                low_gather.receive(hop, piece)

        @pl.when(ready >= 1)
        def _():
            scatter_back.middle(ready - 1)

        @pl.when(ready >= 0)
        def _():
            far_arrived(ready)
            feed(ready)
            scatter_back.start_ends(ready)

        @pl.when(ready >= 1)
        def _():
            back(ready - 1)

            @pl.when(ready - 1 < EARLY)
            def _():
                low_gather.start_own(ready - 1)

    hid_save.start()
    last = pieces - 1

    def low_arrivals(step):
        for hop in range(1, n):
            piece = step - hop
            if 0 <= piece < EARLY:
                low_gather.receive(hop, piece)

    late = [
        (lambda step: lambda: low_arrivals(step))(step) for step in range(pieces - 1, pieces + n - 2)
    ]
    events = [
        (count // 4, lambda: scatter_back.first(last)),
        (count * 5 // 8, lambda: scatter_back.rest(last)),
    ]
    if EARLY:
        events += [(count * (2 * i + 1) // (2 * len(late)), event) for i, event in enumerate(late)]
    weight_grads(events)
    back(last)
    own_rows, early_rows = pl.ds(EARLY * size, rows_all - EARLY * size), pl.ds(0, EARLY * size)
    low_saves = [
        pltpu.make_async_copy(buf.at[me, own_rows], low_hbm.at[me, own_rows], local_sem.at[4])
    ]
    if EARLY:
        low_saves.append(
            pltpu.make_async_copy(
                buf.at[pl.ds(0, n), early_rows], low_hbm.at[:, early_rows], local_sem.at[0]
            )
        )
    for save_low in low_saves:
        save_low.start()
    scatter.finish(middles=False)
    gather.finish()
    scatter_back.finish()
    low_gather.finish(0, EARLY)

    @pl.loop(0, pieces)
    def _(piece):
        far_sent(piece)
        piece_save(1, mid_ref, mid_hbm, piece).wait()
        piece_save(2, grad_ref, grad_hbm, piece).wait()

    for save_low in low_saves:
        save_low.wait()
    hid_save.wait()
    for index in range(max(count - 2, 0), count):
        save(index, index % 2).wait()


def mlp(n, part, x, gain, weights, cotangent, near, pieces=4):
    rows, width = x.shape
    units = weights.shape[1] // 3
    any_spec = pl.BlockSpec(memory_space=pl.ANY)
    return pl.pallas_call(
        functools.partial(mlp_kernel, n, pieces),
        out_shape=(
            jax.ShapeDtypeStruct((1, width), F32),
            jax.ShapeDtypeStruct((rows, width), F32),
            jax.ShapeDtypeStruct((rows, width), F32),
            jax.ShapeDtypeStruct((n, rows, units), BF16),
            jax.ShapeDtypeStruct((width, 3 * units), BF16),
            jax.ShapeDtypeStruct((n, rows, width), BF16),
        ),
        in_specs=[VMEM_SPEC] + [any_spec] * 5,
        out_specs=(VMEM_SPEC,) + (any_spec,) * 5,
        scratch_shapes=[
            pltpu.VMEM((n, rows, width), BF16),
            pltpu.VMEM((rows, width), BF16),
            pltpu.VMEM((rows, width), F32),
            pltpu.VMEM((rows, width), F32),
            pltpu.VMEM((width, 3 * units), BF16),
            pltpu.VMEM((n, rows, width), BF16),
            pltpu.VMEM((n, rows, width), BF16),
            pltpu.VMEM((n + 1, rows, width), BF16),
            pltpu.VMEM((n, rows, width), BF16),
            pltpu.VMEM((n + 1, rows, width), BF16),
            pltpu.VMEM((n, rows, units), BF16),
            pltpu.VMEM((n, rows, units), BF16),
            pltpu.VMEM((n, rows, units), BF16),
            pltpu.VMEM((2, min(LANES, width), 3 * units), BF16),
            pltpu.VMEM((rows, LANES), F32),
        ]
        + sems(n, pieces) * 5
        + [pltpu.SemaphoreType.DMA((5 + n,)), pltpu.SemaphoreType.DMA((2,)), pltpu.SemaphoreType.DMA((3, pieces))],
        compiler_params=pltpu.CompilerParams(
            collective_id=2, has_side_effects=True, vmem_limit_bytes=67043328
        ),
        cost_estimate=pl.CostEstimate(
            flops=18 * n * rows * width * units, bytes_accessed=500 * 1024 * 1024, transcendentals=0
        ),
        name="mlp",
    )(gain, part.reshape(n, rows, width), x, weights, cotangent, near)


def last_kernel(
    n, dp, pieces, gain_ref, dgain_mlp_ref, part_hbm, x_hbm, grad_mid_hbm, seq_hbm, out_ref, gains_ref,
    part_ref, x_ref, grad_mid_ref, seq_ref, total_ref, dgain_ref, packed, held, buf, ssend, srecv, gsend, grecv, load_sem,
):
    def part_load(piece):
        rows = piece_rows(piece, part_ref.shape[1] // pieces)
        return pltpu.make_async_copy(part_hbm.at[:, rows], part_ref.at[:, rows], load_sem.at[2 + piece])

    others = [
        pltpu.make_async_copy(x_hbm, x_ref, load_sem.at[0]),
        pltpu.make_async_copy(grad_mid_hbm, grad_mid_ref, load_sem.at[1]),
        pltpu.make_async_copy(seq_hbm, seq_ref, load_sem.at[2 + pieces]),
    ]
    for piece in range(pieces):
        part_load(piece).start()
    for load in others:
        load.start()
    line = Line(n)
    all_me = lax.axis_index("dp") * n + line.me
    barrier_all(n, dp)
    scatter = Scatter(line, part_ref, buf, ssend, srecv, pieces)
    part_load(0).wait()
    scatter.start_ends(0)
    for piece in range(1, pieces):
        part_load(piece).wait()
    for load in others:
        load.wait()
    dgain_ref[...] = jnp.zeros_like(dgain_ref)
    packed[...] = jnp.zeros_like(packed)

    width = x_ref.shape[1]
    per = width // (n * dp)
    half = pieces // 2
    share = x_ref.shape[0] // half

    def exchange(**kind):
        exchange_all(
            n, dp, lambda peer: packed.at[peer], lambda source: held.at[source], gsend, grecv, **kind
        )

    def gain_share(index):
        rows = piece_rows(index, share)
        x = seq_ref[:, rows, :].reshape(n * share, width).astype(F32)
        term = part_ref[:, rows, :].reshape(n * share, width).astype(F32)
        inv = lax.rsqrt(jnp.mean(x * x, axis=1, keepdims=True) + EPS)
        dgain_ref[...] += jnp.sum(term * x * inv, axis=0, keepdims=True)

    def send_gains():
        for device in range(n * dp):
            cols = slice(device * per, (device + 1) * per)
            packed[device, :, :per] = dgain_ref[:, cols]
            packed[device, :, per : 2 * per] = dgain_mlp_ref[:, cols]
        held[all_me] = packed[all_me]
        exchange(start_only=True)

    @pl.loop(0, pieces)
    def _(piece):
        @pl.when(piece + 1 < pieces)
        def _():
            scatter.start_ends(piece + 1)

        @pl.when(piece < half)
        def _():
            gain_share(piece)

        @pl.when(piece == half)
        def _():
            send_gains()

        scatter.middle(piece)
        rows = scatter.rows(piece)

        def store(total):
            total_ref[...] = total

        scatter.result(piece, store)
        grad = total_ref[...]
        x = x_ref[rows, :].astype(F32)
        inv = lax.rsqrt(jnp.mean(x * x, axis=1, keepdims=True) + EPS)
        scaled = grad * gain_ref[...]
        mean = jnp.mean(scaled * x, axis=1, keepdims=True)
        out = grad_mid_ref[rows, :] + inv * (scaled - x * (inv * inv * mean))
        out_ref[rows, :] = out.astype(BF16)

    exchange(wait_only=True)
    gains_ref[...] = jnp.sum(held[...], axis=0)
    scatter.finish()


def sum_input_grad(n, dp, part, x, gain, grad_mid, dgain_mlp, seq, packed, pieces=8):
    rows, width = x.shape
    any_spec = pl.BlockSpec(memory_space=pl.ANY)
    return pl.pallas_call(
        functools.partial(last_kernel, n, dp, pieces),
        out_shape=(
            jax.ShapeDtypeStruct((rows, width), BF16),
            jax.ShapeDtypeStruct((1, packed), F32),
        ),
        in_specs=[VMEM_SPEC] * 2 + [any_spec] * 4,
        out_specs=(VMEM_SPEC,) * 2,
        scratch_shapes=[
            pltpu.VMEM((n, rows, width), BF16),
            pltpu.VMEM((rows, width), BF16),
            pltpu.VMEM((rows, width), F32),
            pltpu.VMEM((n, rows, width), BF16),
            pltpu.VMEM((rows // pieces, width), F32),
            pltpu.VMEM((1, width), F32),
            pltpu.VMEM((n * dp, 1, packed), F32),
            pltpu.VMEM((n * dp, 1, packed), F32),
            pltpu.VMEM((n + 1, rows, width), BF16),
        ]
        + sems(n, pieces)
        + [pltpu.SemaphoreType.DMA((n * dp,)), pltpu.SemaphoreType.DMA((n * dp,))]
        + [pltpu.SemaphoreType.DMA((3 + pieces,))],
        compiler_params=comm_params(4),
        cost_estimate=pl.CostEstimate(flops=0, bytes_accessed=250 * 1024 * 1024, transcendentals=0),
        name="sum_input_grad",
    )(gain, dgain_mlp, part.reshape(n, rows, width), x, grad_mid, seq)


def widen_kernel(
    mlp_ref, attn_ref, gains_ref, rows_ref, input_ref,
    gate_ref, up_ref, down_ref, query_ref, key_ref, value_ref, out_ref,
    attn_gain_ref, mlp_gain_ref, rows_out_ref, input_out_ref,
):
    units = gate_ref.shape[1]
    per = attn_gain_ref.shape[1]
    attn_gain_ref[...] = gains_ref[:, :per]
    mlp_gain_ref[...] = gains_ref[:, per : 2 * per]
    rows_out_ref[...] = rows_ref[...]
    input_out_ref[...] = input_ref[...]
    gate_ref[...] = mlp_ref[:, :units].astype(F32)
    up_ref[...] = mlp_ref[:, units : 2 * units].astype(F32)
    down_ref[...] = mlp_ref[:, 2 * units :].astype(F32).T
    q_cols, k_cols = query_ref.shape[1], key_ref.shape[0]
    query_ref[...] = attn_ref[:, :q_cols].astype(F32)
    key_ref[...] = attn_ref[:, q_cols : q_cols + k_cols].astype(F32).T
    value_ref[...] = attn_ref[:, q_cols + k_cols : q_cols + 2 * k_cols].astype(F32).T
    out_ref[...] = attn_ref[:, q_cols + 2 * k_cols :].astype(F32).T


def widen(mlp_grad, attn_grad, gains, rows_out, input_out, per, q_cols, k_cols):
    rows, units = mlp_grad.shape[0], mlp_grad.shape[1] // 3
    shapes = [(rows, units)] * 2 + [(units, rows), (rows, q_cols)] + [(k_cols, rows)] * 2 + [(q_cols, rows)]
    return pl.pallas_call(
        widen_kernel,
        out_shape=tuple(jax.ShapeDtypeStruct(shape, F32) for shape in shapes + [(1, per)] * 2)
        + (jax.ShapeDtypeStruct(rows_out.shape, BF16),) * 2,
        in_specs=[VMEM_SPEC] * 5,
        out_specs=(VMEM_SPEC,) * 11,
        compiler_params=pltpu.CompilerParams(vmem_limit_bytes=56 * 1024 * 1024),
        name="widen",
    )(mlp_grad, attn_grad, gains, rows_out, input_out)


def rotate(half_a, half_b, cos, sin):
    return half_a * cos - half_b * sin, half_b * cos + half_a * sin


def unrotate(half_a, half_b, cos, sin):
    return half_a * cos + half_b * sin, half_b * cos - half_a * sin


def mask_block(size):
    key = lax.broadcasted_iota(jnp.int32, (size, size), 0)
    row = lax.broadcasted_iota(jnp.int32, (size, size), 1)
    return jnp.where(key <= row, 0.0, NEG_LARGE)


def attend_kernel(
    n, dp, heads, block, pieces, x_ref, gain_ref, cos_ref, sin_ref, cot_hbm, wq_hbm, wk_hbm, wv_hbm, wo_hbm,
    attn_gain_ref, mlp_gain_ref, kv_ref, out_ref, log_ref, norm_hbm, qkv_hbm, part_hbm, w_out_hbm, wo_out_hbm, near_hbm, seq_hbm,
    norm_ref, qkv_ref, part_ref, w_ref, wo_ref, seq, act_ref, mask_ref, gains, wq, wk, wv, wo, send, recv, gsend, grecv, wsend, wrecv, own_sem, csend, crecv, fsend, frecv, save_sem,
):
    half = HEAD_SIZE // 2
    rows_all, width = x_ref.shape
    length = n * rows_all
    line = Line(n)
    me = line.me
    mine = lax.axis_index("dp")
    barrier_all(n, dp)
    seq[me] = x_ref[...]
    gains[mine * n + me] = gain_ref[...]
    gather = Gather(line, seq, send, recv, pieces)

    @pl.loop(0, pieces)
    def _(piece):
        gather.start_own(piece)

    def gain_rows(**kind):
        exchange_all(
            n, dp, lambda peer: gain_ref, lambda source: gains.at[source], gsend, grecv, **kind
        )

    gain_rows(start_only=True)

    shards = ((wq_hbm, wq), (wk_hbm, wk), (wv_hbm, wv), (wo_hbm, wo))
    own = [pltpu.make_async_copy(src, dst.at[mine], own_sem.at[i]) for i, (src, dst) in enumerate(shards)]
    pair = mine + 1 - 2 * lax.rem(mine, 2)

    def even_copy(i, offset):
        src, dst = shards[i]
        return pltpu.make_async_remote_copy(
            src_ref=src,
            dst_ref=dst.at[mine],
            send_sem=wsend.at[0, i, offset],
            recv_sem=wrecv.at[0, i, offset],
            device_id={"dp": lax.rem(mine + 2 * offset, dp)},
            device_id_type=MESH,
        )

    def pair_copy(i, offset):
        dst = shards[i][1].at[lax.rem(mine + 2 * offset, dp)]
        return pltpu.make_async_remote_copy(
            src_ref=dst,
            dst_ref=dst,
            send_sem=wsend.at[1, i, offset],
            recv_sem=wrecv.at[1, i, offset],
            device_id={"dp": pair},
            device_id_type=MESH,
        )

    for i in range(4):
        own[i].start()

    @pl.loop(1, dp // 2)
    def _(offset):
        for i in range(4):
            even_copy(i, offset).start()

    def cot_copy(right, hop):
        d = 0 if right else 1
        shard = me - (hop - 1) if right else me + (hop - 1)
        src = cot_hbm if hop == 1 else near_hbm.at[shard]
        return line.copy(src, near_hbm.at[shard], csend.at[d, hop - 1], crecv.at[d, hop - 1], 1 if right else -1)

    inner = (me > 0) & (me < n - 1)

    @pl.when(me == 0)
    def _():
        cot_copy(True, 1).start()

    @pl.when(me == n - 1)
    def _():
        cot_copy(False, 1).start()

    q_cols, k_cols = wq.shape[2], wk.shape[1]
    w_rows, w_cols = wq.shape[1], wo.shape[2]

    saves = [
        pltpu.make_async_copy(src, dst, save_sem.at[i])
        for i, (src, dst) in enumerate(
            (
                (w_ref, w_out_hbm),
                (wo_ref, wo_out_hbm),
                (norm_ref, norm_hbm),
                (qkv_ref, qkv_hbm),
                (seq, seq_hbm),
            )
        )
    ]

    def project(shard):
        x = seq[shard].astype(F32)
        inv = lax.rsqrt(jnp.mean(x * x, axis=1, keepdims=True) + EPS)
        norm = (x * inv * attn_gain_ref[...]).astype(BF16)
        rows = piece_rows(shard, rows_all)
        norm_ref[rows, :] = norm
        act_ref[:, rows] = mm(w_ref[...], norm, 0, 1)

    def prepare():
        gain_rows(wait_only=True)
        per = width // (n * dp)
        for device in range(n * dp):
            attn_gain_ref[:, device * per : (device + 1) * per] = gains[device, :, :per]
            mlp_gain_ref[:, device * per : (device + 1) * per] = gains[device, :, per : 2 * per]

        @pl.loop(0, dp // 2)
        def _(offset):
            for i in range(4):
                pair_copy(i, offset).wait_recv()

        for d in range(dp):
            rows = slice(d * w_rows, (d + 1) * w_rows)
            w_ref[rows, :q_cols] = wq[d]
            w_ref[rows, q_cols : q_cols + k_cols] = wk[d].T
            w_ref[rows, q_cols + k_cols :] = wv[d].T
            wo_ref[:, d * w_cols : (d + 1) * w_cols] = wo[d]
        saves[0].start()
        saves[1].start()

    def start_pair():
        for i in range(4):
            own[i].wait()

        @pl.loop(1, dp // 2)
        def _(offset):
            for i in range(4):
                even_copy(i, offset).wait_recv()

        @pl.loop(0, dp // 2)
        def _(offset):
            for i in range(4):
                pair_copy(i, offset).start()

    def arrived(d, hop, shard):
        cot_copy_in(
            line, near_hbm, shard, crecv.at[d, hop - 1], csend.at[d, hop - 1], 1 if d == 1 else -1
        ).wait_recv()

    ready = min(2, n - 1)
    for hop in range(1, ready + 1):

        @pl.loop(0, pieces)
        def _(piece):
            gather.receive(hop, piece)
            if hop == ready:

                @pl.when(piece == pieces // 2)
                def _():
                    start_pair()

        @pl.when((me == hop) & (me < n - 1))
        def _():
            cot_copy(True, 1).start()

        @pl.when((n - 1 - me == hop) & (me > 0))
        def _():
            cot_copy(False, 1).start()

    if n == 4:

        @pl.when(me == 1)
        def _():
            arrived(0, 1, me - 1)
            cot_copy(True, 2).start()

        @pl.when(me == 2)
        def _():
            arrived(1, 1, me + 1)
            cot_copy(False, 2).start()

    prepare()

    @pl.loop(0, 2 * n - 1)
    def _(turn):
        hop = (turn + 1) // 2
        leftward = lax.rem(turn, 2) == 1
        shard = jnp.where(leftward, me - hop, me + hop)

        @pl.when(leftward & (hop > ready))
        def _():
            @pl.loop(0, pieces)
            def _(piece):
                gather.receive(hop, piece)

        @pl.when(within(shard, n))
        def _():
            project(shard)

    saves[4].start()

    def far_copy(right, shard):
        part = near_hbm.at[shard, pl.ds(0, rows_all // pieces * FAR_DONE)]
        d = 0 if right else 1
        return line.copy(part, part, fsend.at[d], frecv.at[d], jnp.where(inner, 1 if right else -1, jnp.where(me == 0, 1, -1)))

    if n == 4:

        @pl.when(me == 1)
        def _():
            arrived(1, 1, me + 1)
            far_copy(False, me + 1).start()

        @pl.when(me == 2)
        def _():
            arrived(0, 1, me - 1)
            far_copy(True, me - 1).start()

    cos, sin = cos_ref[...], sin_ref[...]

    scale = 1.0 / math.sqrt(HEAD_SIZE)

    @pl.loop(0, heads + 1)
    def _(h):
        base = pl.multiple_of(h * HEAD_SIZE, HEAD_SIZE)
        a, b = rotate(act_ref[pl.ds(base, half), :], act_ref[pl.ds(base + half, half), :], cos, sin)
        factor = jnp.where(h < heads, scale, 1.0)
        a, b = a * factor, b * factor
        qkv_ref[pl.ds(base, half), :] = a.astype(BF16)
        qkv_ref[pl.ds(base + half, half), :] = b.astype(BF16)

    values = pl.ds((heads + 1) * HEAD_SIZE, HEAD_SIZE)
    qkv_ref[values, :] = act_ref[values, :].astype(BF16)
    saves[2].start()
    saves[3].start()
    mask_ref[...] = mask_block(block)
    kv_ref[...] = qkv_ref[pl.ds(heads * HEAD_SIZE, 2 * HEAD_SIZE), :].T

    @pl.loop(0, heads)
    def _(h):
        base = pl.multiple_of(h * HEAD_SIZE, HEAD_SIZE)
        for i in range(length // block):
            cols = pl.ds(i * block, block)
            query = qkv_ref[pl.ds(base, HEAD_SIZE), cols]
            scores = []
            peak = None
            for j in range(i + 1):
                s = mm(kv_ref[pl.ds(j * block, block), :HEAD_SIZE], query)
                if i == j:
                    s = s + mask_ref[...]
                top = jnp.max(s, axis=0, keepdims=True)
                peak = top if peak is None else jnp.maximum(peak, top)
                scores.append(s)
            weights = [jnp.exp(s - peak) for s in scores]
            total = sum(jnp.sum(w, axis=0, keepdims=True) for w in weights)
            log_ref[pl.ds(h, 1), cols] = peak + jnp.log(total)
            inverse = 1.0 / total
            mixed = None
            for j in range(i + 1):
                w = (weights[j] * inverse).astype(BF16)
                v = qkv_ref[values, pl.ds(j * block, block)]
                term = mm(v, w)
                mixed = term if mixed is None else mixed + term
            out_ref[pl.ds(base, HEAD_SIZE), cols] = mixed.astype(BF16)

    def part_save(index):
        cols = piece_rows(index, tile)
        return pltpu.make_async_copy(part_ref.at[:, cols], part_hbm.at[:, cols], save_sem.at[len(saves) + index])

    tile = even_tile(width)

    @pl.loop(0, width // tile)
    def _(index):
        cols = piece_rows(index, tile)
        part_ref[:, cols] = mm(out_ref[...], wo_ref[:, cols], 0, 0).astype(BF16)
        part_save(index).start()

    gather.finish()
    for save in saves:
        save.wait()

    @pl.loop(0, width // tile)
    def _(index):
        part_save(index).wait()

    @pl.loop(1, dp // 2)
    def _(offset):
        for i in range(4):
            even_copy(i, offset).wait_send()

    @pl.loop(0, dp // 2)
    def _(offset):
        for i in range(4):
            pair_copy(i, offset).wait_send()

    if n == 4:

        @pl.when(me == 1)
        def _():
            arrived(1, 2, me + 2)
            cot_copy(True, 2).wait_send()
            far_copy(False, me + 1).wait_send()

        @pl.when(me == 2)
        def _():
            arrived(0, 2, me - 2)
            cot_copy(False, 2).wait_send()
            far_copy(True, me - 1).wait_send()

        @pl.when(me == 0)
        def _():
            far_copy(False, me + 2).wait_recv()

        @pl.when(me == n - 1)
        def _():
            far_copy(True, me - 2).wait_recv()

    else:

        @pl.when(inner)
        def _():
            arrived(0, 1, me - 1)
            arrived(1, 1, me + 1)

    @pl.when(me == 0)
    def _():
        arrived(1, 1, me + 1)

    @pl.when(me == n - 1)
    def _():
        arrived(0, 1, me - 1)

    @pl.when(me < n - 1)
    def _():
        cot_copy(True, 1).wait_send()

    @pl.when(me > 0)
    def _():
        cot_copy(False, 1).wait_send()


def cot_copy_in(line, near_hbm, shard, recv, send, step):
    part = near_hbm.at[shard]
    return line.copy(part, part, send, recv, step)


def attend(n, dp, x, gains, weights, cos, sin, cotangent, block=256, pieces=4):
    assert n <= 4 and dp % 2 == 0
    rows, width = x.shape
    length = n * rows
    q_cols, k_cols = weights[0].shape[1], weights[1].shape[0]
    cols_in = q_cols + 2 * k_cols
    heads = cols_in // HEAD_SIZE - 2
    any_spec = pl.BlockSpec(memory_space=pl.ANY)
    dma = pltpu.SemaphoreType.DMA
    return pl.pallas_call(
        functools.partial(attend_kernel, n, dp, heads, block, pieces),
        out_shape=(
            jax.ShapeDtypeStruct((1, width), F32),
            jax.ShapeDtypeStruct((1, width), F32),
            jax.ShapeDtypeStruct((length, 2 * HEAD_SIZE), BF16),
            jax.ShapeDtypeStruct((heads * HEAD_SIZE, length), BF16),
            jax.ShapeDtypeStruct((heads, length), F32),
            jax.ShapeDtypeStruct((length, width), BF16),
            jax.ShapeDtypeStruct((cols_in, length), BF16),
            jax.ShapeDtypeStruct((length, width), BF16),
            jax.ShapeDtypeStruct((width, cols_in), BF16),
            jax.ShapeDtypeStruct((q_cols, width), BF16),
            jax.ShapeDtypeStruct((n,) + cotangent.shape, BF16),
            jax.ShapeDtypeStruct((n, rows, width), BF16),
        ),
        in_specs=[VMEM_SPEC] * 4 + [any_spec] * 5,
        out_specs=(VMEM_SPEC,) * 5 + (any_spec,) * 7,
        scratch_shapes=[
            pltpu.VMEM((length, width), BF16),
            pltpu.VMEM((cols_in, length), BF16),
            pltpu.VMEM((length, width), BF16),
            pltpu.VMEM((width, cols_in), BF16),
            pltpu.VMEM((q_cols, width), BF16),
            pltpu.VMEM((n, rows, width), BF16),
            pltpu.VMEM((cols_in, length), F32),
            pltpu.VMEM((block, block), F32),
            pltpu.VMEM((n * dp, 1, gains.shape[1]), F32),
        ]
        + [pltpu.VMEM((dp,) + w.shape, BF16) for w in weights]
        + sems(n, pieces)
        + [dma((n * dp,)), dma((n * dp,)), dma((2, 4, dp // 2)), dma((2, 4, dp // 2)), dma((4,))]
        + [dma((2, 2)), dma((2, 2)), dma((2,)), dma((2,)), dma((5 + width // even_tile(width),))],
        compiler_params=comm_params(1),
        cost_estimate=pl.CostEstimate(
            flops=2 * length * width * (cols_in + q_cols),
            bytes_accessed=350 * 1024 * 1024,
            transcendentals=heads * length * length,
        ),
        name="attend",
    )(x, gains, cos, sin, cotangent, *weights)


def attend_back_kernel(
    n, heads, block, pieces, kv_ref, log_ref, cos_ref, sin_ref,
    mid_hbm, low_hbm, hid_hbm, w_mlp_hbm, wo_hbm, w_hbm, qkv_hbm, out_hbm, norm_hbm,
    rows_ref, part_hbm, wgrad_hbm,
    mid_ref, part_ref, seq, hid, w_down, down_ref, buf, wo_ref, w_ref, qkv_ref, out_ref, norm_ref,
    dkv, mask_ref, grad_ref, dqkv_ref, wgrad, ssend, srecv, gsend, grecv, load_sem, save_sem,
):
    half = HEAD_SIZE // 2
    rows_all, width = mid_ref.shape
    units = hid.shape[2]
    cols_in = qkv_ref.shape[0]
    scale = 1.0 / math.sqrt(HEAD_SIZE)
    me = lax.axis_index("tensor")
    size = rows_all // pieces
    own_rows, early_rows = pl.ds(EARLY * size, rows_all - EARLY * size), pl.ds(0, EARLY * size)
    pairs = (
        (low_hbm.at[me, own_rows], seq.at[me, own_rows]),
        (hid_hbm, hid),
        (w_mlp_hbm.at[:, pl.ds(2 * units, units)], w_down),
        (wo_hbm, wo_ref),
        (qkv_hbm, qkv_ref),
        (out_hbm, out_ref),
        (w_hbm, w_ref),
        (norm_hbm, norm_ref),
        (mid_hbm, mid_ref),
    )
    if EARLY:
        pairs += ((low_hbm.at[:, early_rows], seq.at[:, early_rows]),)
    loads = [pltpu.make_async_copy(src, dst, load_sem.at[i]) for i, (src, dst) in enumerate(pairs)]
    for load in loads:
        load.start()
    line = Line(n)
    line.barrier()
    scatter = Scatter(line, down_ref, buf, ssend, srecv, pieces)
    gather = Gather(line, seq, gsend, grecv, pieces)
    loads[0].wait()

    @pl.loop(EARLY, pieces)
    def _(piece):
        gather.start_own(piece)

    dkv[...] = jnp.zeros_like(dkv)
    mask_ref[...] = mask_block(block)
    keys = pl.ds(heads * HEAD_SIZE, HEAD_SIZE)

    def project(shard):
        grad_ref[:, piece_rows(shard, rows_all)] = mm(wo_ref[...], seq[shard], 1, 1).astype(BF16)

    tile = even_tile(width)

    def start_sums():
        loads[1].wait()
        loads[2].wait()

        @pl.loop(0, pieces)
        def _(piece):
            rows = scatter.rows(piece)

            @pl.loop(0, width // tile)
            def _(index):
                cols = piece_rows(index, tile)
                value = hid[:, rows, :].reshape(n * scatter.size, units)
                value = mm(value, w_down[cols, :], 1, 1).astype(BF16)
                down_ref[:, rows, cols] = value.reshape(n, scatter.size, tile)

            scatter.start_ends(piece)

    def sum_piece(piece):
        scatter.middle(piece)
        rows = scatter.rows(piece)

        def store(total):
            rows_ref[rows, :] = (mid_ref[rows, :] + total).astype(BF16)

        scatter.result(piece, store)

    start_sums()
    for load in loads[3:]:
        load.wait()

    def attention_rows(i):
        cols = pl.ds(i * block, block)
        cos, sin = cos_ref[:, cols], sin_ref[:, cols]

        @pl.loop(0, heads)
        def _(h):
            base = pl.multiple_of(h * HEAD_SIZE, HEAD_SIZE)
            mine = pl.ds(base, HEAD_SIZE)
            query = qkv_ref[mine, cols]
            grad = grad_ref[mine, cols]
            delta = jnp.sum(
                grad.astype(F32) * out_ref[mine, cols].astype(F32), axis=0, keepdims=True
            )
            log_total = log_ref[pl.ds(h, 1), cols]
            dquery = None
            for j in range(i + 1):
                rows = pl.ds(j * block, block)
                s = mm(kv_ref[rows, :HEAD_SIZE], query)
                if i == j:
                    s = s + mask_ref[...]
                probs = jnp.exp(s - log_total)
                dprobs = mm(kv_ref[rows, HEAD_SIZE:], grad)
                dscores = (probs * (dprobs - delta)).astype(BF16)
                dkv[0, rows, :] += mm(dscores, query, 1, 1)
                dkv[1, rows, :] += mm(probs.astype(BF16), grad, 1, 1)
                term = mm(qkv_ref[keys, rows], dscores)
                dquery = term if dquery is None else dquery + term
            dquery = dquery * scale
            a, b = unrotate(dquery[:half], dquery[half:], cos, sin)
            dqkv_ref[pl.ds(base, half), cols] = a.astype(BF16)
            dqkv_ref[pl.ds(base + half, half), cols] = b.astype(BF16)

    @pl.loop(0, 2 * n - 1)
    def _(turn):
        hop = (turn + 1) // 2
        leftward = lax.rem(turn, 2) == 1
        shard = jnp.where(leftward, me - hop, me + hop)

        @pl.when(leftward)
        def _():
            @pl.loop(EARLY, pieces)
            def _(piece):
                gather.receive(hop, piece)

        @pl.when(within(shard, n))
        def _():
            project(shard)
            for i in range(n):

                @pl.when(shard == i)
                def _():
                    attention_rows(i)

        @pl.when(jnp.logical_not(leftward) & within(hop - 1, min(n, pieces) - 1))
        def _():
            sum_piece(hop - 1)

    dkeys = dkv[0].T
    a, b = unrotate(dkeys[:half], dkeys[half:], cos_ref[...], sin_ref[...])
    dqkv_ref[pl.ds(heads * HEAD_SIZE, half), :] = a.astype(BF16)
    dqkv_ref[pl.ds(heads * HEAD_SIZE + half, half), :] = b.astype(BF16)
    dqkv_ref[pl.ds((heads + 1) * HEAD_SIZE, HEAD_SIZE), :] = dkv[1].T.astype(BF16)

    def part_save(index):
        cols = piece_rows(index, tile)
        return pltpu.make_async_copy(part_ref.at[:, cols], part_hbm.at[:, cols], save_sem.at[0, index])

    def wgrad_save(index):
        rows = piece_rows(index, tile)
        return pltpu.make_async_copy(wgrad.at[rows, :], wgrad_hbm.at[rows, :], save_sem.at[1, index])

    @pl.loop(0, width // tile)
    def _(index):
        cols = piece_rows(index, tile)
        part_ref[:, cols] = mm(dqkv_ref[...], w_ref[cols, :], 0, 1).astype(BF16)
        part_save(index).start()

    @pl.loop(0, width // tile)
    def _(index):
        cols = piece_rows(index, tile)
        wgrad[cols, :cols_in] = mm(norm_ref[:, cols], dqkv_ref[...], 0, 1).astype(BF16)
        for shard in range(n):
            term = mm(seq[shard, :, cols], out_ref[:, shard * rows_all : (shard + 1) * rows_all], 0, 1)
            total = term if shard == 0 else total + term
        wgrad[cols, cols_in:] = total.astype(BF16)
        wgrad_save(index).start()

    for piece in range(min(n, pieces) - 1, pieces):
        sum_piece(piece)
    scatter.finish()
    gather.finish(EARLY, pieces)

    @pl.loop(0, width // tile)
    def _(index):
        part_save(index).wait()
        wgrad_save(index).wait()


def attend_back(
    n, mid, kv, log_total, cos, sin, low, hidden, w_mlp, w_out, w_qkv, qkv, out, norm, pieces=4
):
    rows, width = mid.shape
    block = rows
    length = n * rows
    cols_in = qkv.shape[0]
    heads = cols_in // HEAD_SIZE - 2
    units = hidden.shape[2]
    any_spec = pl.BlockSpec(memory_space=pl.ANY)
    wgrad_shape = (width, cols_in + w_out.shape[0])
    return pl.pallas_call(
        functools.partial(attend_back_kernel, n, heads, block, pieces),
        out_shape=(
            jax.ShapeDtypeStruct((rows, width), BF16),
            jax.ShapeDtypeStruct((length, width), BF16),
            jax.ShapeDtypeStruct(wgrad_shape, BF16),
        ),
        in_specs=[VMEM_SPEC] * 4 + [any_spec] * 9,
        out_specs=(VMEM_SPEC,) + (any_spec,) * 2,
        scratch_shapes=[
            pltpu.VMEM(mid.shape, F32),
            pltpu.VMEM((length, width), BF16),
            pltpu.VMEM((n, rows, width), BF16),
            pltpu.VMEM((n, rows, units), BF16),
            pltpu.VMEM((width, units), BF16),
            pltpu.VMEM((n, rows, width), BF16),
            pltpu.VMEM((n + 1, rows, width), BF16),
            pltpu.VMEM(w_out.shape, BF16),
            pltpu.VMEM(w_qkv.shape, BF16),
            pltpu.VMEM(qkv.shape, BF16),
            pltpu.VMEM(out.shape, BF16),
            pltpu.VMEM(norm.shape, BF16),
            pltpu.VMEM((2, length, HEAD_SIZE), F32),
            pltpu.VMEM((block, block), F32),
            pltpu.VMEM((heads * HEAD_SIZE, length), BF16),
            pltpu.VMEM((cols_in, length), BF16),
            pltpu.VMEM(wgrad_shape, BF16),
        ]
        + sems(n, pieces) * 2
        + [pltpu.SemaphoreType.DMA((9,)), pltpu.SemaphoreType.DMA((2, width // even_tile(width)))],
        compiler_params=comm_params(3),
        cost_estimate=pl.CostEstimate(
            flops=6 * length * width * wgrad_shape[1],
            bytes_accessed=350 * 1024 * 1024,
            transcendentals=heads * length * length,
        ),
        name="attend_back",
    )(kv, log_total, cos, sin, mid, low, hidden, w_mlp, w_out, w_qkv, qkv, out, norm)


def local(
    n, dp, x, gain_attn, gain_mlp, w_query, w_key, w_value, w_out, w_gate, w_up, w_down, cotangent
):
    rows, _ = x.shape
    length = n * rows
    per = gain_attn.shape[0]
    packed = 2 * per + (-2 * per) % LANES

    mlp_all = lax.all_gather(
        jnp.concatenate([w_gate, w_up, w_down.T], axis=1), "dp", axis=0, tiled=True
    )
    gains = [gain_attn, gain_mlp]
    if packed > 2 * per:
        gains.append(jnp.zeros((packed - 2 * per,), F32))
    cos, sin = tables(length)
    full_attn, full_mlp, kv, attended, log_total, norm_attn, qkv, out_part, w_qkv, w_out_all, near, x_seq = attend(
        n,
        dp,
        x,
        jnp.concatenate(gains).reshape(1, packed),
        (w_query, w_key.T, w_value.T, w_out),
        cos,
        sin,
        cotangent,
    )
    dgain_mlp, mid, grad_mid, hidden, mlp_grad, grad_low = mlp(
        n, out_part, x, full_mlp, mlp_all, cotangent, near
    )
    mlp_grad = lax.psum_scatter(mlp_grad, "dp", scatter_dimension=0, tiled=True)
    block_output, attn_part, attn_grad = attend_back(
        n, mid, kv, log_total, cos, sin, grad_low, hidden, mlp_all, w_out_all, w_qkv, qkv, attended, norm_attn
    )
    attn_grad = lax.psum_scatter(attn_grad, "dp", scatter_dimension=0, tiled=True)
    input_grad, dgains = sum_input_grad(
        n, dp, attn_part, x, full_attn, grad_mid, dgain_mlp, x_seq, packed
    )
    gate, up, down, query, key, value, out, dgain_attn, dgain_mlp, block_output, input_grad = widen(
        mlp_grad, attn_grad, dgains, block_output, input_grad, per, w_query.shape[1], w_key.shape[1]
    )
    return (
        block_output,
        input_grad,
        dgain_attn.reshape(per),
        dgain_mlp.reshape(per),
        query,
        key.T,
        value.T,
        out,
        gate,
        up,
        down,
    )


def solution(mesh):
    rows = P(("dp", "tensor"), None)
    gain = P(("dp", "tensor"))
    into = P("dp", "tensor")
    back = P("tensor", "dp")
    in_specs = (rows, gain, gain, into, into, into, back, into, into, back, rows)
    out_specs = (rows, rows, gain, gain, into, into, into, back, into, into, back)

    def body(*args):
        return local(mesh.shape["tensor"], mesh.shape["dp"], *args)

    return jax.shard_map(body, mesh=mesh, in_specs=in_specs, out_specs=out_specs, check_vma=False)
```

```python
import functools
import math

import jax
import jax.numpy as jnp
from jax import lax
from jax.experimental import pallas as pl
from jax.experimental.pallas import tpu as pltpu
from jax.sharding import PartitionSpec as P


HEAD_SIZE = 64
EPS = 1e-05
ROPE_BASE = 10000.0
NEG_LARGE = -1e30
LANES = 128
MESH = pl.DeviceIdType.MESH
F32 = jnp.float32
BF16 = jnp.bfloat16
VMEM_SPEC = pl.BlockSpec(memory_space=pltpu.VMEM)
FAR_DONE = 3


def tables(sequence_length):
    half = HEAD_SIZE // 2
    frequency = ROPE_BASE ** (-(jnp.arange(half, dtype=F32) * 2.0) / HEAD_SIZE)
    angles = frequency[:, None] * jnp.arange(sequence_length, dtype=F32)[None, :]
    return jnp.cos(angles), jnp.sin(angles)


def dims(contract_left, contract_right):
    return (((contract_left,), (contract_right,)), ((), ()))


def mm(left, right, contract_left=1, contract_right=0):
    return lax.dot_general(
        left, right, dims(contract_left, contract_right), preferred_element_type=F32
    )


def piece_rows(piece, size):
    return pl.ds(pl.multiple_of(piece * size, size), size)


class Line:
    def __init__(self, n):
        self.n = n
        self.me = lax.axis_index("tensor")

    def barrier(self):
        barrier = pltpu.get_barrier_semaphore()
        n, me = self.n, self.me

        @pl.when(me > 0)
        def _():
            pl.semaphore_signal(barrier, inc=1, device_id={"tensor": me - 1}, device_id_type=MESH)

        @pl.when(me < n - 1)
        def _():
            pl.semaphore_signal(barrier, inc=1, device_id={"tensor": me + 1}, device_id_type=MESH)

        inner = (me > 0) & (me < n - 1)

        @pl.when(inner)
        def _():
            pl.semaphore_wait(barrier, 2)

        @pl.when(jnp.logical_not(inner))
        def _():
            pl.semaphore_wait(barrier, 1)

    def copy(self, src, dst, send, recv, step):
        return pltpu.make_async_remote_copy(
            src_ref=src,
            dst_ref=dst,
            send_sem=send,
            recv_sem=recv,
            device_id={"tensor": self.me + step},
            device_id_type=MESH,
        )


class Gather:
    def __init__(self, line, buf, send, recv, pieces):
        self.line, self.buf, self.send, self.recv, self.pieces = line, buf, send, recv, pieces
        self.size = buf.shape[1] // pieces

    def message(self, right, hop, piece, shard):
        d = 0 if right else 1
        part = self.buf.at[shard, piece_rows(piece, self.size)]
        return self.line.copy(
            part, part, self.send.at[d, hop - 1, piece], self.recv.at[d, hop - 1, piece], 1 if right else -1
        )

    def start_own(self, piece):
        line = self.line
        me, n = line.me, line.n

        @pl.when(me < n - 1)
        def _():
            self.message(True, 1, piece, me).start()

        @pl.when(me > 0)
        def _():
            self.message(False, 1, piece, me).start()

    def start_hop(self, hop, piece):
        line = self.line
        me, n = line.me, line.n

        @pl.when((me - (hop - 1) >= 0) & (me < n - 1))
        def _():
            self.message(True, hop, piece, me - (hop - 1)).start()

        @pl.when((me + (hop - 1) <= n - 1) & (me > 0))
        def _():
            self.message(False, hop, piece, me + (hop - 1)).start()

    def receive(self, hop, piece, use=None):
        line = self.line
        me, n = line.me, line.n

        @pl.when(me - hop >= 0)
        def _():
            shard = me - hop
            self.message(True, hop, piece, shard).wait_recv()
            if not isinstance(hop, int) or hop < n - 1:

                @pl.when((me < n - 1) & (hop < n - 1))
                def _():
                    self.message(True, hop + 1, piece, shard).start()

            if use is not None:
                use(shard, piece)

        @pl.when(me + hop <= n - 1)
        def _():
            shard = me + hop
            self.message(False, hop, piece, shard).wait_recv()
            if not isinstance(hop, int) or hop < n - 1:

                @pl.when((me > 0) & (hop < n - 1))
                def _():
                    self.message(False, hop + 1, piece, shard).start()

            if use is not None:
                use(shard, piece)

    def finish(self, first_piece=0, end_piece=None):
        line = self.line
        me, n = line.me, line.n

        @pl.loop(first_piece, self.pieces if end_piece is None else end_piece)
        def _(piece):
            for hop in range(1, n):

                @pl.when((me - (hop - 1) >= 0) & (me < n - 1))
                def _():
                    self.message(True, hop, piece, me - (hop - 1)).wait_send()

                @pl.when((me + (hop - 1) <= n - 1) & (me > 0))
                def _():
                    self.message(False, hop, piece, me + (hop - 1)).wait_send()


class Scatter:
    def __init__(self, line, part, buf, send, recv, pieces):
        self.line, self.part, self.buf, self.pieces = line, part, buf, pieces
        self.send, self.recv = send, recv
        self.size = part.shape[1] // pieces

    def rows(self, piece):
        return piece_rows(piece, self.size)

    def outgoing(self, d, target, piece, from_part=False):
        rows, line = self.rows(piece), self.line
        src = (self.part if from_part else self.buf).at[target, rows]
        slot = target
        if d == 1:
            slot = jnp.where(target == line.me - 1, line.n, target)
        return line.copy(
            src,
            self.buf.at[slot, rows],
            self.send.at[d, target, piece],
            self.recv.at[d, target, piece],
            1 if d == 0 else -1,
        )

    def incoming(self, d, target, slot, piece):
        part = self.buf.at[slot, self.rows(piece)]
        return self.line.copy(
            part, part, self.send.at[d, target, piece], self.recv.at[d, target, piece], 1 if d == 0 else -1
        )

    def start_ends(self, piece):
        line = self.line
        me, n = line.me, line.n

        @pl.when(me == 0)
        def _():
            for target in range(n - 1, 0, -1):
                self.outgoing(0, target, piece, True).start()

        @pl.when(me == n - 1)
        def _():
            for target in range(0, n - 1):
                self.outgoing(1, target, piece, True).start()

    def pass_on(self, d, target, piece):
        buf = self.buf
        self.incoming(d, target, target, piece).wait_recv()
        rows = self.rows(piece)
        total = buf[target, rows].astype(F32) + self.part[target, rows].astype(F32)
        buf[target, rows] = total.astype(BF16)
        self.outgoing(d, target, piece).start()

    def passes(self, piece, right, targets, where):
        line = self.line
        me, n = line.me, line.n
        for target in targets:
            held = (me > 0) & (me < target) if right else (me < n - 1) & (me > target)

            @pl.when(where & held)
            def _():
                self.pass_on(0 if right else 1, target, piece)

    def first(self, piece):
        n, left_half = self.line.n, self.line.me < self.line.n // 2
        self.passes(piece, True, (n - 1,), left_half)
        self.passes(piece, False, (0,), jnp.logical_not(left_half))

    def rest(self, piece):
        n, left_half = self.line.n, self.line.me < self.line.n // 2
        right_half = jnp.logical_not(left_half)
        self.passes(piece, True, range(n - 2, 0, -1), left_half)
        self.passes(piece, False, range(1, n - 1), right_half)
        self.passes(piece, False, range(0, n - 1), left_half)
        self.passes(piece, True, range(n - 1, 0, -1), right_half)

    def middle(self, piece):
        self.first(piece)
        self.rest(piece)

    def result(self, piece, store):
        line = self.line
        me, n = line.me, line.n
        rows = self.rows(piece)

        @pl.when(me > 0)
        def _():
            self.incoming(0, me, me, piece).wait_recv()

        @pl.when(me < n - 1)
        def _():
            self.incoming(1, me, n, piece).wait_recv()

        own = self.part[me, rows].astype(F32)

        @pl.when(me == 0)
        def _():
            store(own + self.buf[n, rows].astype(F32))

        @pl.when(me == n - 1)
        def _():
            store(own + self.buf[me, rows].astype(F32))

        @pl.when((me > 0) & (me < n - 1))
        def _():
            store(own + self.buf[me, rows].astype(F32) + self.buf[n, rows].astype(F32))

    def finish(self, ends=True, middles=True):
        line = self.line
        me, n = line.me, line.n
        inner = (me > 0) & (me < n - 1)

        @pl.when((inner & middles) | (jnp.logical_not(inner) & ends))
        def _():
            @pl.loop(0, self.pieces)
            def _(piece):
                for target in range(1, n):

                    @pl.when(me < target)
                    def _():
                        self.outgoing(0, target, piece).wait_send()

                for target in range(0, n - 1):

                    @pl.when(me > target)
                    def _():
                        self.outgoing(1, target, piece).wait_send()


def within(piece, pieces):
    return (piece >= 0) & (piece < pieces)


def sems(n, pieces):
    return [pltpu.SemaphoreType.DMA((2, n, pieces)), pltpu.SemaphoreType.DMA((2, n, pieces))]


def comm_params(collective_id):
    return pltpu.CompilerParams(
        collective_id=collective_id, has_side_effects=True, vmem_limit_bytes=60 * 1024 * 1024
    )


def exchange_all(n, dp, send_row, recv_row, send, recv, start_only=False, wait_only=False):
    devices = n * dp
    me = lax.axis_index("dp") * n + lax.axis_index("tensor")

    def message(offset, peer, source):
        return pltpu.make_async_remote_copy(
            src_ref=send_row(peer),
            dst_ref=recv_row(source),
            send_sem=send.at[offset],
            recv_sem=recv.at[offset],
            device_id={"dp": peer // n, "tensor": peer % n},
            device_id_type=MESH,
        )

    if not wait_only:

        @pl.loop(1, devices)
        def _(offset):
            message(offset, lax.rem(me + offset, devices), me).start()

    if not start_only:

        @pl.loop(1, devices)
        def _(offset):
            copy = message(offset, lax.rem(me + offset, devices), me)
            copy.wait_send()
            copy.wait_recv()


def barrier_all(n, dp):
    devices = n * dp
    me = lax.axis_index("dp") * n + lax.axis_index("tensor")
    barrier = pltpu.get_barrier_semaphore()

    @pl.loop(1, devices)
    def _(offset):
        peer = lax.rem(me + offset, devices)
        pl.semaphore_signal(
            barrier, inc=1, device_id={"dp": peer // n, "tensor": peer % n}, device_id_type=MESH
        )

    pl.semaphore_wait(barrier, devices - 1)


def even_tile(extent):
    return 512 if extent % 512 == 0 else extent


def tiles(extent, size):
    return [(start, min(size, extent - start)) for start in range(0, extent, size)]


def mlp_kernel(
    n, pieces, gain_ref, part_hbm, x_hbm, w_hbm, cot_hbm, near_hbm,
    dgain_ref, mid_hbm, grad_hbm, hid_hbm, wgrad_hbm, low_hbm,
    part_ref, x_ref, mid_ref, grad_ref, w, cot, seq, buf, npart, buf_back, hid, dgate, dup, stage, inv_ref,
    ssend, srecv, gsend, grecv, bsend, brecv, csend, crecv, local_sem, stage_sem, part_sem,
):
    line = Line(n)
    me = line.me
    rows_all, width = part_ref.shape[1:]

    def part_load(piece):
        rows = piece_rows(piece, rows_all // pieces)
        return pltpu.make_async_copy(part_hbm.at[:, rows], part_ref.at[:, rows], part_sem.at[0, piece])

    def piece_save(which, ref, hbm, piece):
        rows = piece_rows(piece, rows_all // pieces)
        return pltpu.make_async_copy(ref.at[rows], hbm.at[rows], part_sem.at[which, piece])

    x_load = pltpu.make_async_copy(x_hbm, x_ref, local_sem.at[3])
    for piece in range(pieces):
        part_load(piece).start()
    x_load.start()

    units = hid.shape[2]
    weight_load = pltpu.make_async_copy(w_hbm, w, local_sem.at[0])
    own_load = pltpu.make_async_copy(cot_hbm, cot.at[me], local_sem.at[1])
    inner = (me > 0) & (me < n - 1)

    def near_load(shard, count):
        rows = pl.ds(0, count)
        return pltpu.make_async_copy(near_hbm.at[shard, rows], cot.at[shard, rows], local_sem.at[5 + shard])

    def each_near(act):
        for shard in range(n):
            here = (me != shard) & (inner | (me - shard == 1) | (shard - me == 1))

            @pl.when(here)
            def _():
                act(near_load(shard, rows_all))

            if n == 4:

                @pl.when(jnp.logical_not(inner) & ((me - shard == 2) | (shard - me == 2)))
                def _():
                    act(near_load(shard, rows_all // pieces * FAR_DONE))

    each_near(lambda copy: copy.start())
    own_load.start()
    weight_load.start()
    line.barrier()
    scatter = Scatter(line, part_ref, buf, ssend, srecv, pieces)
    gather = Gather(line, seq, gsend, grecv, pieces)
    scatter_back = Scatter(line, npart, buf_back, bsend, brecv, pieces)
    cot_gather = Gather(line, cot, csend, crecv, pieces)
    size = scatter.size
    part_load(0).wait()
    scatter.start_ends(0)
    for piece in range(1, pieces):
        part_load(piece).wait()
    x_load.wait()
    dgain_ref[...] = jnp.zeros_like(dgain_ref)

    each_near(lambda copy: copy.wait())

    def still_far(hop, piece):
        return (piece >= FAR_DONE) if hop == 2 and n == 4 else (piece >= 0)

    def each_far(piece, act):
        for hop in range(2, n):

            @pl.when((me == n - 2) & still_far(hop, piece))
            def _():
                act(True, hop, me - (hop - 1))

            @pl.when((me == 1) & still_far(hop, piece))
            def _():
                act(False, hop, me + (hop - 1))

    def far_start(piece):
        each_far(piece, lambda right, hop, shard: cot_gather.message(right, hop, piece, shard).start())

    def far_sent(piece):
        each_far(piece, lambda right, hop, shard: cot_gather.message(right, hop, piece, shard).wait_send())

    def far_arrived(piece):
        for hop in range(2, n):

            @pl.when((me == n - 1) & still_far(hop, piece))
            def _():
                cot_gather.message(True, hop, piece, me - hop).wait_recv()

            @pl.when((me == 0) & still_far(hop, piece))
            def _():
                cot_gather.message(False, hop, piece, me + hop).wait_recv()

    for piece in range(min(3, pieces)):
        far_start(jnp.int32(piece))

    def norm(piece):
        rows = scatter.rows(piece)

        def store(total):
            mid_ref[rows, :] = x_ref[rows, :].astype(F32) + total

        scatter.result(piece, store)
        mid = mid_ref[rows, :]
        inv = lax.rsqrt(jnp.mean(mid * mid, axis=1, keepdims=True) + EPS)
        inv_ref[rows, :] = jnp.broadcast_to(inv, (size, LANES))
        seq[me, rows, :] = (mid * inv * gain_ref[...]).astype(BF16)
        piece_save(1, mid_ref, mid_hbm, piece).start()

    def back(piece):
        rows = scatter.rows(piece)

        def store(total):
            grad_ref[rows, :] = total

        scatter_back.result(piece, store)
        grad = grad_ref[rows, :]
        mid = mid_ref[rows, :]
        inv = inv_ref[rows, 0:1]
        dgain_ref[...] += jnp.sum(grad * mid * inv, axis=0, keepdims=True)
        scaled = grad * gain_ref[...]
        mean = jnp.mean(scaled * mid, axis=1, keepdims=True)
        out = cot[me, rows, :].astype(F32) + inv * (scaled - mid * (inv * inv * mean))
        grad_ref[rows, :] = out
        buf[me, rows, :] = out.astype(BF16)
        piece_save(2, grad_ref, grad_hbm, piece).start()

    def flat(ref, piece):
        value = ref[:, scatter.rows(piece), :]
        return value.reshape(n * size, value.shape[2])

    def feed(piece):
        rows = scatter.rows(piece)
        for start, count in tiles(units, 512):
            x = flat(seq, piece)
            gate = mm(x, w[:, start : start + count])
            up = mm(x, w[:, units + start : units + start + count])
            dhidden = mm(flat(cot, piece), w[:, 2 * units + start : 2 * units + start + count])
            sigmoid = jax.nn.sigmoid(gate)
            act = gate * sigmoid
            cols = slice(start, start + count)
            shape = (n, size, count)
            hid[:, rows, cols] = (act * up).astype(BF16).reshape(shape)
            dup[:, rows, cols] = (dhidden * act).astype(BF16).reshape(shape)
            dgate[:, rows, cols] = (
                (dhidden * up * sigmoid * (1.0 + gate * (1.0 - sigmoid))).astype(BF16).reshape(shape)
            )
        tile = even_tile(width)

        @pl.loop(0, width // tile)
        def _(index):
            cols = piece_rows(index, tile)
            total = mm(flat(dgate, piece), w[cols, :units], 1, 1)
            total += mm(flat(dup, piece), w[cols, units : 2 * units], 1, 1)
            npart[:, rows, cols] = total.astype(BF16).reshape(n, size, tile)

    step_rows = min(LANES, width)
    count = width // step_rows

    def save(index, slot):
        return pltpu.make_async_copy(
            stage.at[slot],
            wgrad_hbm.at[pl.ds(pl.multiple_of(index * step_rows, step_rows), step_rows), :],
            stage_sem.at[slot],
        )

    def weight_grads(events):
        @pl.loop(0, count)
        def _(index):
            for at, event in events:

                @pl.when(index == at)
                def _():
                    event()

            slot = lax.rem(index, 2)
            cols = pl.ds(pl.multiple_of(index * step_rows, step_rows), step_rows)

            @pl.when(index >= 2)
            def _():
                save(index - 2, slot).wait()

            x = seq[:, :, cols].reshape(n * rows_all, step_rows)
            g = cot[:, :, cols].reshape(n * rows_all, step_rows)
            for at, left, right in ((0, x, dgate), (1, x, dup), (2, g, hid)):
                value = right[...].reshape(n * rows_all, units)
                stage[slot, :, at * units : (at + 1) * units] = mm(left, value, 0, 0).astype(BF16)
            save(index, slot).start()

    hid_save = pltpu.make_async_copy(hid, hid_hbm, local_sem.at[2])

    def receive_rows(hop, piece):
        @pl.when(within(piece, pieces))
        def _():
            gather.receive(hop, piece)

    @pl.loop(0, pieces + n - 1)
    def _(step):
        first = step < pieces
        ready = step - (n - 1)
        receive_rows(n - 1, ready)

        @pl.when(step + 1 < pieces)
        def _():
            scatter.start_ends(step + 1)

        @pl.when(ready == 0)
        def _():
            own_load.wait()
            weight_load.wait()

        @pl.when(ready >= 0)
        def _():
            far_arrived(ready)
            feed(ready)
            scatter_back.start_ends(ready)

        @pl.when(first)
        def _():
            scatter.middle(step)

            @pl.when(step + 3 < pieces)
            def _():
                far_start(step + 3)

        for hop in range(n - 2, 1, -1):
            receive_rows(hop, step - hop)

        @pl.when(ready >= 1)
        def _():
            scatter_back.middle(ready - 1)

        if n > 2:
            receive_rows(1, step - 1)

        @pl.when(first)
        def _():
            norm(step)
            gather.start_own(step)

        @pl.when(ready == 2)
        def _():
            scatter.finish(ends=False)

        @pl.when(ready >= 2)
        def _():
            back(ready - 2)

    hid_save.start()
    last = pieces - 1

    events = [
        (count // 4, lambda: scatter_back.first(last)),
        (count * 5 // 8, lambda: scatter_back.rest(last)),
    ]
    weight_grads(events)

    @pl.loop(max(last - 1, 0), pieces)
    def _(piece):
        back(piece)

    low_save = pltpu.make_async_copy(buf.at[me], low_hbm, local_sem.at[4])
    low_save.start()
    scatter.finish(middles=False)
    gather.finish()
    scatter_back.finish()

    @pl.loop(0, pieces)
    def _(piece):
        far_sent(piece)
        piece_save(1, mid_ref, mid_hbm, piece).wait()
        piece_save(2, grad_ref, grad_hbm, piece).wait()

    low_save.wait()
    hid_save.wait()
    for index in range(max(count - 2, 0), count):
        save(index, index % 2).wait()


def mlp(n, part, x, gain, weights, cotangent, near, pieces=4):
    rows, width = x.shape
    units = weights.shape[1] // 3
    any_spec = pl.BlockSpec(memory_space=pl.ANY)
    return pl.pallas_call(
        functools.partial(mlp_kernel, n, pieces),
        out_shape=(
            jax.ShapeDtypeStruct((1, width), F32),
            jax.ShapeDtypeStruct((rows, width), F32),
            jax.ShapeDtypeStruct((rows, width), F32),
            jax.ShapeDtypeStruct((n, rows, units), BF16),
            jax.ShapeDtypeStruct((width, 3 * units), BF16),
            jax.ShapeDtypeStruct((rows, width), BF16),
        ),
        in_specs=[VMEM_SPEC] + [any_spec] * 5,
        out_specs=(VMEM_SPEC,) + (any_spec,) * 5,
        scratch_shapes=[
            pltpu.VMEM((n, rows, width), BF16),
            pltpu.VMEM((rows, width), BF16),
            pltpu.VMEM((rows, width), F32),
            pltpu.VMEM((rows, width), F32),
            pltpu.VMEM((width, 3 * units), BF16),
            pltpu.VMEM((n, rows, width), BF16),
            pltpu.VMEM((n, rows, width), BF16),
            pltpu.VMEM((n + 1, rows, width), BF16),
            pltpu.VMEM((n, rows, width), BF16),
            pltpu.VMEM((n + 1, rows, width), BF16),
            pltpu.VMEM((n, rows, units), BF16),
            pltpu.VMEM((n, rows, units), BF16),
            pltpu.VMEM((n, rows, units), BF16),
            pltpu.VMEM((2, min(LANES, width), 3 * units), BF16),
            pltpu.VMEM((rows, LANES), F32),
        ]
        + sems(n, pieces) * 4
        + [pltpu.SemaphoreType.DMA((5 + n,)), pltpu.SemaphoreType.DMA((2,)), pltpu.SemaphoreType.DMA((3, pieces))],
        compiler_params=pltpu.CompilerParams(
            collective_id=2, has_side_effects=True, vmem_limit_bytes=67043328
        ),
        cost_estimate=pl.CostEstimate(
            flops=18 * n * rows * width * units, bytes_accessed=500 * 1024 * 1024, transcendentals=0
        ),
        name="mlp",
    )(gain, part.reshape(n, rows, width), x, weights, cotangent, near)


def last_kernel(
    n, dp, pieces, gain_ref, dgain_mlp_ref, part_hbm, x_hbm, grad_mid_hbm, seq_hbm, out_ref, gains_ref,
    part_ref, x_ref, grad_mid_ref, seq_ref, total_ref, dgain_ref, packed, held, buf, ssend, srecv, gsend, grecv, load_sem,
):
    def part_load(piece):
        rows = piece_rows(piece, part_ref.shape[1] // pieces)
        return pltpu.make_async_copy(part_hbm.at[:, rows], part_ref.at[:, rows], load_sem.at[2 + piece])

    others = [
        pltpu.make_async_copy(x_hbm, x_ref, load_sem.at[0]),
        pltpu.make_async_copy(grad_mid_hbm, grad_mid_ref, load_sem.at[1]),
        pltpu.make_async_copy(seq_hbm, seq_ref, load_sem.at[2 + pieces]),
    ]
    for piece in range(pieces):
        part_load(piece).start()
    for load in others:
        load.start()
    line = Line(n)
    all_me = lax.axis_index("dp") * n + line.me
    barrier_all(n, dp)
    scatter = Scatter(line, part_ref, buf, ssend, srecv, pieces)
    part_load(0).wait()
    scatter.start_ends(0)
    for piece in range(1, pieces):
        part_load(piece).wait()
    for load in others:
        load.wait()
    dgain_ref[...] = jnp.zeros_like(dgain_ref)
    packed[...] = jnp.zeros_like(packed)

    width = x_ref.shape[1]
    per = width // (n * dp)
    half = pieces // 2
    share = x_ref.shape[0] // half

    def exchange(**kind):
        exchange_all(
            n, dp, lambda peer: packed.at[peer], lambda source: held.at[source], gsend, grecv, **kind
        )

    def gain_share(index):
        rows = piece_rows(index, share)
        x = seq_ref[:, rows, :].reshape(n * share, width).astype(F32)
        term = part_ref[:, rows, :].reshape(n * share, width).astype(F32)
        inv = lax.rsqrt(jnp.mean(x * x, axis=1, keepdims=True) + EPS)
        dgain_ref[...] += jnp.sum(term * x * inv, axis=0, keepdims=True)

    def send_gains():
        for device in range(n * dp):
            cols = slice(device * per, (device + 1) * per)
            packed[device, :, :per] = dgain_ref[:, cols]
            packed[device, :, per : 2 * per] = dgain_mlp_ref[:, cols]
        held[all_me] = packed[all_me]
        exchange(start_only=True)

    @pl.loop(0, pieces)
    def _(piece):
        @pl.when(piece + 1 < pieces)
        def _():
            scatter.start_ends(piece + 1)

        @pl.when(piece < half)
        def _():
            gain_share(piece)

        @pl.when(piece == half)
        def _():
            send_gains()

        scatter.middle(piece)
        rows = scatter.rows(piece)

        def store(total):
            total_ref[...] = total

        scatter.result(piece, store)
        grad = total_ref[...]
        x = x_ref[rows, :].astype(F32)
        inv = lax.rsqrt(jnp.mean(x * x, axis=1, keepdims=True) + EPS)
        scaled = grad * gain_ref[...]
        mean = jnp.mean(scaled * x, axis=1, keepdims=True)
        out = grad_mid_ref[rows, :] + inv * (scaled - x * (inv * inv * mean))
        out_ref[rows, :] = out.astype(BF16)

    exchange(wait_only=True)
    gains_ref[...] = jnp.sum(held[...], axis=0)
    scatter.finish()


def sum_input_grad(n, dp, part, x, gain, grad_mid, dgain_mlp, seq, packed, pieces=8):
    rows, width = x.shape
    any_spec = pl.BlockSpec(memory_space=pl.ANY)
    return pl.pallas_call(
        functools.partial(last_kernel, n, dp, pieces),
        out_shape=(
            jax.ShapeDtypeStruct((rows, width), BF16),
            jax.ShapeDtypeStruct((1, packed), F32),
        ),
        in_specs=[VMEM_SPEC] * 2 + [any_spec] * 4,
        out_specs=(VMEM_SPEC,) * 2,
        scratch_shapes=[
            pltpu.VMEM((n, rows, width), BF16),
            pltpu.VMEM((rows, width), BF16),
            pltpu.VMEM((rows, width), F32),
            pltpu.VMEM((n, rows, width), BF16),
            pltpu.VMEM((rows // pieces, width), F32),
            pltpu.VMEM((1, width), F32),
            pltpu.VMEM((n * dp, 1, packed), F32),
            pltpu.VMEM((n * dp, 1, packed), F32),
            pltpu.VMEM((n + 1, rows, width), BF16),
        ]
        + sems(n, pieces)
        + [pltpu.SemaphoreType.DMA((n * dp,)), pltpu.SemaphoreType.DMA((n * dp,))]
        + [pltpu.SemaphoreType.DMA((3 + pieces,))],
        compiler_params=comm_params(4),
        cost_estimate=pl.CostEstimate(flops=0, bytes_accessed=250 * 1024 * 1024, transcendentals=0),
        name="sum_input_grad",
    )(gain, dgain_mlp, part.reshape(n, rows, width), x, grad_mid, seq)


def widen_kernel(
    mlp_ref, attn_ref, gains_ref, rows_ref, input_ref,
    gate_ref, up_ref, down_ref, query_ref, key_ref, value_ref, out_ref,
    attn_gain_ref, mlp_gain_ref, rows_out_ref, input_out_ref,
):
    units = gate_ref.shape[1]
    per = attn_gain_ref.shape[1]
    attn_gain_ref[...] = gains_ref[:, :per]
    mlp_gain_ref[...] = gains_ref[:, per : 2 * per]
    rows_out_ref[...] = rows_ref[...]
    input_out_ref[...] = input_ref[...]
    gate_ref[...] = mlp_ref[:, :units].astype(F32)
    up_ref[...] = mlp_ref[:, units : 2 * units].astype(F32)
    down_ref[...] = mlp_ref[:, 2 * units :].astype(F32).T
    q_cols, k_cols = query_ref.shape[1], key_ref.shape[0]
    query_ref[...] = attn_ref[:, :q_cols].astype(F32)
    key_ref[...] = attn_ref[:, q_cols : q_cols + k_cols].astype(F32).T
    value_ref[...] = attn_ref[:, q_cols + k_cols : q_cols + 2 * k_cols].astype(F32).T
    out_ref[...] = attn_ref[:, q_cols + 2 * k_cols :].astype(F32).T


def widen(mlp_grad, attn_grad, gains, rows_out, input_out, per, q_cols, k_cols):
    rows, units = mlp_grad.shape[0], mlp_grad.shape[1] // 3
    shapes = [(rows, units)] * 2 + [(units, rows), (rows, q_cols)] + [(k_cols, rows)] * 2 + [(q_cols, rows)]
    return pl.pallas_call(
        widen_kernel,
        out_shape=tuple(jax.ShapeDtypeStruct(shape, F32) for shape in shapes + [(1, per)] * 2)
        + (jax.ShapeDtypeStruct(rows_out.shape, BF16),) * 2,
        in_specs=[VMEM_SPEC] * 5,
        out_specs=(VMEM_SPEC,) * 11,
        compiler_params=pltpu.CompilerParams(vmem_limit_bytes=56 * 1024 * 1024),
        name="widen",
    )(mlp_grad, attn_grad, gains, rows_out, input_out)


def rotate(half_a, half_b, cos, sin):
    return half_a * cos - half_b * sin, half_b * cos + half_a * sin


def unrotate(half_a, half_b, cos, sin):
    return half_a * cos + half_b * sin, half_b * cos - half_a * sin


def mask_block(size):
    key = lax.broadcasted_iota(jnp.int32, (size, size), 0)
    row = lax.broadcasted_iota(jnp.int32, (size, size), 1)
    return jnp.where(key <= row, 0.0, NEG_LARGE)


def attend_kernel(
    n, dp, heads, block, pieces, x_ref, gain_ref, cos_ref, sin_ref, cot_hbm, wq_hbm, wk_hbm, wv_hbm, wo_hbm,
    attn_gain_ref, mlp_gain_ref, kv_ref, out_ref, log_ref, norm_hbm, qkv_hbm, part_hbm, w_out_hbm, wo_out_hbm, near_hbm, seq_hbm,
    norm_ref, qkv_ref, part_ref, w_ref, wo_ref, seq, act_ref, mask_ref, gains, wq, wk, wv, wo, send, recv, gsend, grecv, wsend, wrecv, own_sem, csend, crecv, fsend, frecv, save_sem,
):
    half = HEAD_SIZE // 2
    rows_all, width = x_ref.shape
    length = n * rows_all
    line = Line(n)
    me = line.me
    mine = lax.axis_index("dp")
    barrier_all(n, dp)
    seq[me] = x_ref[...]
    gains[mine * n + me] = gain_ref[...]
    gather = Gather(line, seq, send, recv, pieces)

    @pl.loop(0, pieces)
    def _(piece):
        gather.start_own(piece)

    def gain_rows(**kind):
        exchange_all(
            n, dp, lambda peer: gain_ref, lambda source: gains.at[source], gsend, grecv, **kind
        )

    gain_rows(start_only=True)

    shards = ((wq_hbm, wq), (wk_hbm, wk), (wv_hbm, wv), (wo_hbm, wo))
    own = [pltpu.make_async_copy(src, dst.at[mine], own_sem.at[i]) for i, (src, dst) in enumerate(shards)]
    pair = mine + 1 - 2 * lax.rem(mine, 2)

    def even_copy(i, offset):
        src, dst = shards[i]
        return pltpu.make_async_remote_copy(
            src_ref=src,
            dst_ref=dst.at[mine],
            send_sem=wsend.at[0, i, offset],
            recv_sem=wrecv.at[0, i, offset],
            device_id={"dp": lax.rem(mine + 2 * offset, dp)},
            device_id_type=MESH,
        )

    def pair_copy(i, offset):
        dst = shards[i][1].at[lax.rem(mine + 2 * offset, dp)]
        return pltpu.make_async_remote_copy(
            src_ref=dst,
            dst_ref=dst,
            send_sem=wsend.at[1, i, offset],
            recv_sem=wrecv.at[1, i, offset],
            device_id={"dp": pair},
            device_id_type=MESH,
        )

    for i in range(4):
        own[i].start()

    @pl.loop(1, dp // 2)
    def _(offset):
        for i in range(4):
            even_copy(i, offset).start()

    def cot_copy(right, hop):
        d = 0 if right else 1
        shard = me - (hop - 1) if right else me + (hop - 1)
        src = cot_hbm if hop == 1 else near_hbm.at[shard]
        return line.copy(src, near_hbm.at[shard], csend.at[d, hop - 1], crecv.at[d, hop - 1], 1 if right else -1)

    inner = (me > 0) & (me < n - 1)

    @pl.when(me == 0)
    def _():
        cot_copy(True, 1).start()

    @pl.when(me == n - 1)
    def _():
        cot_copy(False, 1).start()

    q_cols, k_cols = wq.shape[2], wk.shape[1]
    w_rows, w_cols = wq.shape[1], wo.shape[2]

    saves = [
        pltpu.make_async_copy(src, dst, save_sem.at[i])
        for i, (src, dst) in enumerate(
            (
                (w_ref, w_out_hbm),
                (wo_ref, wo_out_hbm),
                (norm_ref, norm_hbm),
                (qkv_ref, qkv_hbm),
                (seq, seq_hbm),
            )
        )
    ]

    def project(shard):
        x = seq[shard].astype(F32)
        inv = lax.rsqrt(jnp.mean(x * x, axis=1, keepdims=True) + EPS)
        norm = (x * inv * attn_gain_ref[...]).astype(BF16)
        rows = piece_rows(shard, rows_all)
        norm_ref[rows, :] = norm
        act_ref[:, rows] = mm(w_ref[...], norm, 0, 1)

    def prepare():
        gain_rows(wait_only=True)
        per = width // (n * dp)
        for device in range(n * dp):
            attn_gain_ref[:, device * per : (device + 1) * per] = gains[device, :, :per]
            mlp_gain_ref[:, device * per : (device + 1) * per] = gains[device, :, per : 2 * per]

        @pl.loop(0, dp // 2)
        def _(offset):
            for i in range(4):
                pair_copy(i, offset).wait_recv()

        for d in range(dp):
            rows = slice(d * w_rows, (d + 1) * w_rows)
            w_ref[rows, :q_cols] = wq[d]
            w_ref[rows, q_cols : q_cols + k_cols] = wk[d].T
            w_ref[rows, q_cols + k_cols :] = wv[d].T
            wo_ref[:, d * w_cols : (d + 1) * w_cols] = wo[d]
        saves[0].start()
        saves[1].start()

    def start_pair():
        for i in range(4):
            own[i].wait()

        @pl.loop(1, dp // 2)
        def _(offset):
            for i in range(4):
                even_copy(i, offset).wait_recv()

        @pl.loop(0, dp // 2)
        def _(offset):
            for i in range(4):
                pair_copy(i, offset).start()

    def arrived(d, hop, shard):
        cot_copy_in(
            line, near_hbm, shard, crecv.at[d, hop - 1], csend.at[d, hop - 1], 1 if d == 1 else -1
        ).wait_recv()

    ready = min(2, n - 1)
    for hop in range(1, ready + 1):

        @pl.loop(0, pieces)
        def _(piece):
            gather.receive(hop, piece)
            if hop == ready:

                @pl.when(piece == pieces // 2)
                def _():
                    start_pair()

        @pl.when((me == hop) & (me < n - 1))
        def _():
            cot_copy(True, 1).start()

        @pl.when((n - 1 - me == hop) & (me > 0))
        def _():
            cot_copy(False, 1).start()

    if n == 4:

        @pl.when(me == 1)
        def _():
            arrived(0, 1, me - 1)
            cot_copy(True, 2).start()

        @pl.when(me == 2)
        def _():
            arrived(1, 1, me + 1)
            cot_copy(False, 2).start()

    prepare()

    @pl.loop(0, 2 * n - 1)
    def _(turn):
        hop = (turn + 1) // 2
        leftward = lax.rem(turn, 2) == 1
        shard = jnp.where(leftward, me - hop, me + hop)

        @pl.when(leftward & (hop > ready))
        def _():
            @pl.loop(0, pieces)
            def _(piece):
                gather.receive(hop, piece)

        @pl.when(within(shard, n))
        def _():
            project(shard)

    saves[4].start()

    def far_copy(right, shard):
        part = near_hbm.at[shard, pl.ds(0, rows_all // pieces * FAR_DONE)]
        d = 0 if right else 1
        return line.copy(part, part, fsend.at[d], frecv.at[d], jnp.where(inner, 1 if right else -1, jnp.where(me == 0, 1, -1)))

    if n == 4:

        @pl.when(me == 1)
        def _():
            arrived(1, 1, me + 1)
            far_copy(False, me + 1).start()

        @pl.when(me == 2)
        def _():
            arrived(0, 1, me - 1)
            far_copy(True, me - 1).start()

    cos, sin = cos_ref[...], sin_ref[...]

    scale = 1.0 / math.sqrt(HEAD_SIZE)

    @pl.loop(0, heads + 1)
    def _(h):
        base = pl.multiple_of(h * HEAD_SIZE, HEAD_SIZE)
        a, b = rotate(act_ref[pl.ds(base, half), :], act_ref[pl.ds(base + half, half), :], cos, sin)
        factor = jnp.where(h < heads, scale, 1.0)
        a, b = a * factor, b * factor
        qkv_ref[pl.ds(base, half), :] = a.astype(BF16)
        qkv_ref[pl.ds(base + half, half), :] = b.astype(BF16)

    values = pl.ds((heads + 1) * HEAD_SIZE, HEAD_SIZE)
    qkv_ref[values, :] = act_ref[values, :].astype(BF16)
    saves[2].start()
    saves[3].start()
    mask_ref[...] = mask_block(block)
    kv_ref[...] = qkv_ref[pl.ds(heads * HEAD_SIZE, 2 * HEAD_SIZE), :].T

    @pl.loop(0, heads)
    def _(h):
        base = pl.multiple_of(h * HEAD_SIZE, HEAD_SIZE)
        for i in range(length // block):
            cols = pl.ds(i * block, block)
            query = qkv_ref[pl.ds(base, HEAD_SIZE), cols]
            scores = []
            peak = None
            for j in range(i + 1):
                s = mm(kv_ref[pl.ds(j * block, block), :HEAD_SIZE], query)
                if i == j:
                    s = s + mask_ref[...]
                top = jnp.max(s, axis=0, keepdims=True)
                peak = top if peak is None else jnp.maximum(peak, top)
                scores.append(s)
            weights = [jnp.exp(s - peak) for s in scores]
            total = sum(jnp.sum(w, axis=0, keepdims=True) for w in weights)
            log_ref[pl.ds(h, 1), cols] = peak + jnp.log(total)
            inverse = 1.0 / total
            mixed = None
            for j in range(i + 1):
                w = (weights[j] * inverse).astype(BF16)
                v = qkv_ref[values, pl.ds(j * block, block)]
                term = mm(v, w)
                mixed = term if mixed is None else mixed + term
            out_ref[pl.ds(base, HEAD_SIZE), cols] = mixed.astype(BF16)

    def part_save(index):
        cols = piece_rows(index, tile)
        return pltpu.make_async_copy(part_ref.at[:, cols], part_hbm.at[:, cols], save_sem.at[len(saves) + index])

    tile = even_tile(width)

    @pl.loop(0, width // tile)
    def _(index):
        cols = piece_rows(index, tile)
        part_ref[:, cols] = mm(out_ref[...], wo_ref[:, cols], 0, 0).astype(BF16)
        part_save(index).start()

    gather.finish()
    for save in saves:
        save.wait()

    @pl.loop(0, width // tile)
    def _(index):
        part_save(index).wait()

    @pl.loop(1, dp // 2)
    def _(offset):
        for i in range(4):
            even_copy(i, offset).wait_send()

    @pl.loop(0, dp // 2)
    def _(offset):
        for i in range(4):
            pair_copy(i, offset).wait_send()

    if n == 4:

        @pl.when(me == 1)
        def _():
            arrived(1, 2, me + 2)
            cot_copy(True, 2).wait_send()
            far_copy(False, me + 1).wait_send()

        @pl.when(me == 2)
        def _():
            arrived(0, 2, me - 2)
            cot_copy(False, 2).wait_send()
            far_copy(True, me - 1).wait_send()

        @pl.when(me == 0)
        def _():
            far_copy(False, me + 2).wait_recv()

        @pl.when(me == n - 1)
        def _():
            far_copy(True, me - 2).wait_recv()

    else:

        @pl.when(inner)
        def _():
            arrived(0, 1, me - 1)
            arrived(1, 1, me + 1)

    @pl.when(me == 0)
    def _():
        arrived(1, 1, me + 1)

    @pl.when(me == n - 1)
    def _():
        arrived(0, 1, me - 1)

    @pl.when(me < n - 1)
    def _():
        cot_copy(True, 1).wait_send()

    @pl.when(me > 0)
    def _():
        cot_copy(False, 1).wait_send()


def cot_copy_in(line, near_hbm, shard, recv, send, step):
    part = near_hbm.at[shard]
    return line.copy(part, part, send, recv, step)


def attend(n, dp, x, gains, weights, cos, sin, cotangent, block=256, pieces=4):
    assert n <= 4 and dp % 2 == 0
    rows, width = x.shape
    length = n * rows
    q_cols, k_cols = weights[0].shape[1], weights[1].shape[0]
    cols_in = q_cols + 2 * k_cols
    heads = cols_in // HEAD_SIZE - 2
    any_spec = pl.BlockSpec(memory_space=pl.ANY)
    dma = pltpu.SemaphoreType.DMA
    return pl.pallas_call(
        functools.partial(attend_kernel, n, dp, heads, block, pieces),
        out_shape=(
            jax.ShapeDtypeStruct((1, width), F32),
            jax.ShapeDtypeStruct((1, width), F32),
            jax.ShapeDtypeStruct((length, 2 * HEAD_SIZE), BF16),
            jax.ShapeDtypeStruct((heads * HEAD_SIZE, length), BF16),
            jax.ShapeDtypeStruct((heads, length), F32),
            jax.ShapeDtypeStruct((length, width), BF16),
            jax.ShapeDtypeStruct((cols_in, length), BF16),
            jax.ShapeDtypeStruct((length, width), BF16),
            jax.ShapeDtypeStruct((width, cols_in), BF16),
            jax.ShapeDtypeStruct((q_cols, width), BF16),
            jax.ShapeDtypeStruct((n,) + cotangent.shape, BF16),
            jax.ShapeDtypeStruct((n, rows, width), BF16),
        ),
        in_specs=[VMEM_SPEC] * 4 + [any_spec] * 5,
        out_specs=(VMEM_SPEC,) * 5 + (any_spec,) * 7,
        scratch_shapes=[
            pltpu.VMEM((length, width), BF16),
            pltpu.VMEM((cols_in, length), BF16),
            pltpu.VMEM((length, width), BF16),
            pltpu.VMEM((width, cols_in), BF16),
            pltpu.VMEM((q_cols, width), BF16),
            pltpu.VMEM((n, rows, width), BF16),
            pltpu.VMEM((cols_in, length), F32),
            pltpu.VMEM((block, block), F32),
            pltpu.VMEM((n * dp, 1, gains.shape[1]), F32),
        ]
        + [pltpu.VMEM((dp,) + w.shape, BF16) for w in weights]
        + sems(n, pieces)
        + [dma((n * dp,)), dma((n * dp,)), dma((2, 4, dp // 2)), dma((2, 4, dp // 2)), dma((4,))]
        + [dma((2, 2)), dma((2, 2)), dma((2,)), dma((2,)), dma((5 + width // even_tile(width),))],
        compiler_params=comm_params(1),
        cost_estimate=pl.CostEstimate(
            flops=2 * length * width * (cols_in + q_cols),
            bytes_accessed=350 * 1024 * 1024,
            transcendentals=heads * length * length,
        ),
        name="attend",
    )(x, gains, cos, sin, cotangent, *weights)


def attend_back_kernel(
    n, heads, block, pieces, kv_ref, log_ref, cos_ref, sin_ref,
    mid_hbm, low_hbm, hid_hbm, w_mlp_hbm, wo_hbm, w_hbm, qkv_hbm, out_hbm, norm_hbm,
    rows_ref, part_hbm, wgrad_hbm,
    mid_ref, part_ref, seq, hid, w_down, down_ref, buf, wo_ref, w_ref, qkv_ref, out_ref, norm_ref,
    dkv, mask_ref, grad_ref, dqkv_ref, wgrad, ssend, srecv, gsend, grecv, load_sem, save_sem,
):
    half = HEAD_SIZE // 2
    rows_all, width = mid_ref.shape
    units = hid.shape[2]
    cols_in = qkv_ref.shape[0]
    scale = 1.0 / math.sqrt(HEAD_SIZE)
    me = lax.axis_index("tensor")
    pairs = (
        (low_hbm, seq.at[me]),
        (hid_hbm, hid),
        (w_mlp_hbm.at[:, pl.ds(2 * units, units)], w_down),
        (wo_hbm, wo_ref),
        (qkv_hbm, qkv_ref),
        (out_hbm, out_ref),
        (w_hbm, w_ref),
        (norm_hbm, norm_ref),
        (mid_hbm, mid_ref),
    )
    loads = [pltpu.make_async_copy(src, dst, load_sem.at[i]) for i, (src, dst) in enumerate(pairs)]
    for load in loads:
        load.start()
    line = Line(n)
    line.barrier()
    scatter = Scatter(line, down_ref, buf, ssend, srecv, pieces)
    gather = Gather(line, seq, gsend, grecv, pieces)
    loads[0].wait()

    @pl.loop(0, pieces)
    def _(piece):
        gather.start_own(piece)

    dkv[...] = jnp.zeros_like(dkv)
    mask_ref[...] = mask_block(block)
    keys = pl.ds(heads * HEAD_SIZE, HEAD_SIZE)

    def project(shard):
        grad_ref[:, piece_rows(shard, rows_all)] = mm(wo_ref[...], seq[shard], 1, 1).astype(BF16)

    tile = even_tile(width)

    def start_sums():
        loads[1].wait()
        loads[2].wait()

        @pl.loop(0, pieces)
        def _(piece):
            rows = scatter.rows(piece)

            @pl.loop(0, width // tile)
            def _(index):
                cols = piece_rows(index, tile)
                value = hid[:, rows, :].reshape(n * scatter.size, units)
                value = mm(value, w_down[cols, :], 1, 1).astype(BF16)
                down_ref[:, rows, cols] = value.reshape(n, scatter.size, tile)

            scatter.start_ends(piece)

    def sum_piece(piece):
        scatter.middle(piece)
        rows = scatter.rows(piece)

        def store(total):
            rows_ref[rows, :] = (mid_ref[rows, :] + total).astype(BF16)

        scatter.result(piece, store)

    start_sums()
    for load in loads[3:]:
        load.wait()

    def attention_rows(i):
        cols = pl.ds(i * block, block)
        cos, sin = cos_ref[:, cols], sin_ref[:, cols]

        @pl.loop(0, heads)
        def _(h):
            base = pl.multiple_of(h * HEAD_SIZE, HEAD_SIZE)
            mine = pl.ds(base, HEAD_SIZE)
            query = qkv_ref[mine, cols]
            grad = grad_ref[mine, cols]
            delta = jnp.sum(
                grad.astype(F32) * out_ref[mine, cols].astype(F32), axis=0, keepdims=True
            )
            log_total = log_ref[pl.ds(h, 1), cols]
            dquery = None
            for j in range(i + 1):
                rows = pl.ds(j * block, block)
                s = mm(kv_ref[rows, :HEAD_SIZE], query)
                if i == j:
                    s = s + mask_ref[...]
                probs = jnp.exp(s - log_total)
                dprobs = mm(kv_ref[rows, HEAD_SIZE:], grad)
                dscores = (probs * (dprobs - delta)).astype(BF16)
                dkv[0, rows, :] += mm(dscores, query, 1, 1)
                dkv[1, rows, :] += mm(probs.astype(BF16), grad, 1, 1)
                term = mm(qkv_ref[keys, rows], dscores)
                dquery = term if dquery is None else dquery + term
            dquery = dquery * scale
            a, b = unrotate(dquery[:half], dquery[half:], cos, sin)
            dqkv_ref[pl.ds(base, half), cols] = a.astype(BF16)
            dqkv_ref[pl.ds(base + half, half), cols] = b.astype(BF16)

    @pl.loop(0, 2 * n - 1)
    def _(turn):
        hop = (turn + 1) // 2
        leftward = lax.rem(turn, 2) == 1
        shard = jnp.where(leftward, me - hop, me + hop)

        @pl.when(leftward)
        def _():
            @pl.loop(0, pieces)
            def _(piece):
                gather.receive(hop, piece)

        @pl.when(within(shard, n))
        def _():
            project(shard)
            for i in range(n):

                @pl.when(shard == i)
                def _():
                    attention_rows(i)

        @pl.when(jnp.logical_not(leftward) & within(hop - 1, min(n, pieces) - 1))
        def _():
            sum_piece(hop - 1)

    dkeys = dkv[0].T
    a, b = unrotate(dkeys[:half], dkeys[half:], cos_ref[...], sin_ref[...])
    dqkv_ref[pl.ds(heads * HEAD_SIZE, half), :] = a.astype(BF16)
    dqkv_ref[pl.ds(heads * HEAD_SIZE + half, half), :] = b.astype(BF16)
    dqkv_ref[pl.ds((heads + 1) * HEAD_SIZE, HEAD_SIZE), :] = dkv[1].T.astype(BF16)

    def part_save(index):
        cols = piece_rows(index, tile)
        return pltpu.make_async_copy(part_ref.at[:, cols], part_hbm.at[:, cols], save_sem.at[0, index])

    def wgrad_save(index):
        rows = piece_rows(index, tile)
        return pltpu.make_async_copy(wgrad.at[rows, :], wgrad_hbm.at[rows, :], save_sem.at[1, index])

    @pl.loop(0, width // tile)
    def _(index):
        cols = piece_rows(index, tile)
        part_ref[:, cols] = mm(dqkv_ref[...], w_ref[cols, :], 0, 1).astype(BF16)
        part_save(index).start()

    @pl.loop(0, width // tile)
    def _(index):
        cols = piece_rows(index, tile)
        wgrad[cols, :cols_in] = mm(norm_ref[:, cols], dqkv_ref[...], 0, 1).astype(BF16)
        for shard in range(n):
            term = mm(seq[shard, :, cols], out_ref[:, shard * rows_all : (shard + 1) * rows_all], 0, 1)
            total = term if shard == 0 else total + term
        wgrad[cols, cols_in:] = total.astype(BF16)
        wgrad_save(index).start()

    for piece in range(min(n, pieces) - 1, pieces):
        sum_piece(piece)
    scatter.finish()
    gather.finish()

    @pl.loop(0, width // tile)
    def _(index):
        part_save(index).wait()
        wgrad_save(index).wait()


def attend_back(
    n, mid, kv, log_total, cos, sin, low, hidden, w_mlp, w_out, w_qkv, qkv, out, norm, pieces=4
):
    rows, width = mid.shape
    block = rows
    length = n * rows
    cols_in = qkv.shape[0]
    heads = cols_in // HEAD_SIZE - 2
    units = hidden.shape[2]
    any_spec = pl.BlockSpec(memory_space=pl.ANY)
    wgrad_shape = (width, cols_in + w_out.shape[0])
    return pl.pallas_call(
        functools.partial(attend_back_kernel, n, heads, block, pieces),
        out_shape=(
            jax.ShapeDtypeStruct((rows, width), BF16),
            jax.ShapeDtypeStruct((length, width), BF16),
            jax.ShapeDtypeStruct(wgrad_shape, BF16),
        ),
        in_specs=[VMEM_SPEC] * 4 + [any_spec] * 9,
        out_specs=(VMEM_SPEC,) + (any_spec,) * 2,
        scratch_shapes=[
            pltpu.VMEM(mid.shape, F32),
            pltpu.VMEM((length, width), BF16),
            pltpu.VMEM((n, rows, width), BF16),
            pltpu.VMEM((n, rows, units), BF16),
            pltpu.VMEM((width, units), BF16),
            pltpu.VMEM((n, rows, width), BF16),
            pltpu.VMEM((n + 1, rows, width), BF16),
            pltpu.VMEM(w_out.shape, BF16),
            pltpu.VMEM(w_qkv.shape, BF16),
            pltpu.VMEM(qkv.shape, BF16),
            pltpu.VMEM(out.shape, BF16),
            pltpu.VMEM(norm.shape, BF16),
            pltpu.VMEM((2, length, HEAD_SIZE), F32),
            pltpu.VMEM((block, block), F32),
            pltpu.VMEM((heads * HEAD_SIZE, length), BF16),
            pltpu.VMEM((cols_in, length), BF16),
            pltpu.VMEM(wgrad_shape, BF16),
        ]
        + sems(n, pieces) * 2
        + [pltpu.SemaphoreType.DMA((9,)), pltpu.SemaphoreType.DMA((2, width // even_tile(width)))],
        compiler_params=comm_params(3),
        cost_estimate=pl.CostEstimate(
            flops=6 * length * width * wgrad_shape[1],
            bytes_accessed=350 * 1024 * 1024,
            transcendentals=heads * length * length,
        ),
        name="attend_back",
    )(kv, log_total, cos, sin, mid, low, hidden, w_mlp, w_out, w_qkv, qkv, out, norm)


def local(
    n, dp, x, gain_attn, gain_mlp, w_query, w_key, w_value, w_out, w_gate, w_up, w_down, cotangent
):
    rows, _ = x.shape
    length = n * rows
    per = gain_attn.shape[0]
    packed = 2 * per + (-2 * per) % LANES

    mlp_all = lax.all_gather(
        jnp.concatenate([w_gate, w_up, w_down.T], axis=1), "dp", axis=0, tiled=True
    )
    gains = [gain_attn, gain_mlp]
    if packed > 2 * per:
        gains.append(jnp.zeros((packed - 2 * per,), F32))
    cos, sin = tables(length)
    full_attn, full_mlp, kv, attended, log_total, norm_attn, qkv, out_part, w_qkv, w_out_all, near, x_seq = attend(
        n,
        dp,
        x,
        jnp.concatenate(gains).reshape(1, packed),
        (w_query, w_key.T, w_value.T, w_out),
        cos,
        sin,
        cotangent,
    )
    dgain_mlp, mid, grad_mid, hidden, mlp_grad, grad_low = mlp(
        n, out_part, x, full_mlp, mlp_all, cotangent, near
    )
    mlp_grad = lax.psum_scatter(mlp_grad, "dp", scatter_dimension=0, tiled=True)
    block_output, attn_part, attn_grad = attend_back(
        n, mid, kv, log_total, cos, sin, grad_low, hidden, mlp_all, w_out_all, w_qkv, qkv, attended, norm_attn
    )
    attn_grad = lax.psum_scatter(attn_grad, "dp", scatter_dimension=0, tiled=True)
    input_grad, dgains = sum_input_grad(
        n, dp, attn_part, x, full_attn, grad_mid, dgain_mlp, x_seq, packed
    )
    gate, up, down, query, key, value, out, dgain_attn, dgain_mlp, block_output, input_grad = widen(
        mlp_grad, attn_grad, dgains, block_output, input_grad, per, w_query.shape[1], w_key.shape[1]
    )
    return (
        block_output,
        input_grad,
        dgain_attn.reshape(per),
        dgain_mlp.reshape(per),
        query,
        key.T,
        value.T,
        out,
        gate,
        up,
        down,
    )


def solution(mesh):
    rows = P(("dp", "tensor"), None)
    gain = P(("dp", "tensor"))
    into = P("dp", "tensor")
    back = P("tensor", "dp")
    in_specs = (rows, gain, gain, into, into, into, back, into, into, back, rows)
    out_specs = (rows, rows, gain, gain, into, into, into, back, into, into, back)

    def body(*args):
        return local(mesh.shape["tensor"], mesh.shape["dp"], *args)

    return jax.shard_map(body, mesh=mesh, in_specs=in_specs, out_specs=out_specs, check_vma=False)
```

```python
import functools
import math

import jax
import jax.numpy as jnp
from jax import lax
from jax.experimental import pallas as pl
from jax.experimental.pallas import tpu as pltpu
from jax.sharding import PartitionSpec as P


HEAD_SIZE = 64
EPS = 1e-05
ROPE_BASE = 10000.0
NEG_LARGE = -1e30
LANES = 128
MESH = pl.DeviceIdType.MESH
F32 = jnp.float32
BF16 = jnp.bfloat16
VMEM_SPEC = pl.BlockSpec(memory_space=pltpu.VMEM)
FAR_DONE = 2


def tables(sequence_length):
    half = HEAD_SIZE // 2
    frequency = ROPE_BASE ** (-(jnp.arange(half, dtype=F32) * 2.0) / HEAD_SIZE)
    angles = frequency[:, None] * jnp.arange(sequence_length, dtype=F32)[None, :]
    return jnp.cos(angles), jnp.sin(angles)


def dims(contract_left, contract_right):
    return (((contract_left,), (contract_right,)), ((), ()))


def mm(left, right, contract_left=1, contract_right=0):
    return lax.dot_general(
        left, right, dims(contract_left, contract_right), preferred_element_type=F32
    )


def piece_rows(piece, size):
    return pl.ds(pl.multiple_of(piece * size, size), size)


class Line:
    def __init__(self, n):
        self.n = n
        self.me = lax.axis_index("tensor")

    def barrier(self):
        barrier = pltpu.get_barrier_semaphore()
        n, me = self.n, self.me

        @pl.when(me > 0)
        def _():
            pl.semaphore_signal(barrier, inc=1, device_id={"tensor": me - 1}, device_id_type=MESH)

        @pl.when(me < n - 1)
        def _():
            pl.semaphore_signal(barrier, inc=1, device_id={"tensor": me + 1}, device_id_type=MESH)

        inner = (me > 0) & (me < n - 1)

        @pl.when(inner)
        def _():
            pl.semaphore_wait(barrier, 2)

        @pl.when(jnp.logical_not(inner))
        def _():
            pl.semaphore_wait(barrier, 1)

    def copy(self, src, dst, send, recv, step):
        return pltpu.make_async_remote_copy(
            src_ref=src,
            dst_ref=dst,
            send_sem=send,
            recv_sem=recv,
            device_id={"tensor": self.me + step},
            device_id_type=MESH,
        )


class Gather:
    def __init__(self, line, buf, send, recv, pieces):
        self.line, self.buf, self.send, self.recv, self.pieces = line, buf, send, recv, pieces
        self.size = buf.shape[1] // pieces

    def message(self, right, hop, piece, shard):
        d = 0 if right else 1
        part = self.buf.at[shard, piece_rows(piece, self.size)]
        return self.line.copy(
            part, part, self.send.at[d, hop - 1, piece], self.recv.at[d, hop - 1, piece], 1 if right else -1
        )

    def start_own(self, piece):
        line = self.line
        me, n = line.me, line.n

        @pl.when(me < n - 1)
        def _():
            self.message(True, 1, piece, me).start()

        @pl.when(me > 0)
        def _():
            self.message(False, 1, piece, me).start()

    def start_hop(self, hop, piece):
        line = self.line
        me, n = line.me, line.n

        @pl.when((me - (hop - 1) >= 0) & (me < n - 1))
        def _():
            self.message(True, hop, piece, me - (hop - 1)).start()

        @pl.when((me + (hop - 1) <= n - 1) & (me > 0))
        def _():
            self.message(False, hop, piece, me + (hop - 1)).start()

    def receive(self, hop, piece, use=None):
        line = self.line
        me, n = line.me, line.n

        @pl.when(me - hop >= 0)
        def _():
            shard = me - hop
            self.message(True, hop, piece, shard).wait_recv()
            if not isinstance(hop, int) or hop < n - 1:

                @pl.when((me < n - 1) & (hop < n - 1))
                def _():
                    self.message(True, hop + 1, piece, shard).start()

            if use is not None:
                use(shard, piece)

        @pl.when(me + hop <= n - 1)
        def _():
            shard = me + hop
            self.message(False, hop, piece, shard).wait_recv()
            if not isinstance(hop, int) or hop < n - 1:

                @pl.when((me > 0) & (hop < n - 1))
                def _():
                    self.message(False, hop + 1, piece, shard).start()

            if use is not None:
                use(shard, piece)

    def finish(self, first_piece=0, end_piece=None):
        line = self.line
        me, n = line.me, line.n

        @pl.loop(first_piece, self.pieces if end_piece is None else end_piece)
        def _(piece):
            for hop in range(1, n):

                @pl.when((me - (hop - 1) >= 0) & (me < n - 1))
                def _():
                    self.message(True, hop, piece, me - (hop - 1)).wait_send()

                @pl.when((me + (hop - 1) <= n - 1) & (me > 0))
                def _():
                    self.message(False, hop, piece, me + (hop - 1)).wait_send()


class Scatter:
    def __init__(self, line, part, buf, send, recv, pieces):
        self.line, self.part, self.buf, self.pieces = line, part, buf, pieces
        self.send, self.recv = send, recv
        self.size = part.shape[1] // pieces

    def rows(self, piece):
        return piece_rows(piece, self.size)

    def outgoing(self, d, target, piece, from_part=False):
        rows, line = self.rows(piece), self.line
        src = (self.part if from_part else self.buf).at[target, rows]
        slot = target
        if d == 1:
            slot = jnp.where(target == line.me - 1, line.n, target)
        return line.copy(
            src,
            self.buf.at[slot, rows],
            self.send.at[d, target, piece],
            self.recv.at[d, target, piece],
            1 if d == 0 else -1,
        )

    def incoming(self, d, target, slot, piece):
        part = self.buf.at[slot, self.rows(piece)]
        return self.line.copy(
            part, part, self.send.at[d, target, piece], self.recv.at[d, target, piece], 1 if d == 0 else -1
        )

    def start_ends(self, piece):
        line = self.line
        me, n = line.me, line.n

        @pl.when(me == 0)
        def _():
            for target in range(n - 1, 0, -1):
                self.outgoing(0, target, piece, True).start()

        @pl.when(me == n - 1)
        def _():
            for target in range(0, n - 1):
                self.outgoing(1, target, piece, True).start()

    def pass_on(self, d, target, piece):
        buf = self.buf
        self.incoming(d, target, target, piece).wait_recv()
        rows = self.rows(piece)
        total = buf[target, rows].astype(F32) + self.part[target, rows].astype(F32)
        buf[target, rows] = total.astype(BF16)
        self.outgoing(d, target, piece).start()

    def passes(self, piece, right, targets, where):
        line = self.line
        me, n = line.me, line.n
        for target in targets:
            held = (me > 0) & (me < target) if right else (me < n - 1) & (me > target)

            @pl.when(where & held)
            def _():
                self.pass_on(0 if right else 1, target, piece)

    def first(self, piece):
        n, left_half = self.line.n, self.line.me < self.line.n // 2
        self.passes(piece, True, (n - 1,), left_half)
        self.passes(piece, False, (0,), jnp.logical_not(left_half))

    def rest(self, piece):
        n, left_half = self.line.n, self.line.me < self.line.n // 2
        right_half = jnp.logical_not(left_half)
        self.passes(piece, True, range(n - 2, 0, -1), left_half)
        self.passes(piece, False, range(1, n - 1), right_half)
        self.passes(piece, False, range(0, n - 1), left_half)
        self.passes(piece, True, range(n - 1, 0, -1), right_half)

    def middle(self, piece):
        self.first(piece)
        self.rest(piece)

    def result(self, piece, store):
        line = self.line
        me, n = line.me, line.n
        rows = self.rows(piece)

        @pl.when(me > 0)
        def _():
            self.incoming(0, me, me, piece).wait_recv()

        @pl.when(me < n - 1)
        def _():
            self.incoming(1, me, n, piece).wait_recv()

        own = self.part[me, rows].astype(F32)

        @pl.when(me == 0)
        def _():
            store(own + self.buf[n, rows].astype(F32))

        @pl.when(me == n - 1)
        def _():
            store(own + self.buf[me, rows].astype(F32))

        @pl.when((me > 0) & (me < n - 1))
        def _():
            store(own + self.buf[me, rows].astype(F32) + self.buf[n, rows].astype(F32))

    def finish(self, ends=True, middles=True):
        line = self.line
        me, n = line.me, line.n
        inner = (me > 0) & (me < n - 1)

        @pl.when((inner & middles) | (jnp.logical_not(inner) & ends))
        def _():
            @pl.loop(0, self.pieces)
            def _(piece):
                for target in range(1, n):

                    @pl.when(me < target)
                    def _():
                        self.outgoing(0, target, piece).wait_send()

                for target in range(0, n - 1):

                    @pl.when(me > target)
                    def _():
                        self.outgoing(1, target, piece).wait_send()


def within(piece, pieces):
    return (piece >= 0) & (piece < pieces)


def sems(n, pieces):
    return [pltpu.SemaphoreType.DMA((2, n, pieces)), pltpu.SemaphoreType.DMA((2, n, pieces))]


def comm_params(collective_id):
    return pltpu.CompilerParams(
        collective_id=collective_id, has_side_effects=True, vmem_limit_bytes=60 * 1024 * 1024
    )


def exchange_all(n, dp, send_row, recv_row, send, recv, start_only=False, wait_only=False):
    devices = n * dp
    me = lax.axis_index("dp") * n + lax.axis_index("tensor")

    def message(offset, peer, source):
        return pltpu.make_async_remote_copy(
            src_ref=send_row(peer),
            dst_ref=recv_row(source),
            send_sem=send.at[offset],
            recv_sem=recv.at[offset],
            device_id={"dp": peer // n, "tensor": peer % n},
            device_id_type=MESH,
        )

    if not wait_only:

        @pl.loop(1, devices)
        def _(offset):
            message(offset, lax.rem(me + offset, devices), me).start()

    if not start_only:

        @pl.loop(1, devices)
        def _(offset):
            copy = message(offset, lax.rem(me + offset, devices), me)
            copy.wait_send()
            copy.wait_recv()


def barrier_all(n, dp):
    devices = n * dp
    me = lax.axis_index("dp") * n + lax.axis_index("tensor")
    barrier = pltpu.get_barrier_semaphore()

    @pl.loop(1, devices)
    def _(offset):
        peer = lax.rem(me + offset, devices)
        pl.semaphore_signal(
            barrier, inc=1, device_id={"dp": peer // n, "tensor": peer % n}, device_id_type=MESH
        )

    pl.semaphore_wait(barrier, devices - 1)


def even_tile(extent):
    return 512 if extent % 512 == 0 else extent


def tiles(extent, size):
    return [(start, min(size, extent - start)) for start in range(0, extent, size)]


def mlp_kernel(
    n, pieces, gain_ref, part_hbm, x_hbm, w_hbm, cot_hbm, near_hbm,
    dgain_ref, mid_hbm, grad_hbm, hid_hbm, wgrad_hbm, low_hbm,
    part_ref, x_ref, mid_ref, grad_ref, w, cot, seq, buf, npart, buf_back, hid, dgate, dup, stage, inv_ref,
    ssend, srecv, gsend, grecv, bsend, brecv, csend, crecv, local_sem, stage_sem, part_sem,
):
    line = Line(n)
    me = line.me
    rows_all, width = part_ref.shape[1:]

    def part_load(piece):
        rows = piece_rows(piece, rows_all // pieces)
        return pltpu.make_async_copy(part_hbm.at[:, rows], part_ref.at[:, rows], part_sem.at[0, piece])

    def piece_save(which, ref, hbm, piece):
        rows = piece_rows(piece, rows_all // pieces)
        return pltpu.make_async_copy(ref.at[rows], hbm.at[rows], part_sem.at[which, piece])

    x_load = pltpu.make_async_copy(x_hbm, x_ref, local_sem.at[3])
    for piece in range(pieces):
        part_load(piece).start()
    x_load.start()

    units = hid.shape[2]
    weight_load = pltpu.make_async_copy(w_hbm, w, local_sem.at[0])
    own_load = pltpu.make_async_copy(cot_hbm, cot.at[me], local_sem.at[1])
    inner = (me > 0) & (me < n - 1)

    def near_load(shard, count):
        rows = pl.ds(0, count)
        return pltpu.make_async_copy(near_hbm.at[shard, rows], cot.at[shard, rows], local_sem.at[5 + shard])

    def each_near(act):
        for shard in range(n):
            here = (me != shard) & (inner | (me - shard == 1) | (shard - me == 1))

            @pl.when(here)
            def _():
                act(near_load(shard, rows_all))

            if n == 4:

                @pl.when(jnp.logical_not(inner) & ((me - shard == 2) | (shard - me == 2)))
                def _():
                    act(near_load(shard, rows_all // pieces * FAR_DONE))

    each_near(lambda copy: copy.start())
    own_load.start()
    weight_load.start()
    line.barrier()
    scatter = Scatter(line, part_ref, buf, ssend, srecv, pieces)
    gather = Gather(line, seq, gsend, grecv, pieces)
    scatter_back = Scatter(line, npart, buf_back, bsend, brecv, pieces)
    cot_gather = Gather(line, cot, csend, crecv, pieces)
    size = scatter.size
    part_load(0).wait()
    scatter.start_ends(0)
    for piece in range(1, pieces):
        part_load(piece).wait()
    x_load.wait()
    dgain_ref[...] = jnp.zeros_like(dgain_ref)

    each_near(lambda copy: copy.wait())

    def still_far(hop, piece):
        return (piece >= FAR_DONE) if hop == 2 and n == 4 else (piece >= 0)

    def each_far(piece, act):
        for hop in range(2, n):

            @pl.when((me == n - 2) & still_far(hop, piece))
            def _():
                act(True, hop, me - (hop - 1))

            @pl.when((me == 1) & still_far(hop, piece))
            def _():
                act(False, hop, me + (hop - 1))

    def far_start(piece):
        each_far(piece, lambda right, hop, shard: cot_gather.message(right, hop, piece, shard).start())

    def far_sent(piece):
        each_far(piece, lambda right, hop, shard: cot_gather.message(right, hop, piece, shard).wait_send())

    def far_arrived(piece):
        for hop in range(2, n):

            @pl.when((me == n - 1) & still_far(hop, piece))
            def _():
                cot_gather.message(True, hop, piece, me - hop).wait_recv()

            @pl.when((me == 0) & still_far(hop, piece))
            def _():
                cot_gather.message(False, hop, piece, me + hop).wait_recv()

    for piece in range(min(2, pieces)):
        far_start(jnp.int32(piece))

    def norm(piece):
        rows = scatter.rows(piece)

        def store(total):
            mid_ref[rows, :] = x_ref[rows, :].astype(F32) + total

        scatter.result(piece, store)
        mid = mid_ref[rows, :]
        inv = lax.rsqrt(jnp.mean(mid * mid, axis=1, keepdims=True) + EPS)
        inv_ref[rows, :] = jnp.broadcast_to(inv, (size, LANES))
        seq[me, rows, :] = (mid * inv * gain_ref[...]).astype(BF16)
        piece_save(1, mid_ref, mid_hbm, piece).start()

    def back(piece):
        rows = scatter.rows(piece)

        def store(total):
            grad_ref[rows, :] = total

        scatter_back.result(piece, store)
        grad = grad_ref[rows, :]
        mid = mid_ref[rows, :]
        inv = inv_ref[rows, 0:1]
        dgain_ref[...] += jnp.sum(grad * mid * inv, axis=0, keepdims=True)
        scaled = grad * gain_ref[...]
        mean = jnp.mean(scaled * mid, axis=1, keepdims=True)
        out = cot[me, rows, :].astype(F32) + inv * (scaled - mid * (inv * inv * mean))
        grad_ref[rows, :] = out
        buf[me, rows, :] = out.astype(BF16)
        piece_save(2, grad_ref, grad_hbm, piece).start()

    def flat(ref, piece):
        value = ref[:, scatter.rows(piece), :]
        return value.reshape(n * size, value.shape[2])

    def feed(piece):
        rows = scatter.rows(piece)
        for start, count in tiles(units, 512):
            x = flat(seq, piece)
            gate = mm(x, w[:, start : start + count])
            up = mm(x, w[:, units + start : units + start + count])
            dhidden = mm(flat(cot, piece), w[:, 2 * units + start : 2 * units + start + count])
            sigmoid = jax.nn.sigmoid(gate)
            act = gate * sigmoid
            cols = slice(start, start + count)
            shape = (n, size, count)
            hid[:, rows, cols] = (act * up).astype(BF16).reshape(shape)
            dup[:, rows, cols] = (dhidden * act).astype(BF16).reshape(shape)
            dgate[:, rows, cols] = (
                (dhidden * up * sigmoid * (1.0 + gate * (1.0 - sigmoid))).astype(BF16).reshape(shape)
            )
        tile = even_tile(width)

        @pl.loop(0, width // tile)
        def _(index):
            cols = piece_rows(index, tile)
            total = mm(flat(dgate, piece), w[cols, :units], 1, 1)
            total += mm(flat(dup, piece), w[cols, units : 2 * units], 1, 1)
            npart[:, rows, cols] = total.astype(BF16).reshape(n, size, tile)

    step_rows = min(LANES, width)
    count = width // step_rows

    def save(index, slot):
        return pltpu.make_async_copy(
            stage.at[slot],
            wgrad_hbm.at[pl.ds(pl.multiple_of(index * step_rows, step_rows), step_rows), :],
            stage_sem.at[slot],
        )

    def weight_grads(events):
        @pl.loop(0, count)
        def _(index):
            for at, event in events:

                @pl.when(index == at)
                def _():
                    event()

            slot = lax.rem(index, 2)
            cols = pl.ds(pl.multiple_of(index * step_rows, step_rows), step_rows)

            @pl.when(index >= 2)
            def _():
                save(index - 2, slot).wait()

            x = seq[:, :, cols].reshape(n * rows_all, step_rows)
            g = cot[:, :, cols].reshape(n * rows_all, step_rows)
            for at, left, right in ((0, x, dgate), (1, x, dup), (2, g, hid)):
                value = right[...].reshape(n * rows_all, units)
                stage[slot, :, at * units : (at + 1) * units] = mm(left, value, 0, 0).astype(BF16)
            save(index, slot).start()

    hid_save = pltpu.make_async_copy(hid, hid_hbm, local_sem.at[2])

    def receive_rows(hop, piece):
        @pl.when(within(piece, pieces))
        def _():
            gather.receive(hop, piece)

    @pl.loop(0, pieces + n - 1)
    def _(step):
        first = step < pieces
        ready = step - (n - 1)
        receive_rows(n - 1, ready)

        @pl.when(step + 1 < pieces)
        def _():
            scatter.start_ends(step + 1)

        @pl.when(ready == 0)
        def _():
            own_load.wait()
            weight_load.wait()

        @pl.when(ready >= 0)
        def _():
            far_arrived(ready)
            feed(ready)
            scatter_back.start_ends(ready)

        @pl.when(first)
        def _():
            scatter.middle(step)

            @pl.when(step + 2 < pieces)
            def _():
                far_start(step + 2)

        for hop in range(n - 2, 1, -1):
            receive_rows(hop, step - hop)

        @pl.when(ready >= 1)
        def _():
            scatter_back.middle(ready - 1)

        if n > 2:
            receive_rows(1, step - 1)

        @pl.when(first)
        def _():
            norm(step)
            gather.start_own(step)

        @pl.when(ready == 2)
        def _():
            scatter.finish(ends=False)

        @pl.when(ready >= 2)
        def _():
            back(ready - 2)

    hid_save.start()
    last = pieces - 1

    events = [
        (count // 4, lambda: scatter_back.first(last)),
        (count * 5 // 8, lambda: scatter_back.rest(last)),
    ]
    weight_grads(events)

    @pl.loop(max(last - 1, 0), pieces)
    def _(piece):
        back(piece)

    low_save = pltpu.make_async_copy(buf.at[me], low_hbm, local_sem.at[4])
    low_save.start()
    scatter.finish(middles=False)
    gather.finish()
    scatter_back.finish()

    @pl.loop(0, pieces)
    def _(piece):
        far_sent(piece)
        piece_save(1, mid_ref, mid_hbm, piece).wait()
        piece_save(2, grad_ref, grad_hbm, piece).wait()

    low_save.wait()
    hid_save.wait()
    for index in range(max(count - 2, 0), count):
        save(index, index % 2).wait()


def mlp(n, part, x, gain, weights, cotangent, near, pieces=4):
    rows, width = x.shape
    units = weights.shape[1] // 3
    any_spec = pl.BlockSpec(memory_space=pl.ANY)
    return pl.pallas_call(
        functools.partial(mlp_kernel, n, pieces),
        out_shape=(
            jax.ShapeDtypeStruct((1, width), F32),
            jax.ShapeDtypeStruct((rows, width), F32),
            jax.ShapeDtypeStruct((rows, width), F32),
            jax.ShapeDtypeStruct((n, rows, units), BF16),
            jax.ShapeDtypeStruct((width, 3 * units), BF16),
            jax.ShapeDtypeStruct((rows, width), BF16),
        ),
        in_specs=[VMEM_SPEC] + [any_spec] * 5,
        out_specs=(VMEM_SPEC,) + (any_spec,) * 5,
        scratch_shapes=[
            pltpu.VMEM((n, rows, width), BF16),
            pltpu.VMEM((rows, width), BF16),
            pltpu.VMEM((rows, width), F32),
            pltpu.VMEM((rows, width), F32),
            pltpu.VMEM((width, 3 * units), BF16),
            pltpu.VMEM((n, rows, width), BF16),
            pltpu.VMEM((n, rows, width), BF16),
            pltpu.VMEM((n + 1, rows, width), BF16),
            pltpu.VMEM((n, rows, width), BF16),
            pltpu.VMEM((n + 1, rows, width), BF16),
            pltpu.VMEM((n, rows, units), BF16),
            pltpu.VMEM((n, rows, units), BF16),
            pltpu.VMEM((n, rows, units), BF16),
            pltpu.VMEM((2, min(LANES, width), 3 * units), BF16),
            pltpu.VMEM((rows, LANES), F32),
        ]
        + sems(n, pieces) * 4
        + [pltpu.SemaphoreType.DMA((5 + n,)), pltpu.SemaphoreType.DMA((2,)), pltpu.SemaphoreType.DMA((3, pieces))],
        compiler_params=pltpu.CompilerParams(
            collective_id=2, has_side_effects=True, vmem_limit_bytes=67043328
        ),
        cost_estimate=pl.CostEstimate(
            flops=18 * n * rows * width * units, bytes_accessed=500 * 1024 * 1024, transcendentals=0
        ),
        name="mlp",
    )(gain, part.reshape(n, rows, width), x, weights, cotangent, near)


def last_kernel(
    n, dp, pieces, gain_ref, dgain_mlp_ref, part_hbm, x_hbm, grad_mid_hbm, seq_hbm, out_ref, gains_ref,
    part_ref, x_ref, grad_mid_ref, seq_ref, total_ref, dgain_ref, packed, held, buf, ssend, srecv, gsend, grecv, load_sem,
):
    def part_load(piece):
        rows = piece_rows(piece, part_ref.shape[1] // pieces)
        return pltpu.make_async_copy(part_hbm.at[:, rows], part_ref.at[:, rows], load_sem.at[2 + piece])

    others = [
        pltpu.make_async_copy(x_hbm, x_ref, load_sem.at[0]),
        pltpu.make_async_copy(grad_mid_hbm, grad_mid_ref, load_sem.at[1]),
        pltpu.make_async_copy(seq_hbm, seq_ref, load_sem.at[2 + pieces]),
    ]
    for piece in range(pieces):
        part_load(piece).start()
    for load in others:
        load.start()
    line = Line(n)
    all_me = lax.axis_index("dp") * n + line.me
    barrier_all(n, dp)
    scatter = Scatter(line, part_ref, buf, ssend, srecv, pieces)
    part_load(0).wait()
    scatter.start_ends(0)
    for piece in range(1, pieces):
        part_load(piece).wait()
    for load in others:
        load.wait()
    dgain_ref[...] = jnp.zeros_like(dgain_ref)
    packed[...] = jnp.zeros_like(packed)

    width = x_ref.shape[1]
    per = width // (n * dp)
    half = pieces // 2
    share = x_ref.shape[0] // half

    def exchange(**kind):
        exchange_all(
            n, dp, lambda peer: packed.at[peer], lambda source: held.at[source], gsend, grecv, **kind
        )

    def gain_share(index):
        rows = piece_rows(index, share)
        x = seq_ref[:, rows, :].reshape(n * share, width).astype(F32)
        term = part_ref[:, rows, :].reshape(n * share, width).astype(F32)
        inv = lax.rsqrt(jnp.mean(x * x, axis=1, keepdims=True) + EPS)
        dgain_ref[...] += jnp.sum(term * x * inv, axis=0, keepdims=True)

    def send_gains():
        for device in range(n * dp):
            cols = slice(device * per, (device + 1) * per)
            packed[device, :, :per] = dgain_ref[:, cols]
            packed[device, :, per : 2 * per] = dgain_mlp_ref[:, cols]
        held[all_me] = packed[all_me]
        exchange(start_only=True)

    @pl.loop(0, pieces)
    def _(piece):
        @pl.when(piece + 1 < pieces)
        def _():
            scatter.start_ends(piece + 1)

        @pl.when(piece < half)
        def _():
            gain_share(piece)

        @pl.when(piece == half)
        def _():
            send_gains()

        scatter.middle(piece)
        rows = scatter.rows(piece)

        def store(total):
            total_ref[...] = total

        scatter.result(piece, store)
        grad = total_ref[...]
        x = x_ref[rows, :].astype(F32)
        inv = lax.rsqrt(jnp.mean(x * x, axis=1, keepdims=True) + EPS)
        scaled = grad * gain_ref[...]
        mean = jnp.mean(scaled * x, axis=1, keepdims=True)
        out = grad_mid_ref[rows, :] + inv * (scaled - x * (inv * inv * mean))
        out_ref[rows, :] = out.astype(BF16)

    exchange(wait_only=True)
    gains_ref[...] = jnp.sum(held[...], axis=0)
    scatter.finish()


def sum_input_grad(n, dp, part, x, gain, grad_mid, dgain_mlp, seq, packed, pieces=8):
    rows, width = x.shape
    any_spec = pl.BlockSpec(memory_space=pl.ANY)
    return pl.pallas_call(
        functools.partial(last_kernel, n, dp, pieces),
        out_shape=(
            jax.ShapeDtypeStruct((rows, width), BF16),
            jax.ShapeDtypeStruct((1, packed), F32),
        ),
        in_specs=[VMEM_SPEC] * 2 + [any_spec] * 4,
        out_specs=(VMEM_SPEC,) * 2,
        scratch_shapes=[
            pltpu.VMEM((n, rows, width), BF16),
            pltpu.VMEM((rows, width), BF16),
            pltpu.VMEM((rows, width), F32),
            pltpu.VMEM((n, rows, width), BF16),
            pltpu.VMEM((rows // pieces, width), F32),
            pltpu.VMEM((1, width), F32),
            pltpu.VMEM((n * dp, 1, packed), F32),
            pltpu.VMEM((n * dp, 1, packed), F32),
            pltpu.VMEM((n + 1, rows, width), BF16),
        ]
        + sems(n, pieces)
        + [pltpu.SemaphoreType.DMA((n * dp,)), pltpu.SemaphoreType.DMA((n * dp,))]
        + [pltpu.SemaphoreType.DMA((3 + pieces,))],
        compiler_params=comm_params(4),
        cost_estimate=pl.CostEstimate(flops=0, bytes_accessed=250 * 1024 * 1024, transcendentals=0),
        name="sum_input_grad",
    )(gain, dgain_mlp, part.reshape(n, rows, width), x, grad_mid, seq)


def widen_kernel(
    mlp_ref, attn_ref, gains_ref, rows_ref, input_ref,
    gate_ref, up_ref, down_ref, query_ref, key_ref, value_ref, out_ref,
    attn_gain_ref, mlp_gain_ref, rows_out_ref, input_out_ref,
):
    units = gate_ref.shape[1]
    per = attn_gain_ref.shape[1]
    attn_gain_ref[...] = gains_ref[:, :per]
    mlp_gain_ref[...] = gains_ref[:, per : 2 * per]
    rows_out_ref[...] = rows_ref[...]
    input_out_ref[...] = input_ref[...]
    gate_ref[...] = mlp_ref[:, :units].astype(F32)
    up_ref[...] = mlp_ref[:, units : 2 * units].astype(F32)
    down_ref[...] = mlp_ref[:, 2 * units :].astype(F32).T
    q_cols, k_cols = query_ref.shape[1], key_ref.shape[0]
    query_ref[...] = attn_ref[:, :q_cols].astype(F32)
    key_ref[...] = attn_ref[:, q_cols : q_cols + k_cols].astype(F32).T
    value_ref[...] = attn_ref[:, q_cols + k_cols : q_cols + 2 * k_cols].astype(F32).T
    out_ref[...] = attn_ref[:, q_cols + 2 * k_cols :].astype(F32).T


def widen(mlp_grad, attn_grad, gains, rows_out, input_out, per, q_cols, k_cols):
    rows, units = mlp_grad.shape[0], mlp_grad.shape[1] // 3
    shapes = [(rows, units)] * 2 + [(units, rows), (rows, q_cols)] + [(k_cols, rows)] * 2 + [(q_cols, rows)]
    return pl.pallas_call(
        widen_kernel,
        out_shape=tuple(jax.ShapeDtypeStruct(shape, F32) for shape in shapes + [(1, per)] * 2)
        + (jax.ShapeDtypeStruct(rows_out.shape, BF16),) * 2,
        in_specs=[VMEM_SPEC] * 5,
        out_specs=(VMEM_SPEC,) * 11,
        compiler_params=pltpu.CompilerParams(vmem_limit_bytes=56 * 1024 * 1024),
        name="widen",
    )(mlp_grad, attn_grad, gains, rows_out, input_out)


def rotate(half_a, half_b, cos, sin):
    return half_a * cos - half_b * sin, half_b * cos + half_a * sin


def unrotate(half_a, half_b, cos, sin):
    return half_a * cos + half_b * sin, half_b * cos - half_a * sin


def mask_block(size):
    key = lax.broadcasted_iota(jnp.int32, (size, size), 0)
    row = lax.broadcasted_iota(jnp.int32, (size, size), 1)
    return jnp.where(key <= row, 0.0, NEG_LARGE)


def attend_kernel(
    n, dp, heads, block, pieces, x_ref, gain_ref, cos_ref, sin_ref, cot_hbm, wq_hbm, wk_hbm, wv_hbm, wo_hbm,
    attn_gain_ref, mlp_gain_ref, kv_ref, out_ref, log_ref, norm_hbm, qkv_hbm, part_hbm, w_out_hbm, wo_out_hbm, near_hbm, seq_hbm,
    norm_ref, qkv_ref, part_ref, w_ref, wo_ref, seq, act_ref, mask_ref, gains, wq, wk, wv, wo, send, recv, gsend, grecv, wsend, wrecv, own_sem, csend, crecv, fsend, frecv, save_sem,
):
    half = HEAD_SIZE // 2
    rows_all, width = x_ref.shape
    length = n * rows_all
    line = Line(n)
    me = line.me
    mine = lax.axis_index("dp")
    barrier_all(n, dp)
    seq[me] = x_ref[...]
    gains[mine * n + me] = gain_ref[...]
    gather = Gather(line, seq, send, recv, pieces)

    @pl.loop(0, pieces)
    def _(piece):
        gather.start_own(piece)

    def gain_rows(**kind):
        exchange_all(
            n, dp, lambda peer: gain_ref, lambda source: gains.at[source], gsend, grecv, **kind
        )

    gain_rows(start_only=True)

    shards = ((wq_hbm, wq), (wk_hbm, wk), (wv_hbm, wv), (wo_hbm, wo))
    own = [pltpu.make_async_copy(src, dst.at[mine], own_sem.at[i]) for i, (src, dst) in enumerate(shards)]
    pair = mine + 1 - 2 * lax.rem(mine, 2)

    def even_copy(i, offset):
        src, dst = shards[i]
        return pltpu.make_async_remote_copy(
            src_ref=src,
            dst_ref=dst.at[mine],
            send_sem=wsend.at[0, i, offset],
            recv_sem=wrecv.at[0, i, offset],
            device_id={"dp": lax.rem(mine + 2 * offset, dp)},
            device_id_type=MESH,
        )

    def pair_copy(i, offset):
        dst = shards[i][1].at[lax.rem(mine + 2 * offset, dp)]
        return pltpu.make_async_remote_copy(
            src_ref=dst,
            dst_ref=dst,
            send_sem=wsend.at[1, i, offset],
            recv_sem=wrecv.at[1, i, offset],
            device_id={"dp": pair},
            device_id_type=MESH,
        )

    for i in range(4):
        own[i].start()

    @pl.loop(1, dp // 2)
    def _(offset):
        for i in range(4):
            even_copy(i, offset).start()

    def cot_copy(right, hop):
        d = 0 if right else 1
        shard = me - (hop - 1) if right else me + (hop - 1)
        src = cot_hbm if hop == 1 else near_hbm.at[shard]
        return line.copy(src, near_hbm.at[shard], csend.at[d, hop - 1], crecv.at[d, hop - 1], 1 if right else -1)

    inner = (me > 0) & (me < n - 1)

    @pl.when(me == 0)
    def _():
        cot_copy(True, 1).start()

    @pl.when(me == n - 1)
    def _():
        cot_copy(False, 1).start()

    q_cols, k_cols = wq.shape[2], wk.shape[1]
    w_rows, w_cols = wq.shape[1], wo.shape[2]

    saves = [
        pltpu.make_async_copy(src, dst, save_sem.at[i])
        for i, (src, dst) in enumerate(
            (
                (w_ref, w_out_hbm),
                (wo_ref, wo_out_hbm),
                (norm_ref, norm_hbm),
                (qkv_ref, qkv_hbm),
                (seq, seq_hbm),
            )
        )
    ]

    def project(shard):
        x = seq[shard].astype(F32)
        inv = lax.rsqrt(jnp.mean(x * x, axis=1, keepdims=True) + EPS)
        norm = (x * inv * attn_gain_ref[...]).astype(BF16)
        rows = piece_rows(shard, rows_all)
        norm_ref[rows, :] = norm
        act_ref[:, rows] = mm(w_ref[...], norm, 0, 1)

    def prepare():
        gain_rows(wait_only=True)
        per = width // (n * dp)
        for device in range(n * dp):
            attn_gain_ref[:, device * per : (device + 1) * per] = gains[device, :, :per]
            mlp_gain_ref[:, device * per : (device + 1) * per] = gains[device, :, per : 2 * per]

        @pl.loop(0, dp // 2)
        def _(offset):
            for i in range(4):
                pair_copy(i, offset).wait_recv()

        for d in range(dp):
            rows = slice(d * w_rows, (d + 1) * w_rows)
            w_ref[rows, :q_cols] = wq[d]
            w_ref[rows, q_cols : q_cols + k_cols] = wk[d].T
            w_ref[rows, q_cols + k_cols :] = wv[d].T
            wo_ref[:, d * w_cols : (d + 1) * w_cols] = wo[d]
        saves[0].start()
        saves[1].start()

    def start_pair():
        for i in range(4):
            own[i].wait()

        @pl.loop(1, dp // 2)
        def _(offset):
            for i in range(4):
                even_copy(i, offset).wait_recv()

        @pl.loop(0, dp // 2)
        def _(offset):
            for i in range(4):
                pair_copy(i, offset).start()

    def arrived(d, hop, shard):
        cot_copy_in(
            line, near_hbm, shard, crecv.at[d, hop - 1], csend.at[d, hop - 1], 1 if d == 1 else -1
        ).wait_recv()

    ready = min(2, n - 1)
    for hop in range(1, ready + 1):

        @pl.loop(0, pieces)
        def _(piece):
            gather.receive(hop, piece)
            if hop == ready:

                @pl.when(piece == pieces // 2)
                def _():
                    start_pair()

        @pl.when((me == hop) & (me < n - 1))
        def _():
            cot_copy(True, 1).start()

        @pl.when((n - 1 - me == hop) & (me > 0))
        def _():
            cot_copy(False, 1).start()

    if n == 4:

        @pl.when(me == 1)
        def _():
            arrived(0, 1, me - 1)
            cot_copy(True, 2).start()

        @pl.when(me == 2)
        def _():
            arrived(1, 1, me + 1)
            cot_copy(False, 2).start()

    prepare()

    @pl.loop(0, 2 * n - 1)
    def _(turn):
        hop = (turn + 1) // 2
        leftward = lax.rem(turn, 2) == 1
        shard = jnp.where(leftward, me - hop, me + hop)

        @pl.when(leftward & (hop > ready))
        def _():
            @pl.loop(0, pieces)
            def _(piece):
                gather.receive(hop, piece)

        @pl.when(within(shard, n))
        def _():
            project(shard)

    saves[4].start()

    def far_copy(right, shard):
        part = near_hbm.at[shard, pl.ds(0, rows_all // pieces * FAR_DONE)]
        d = 0 if right else 1
        return line.copy(part, part, fsend.at[d], frecv.at[d], jnp.where(inner, 1 if right else -1, jnp.where(me == 0, 1, -1)))

    if n == 4:

        @pl.when(me == 1)
        def _():
            arrived(1, 1, me + 1)
            far_copy(False, me + 1).start()

        @pl.when(me == 2)
        def _():
            arrived(0, 1, me - 1)
            far_copy(True, me - 1).start()

    cos, sin = cos_ref[...], sin_ref[...]

    scale = 1.0 / math.sqrt(HEAD_SIZE)

    @pl.loop(0, heads + 1)
    def _(h):
        base = pl.multiple_of(h * HEAD_SIZE, HEAD_SIZE)
        a, b = rotate(act_ref[pl.ds(base, half), :], act_ref[pl.ds(base + half, half), :], cos, sin)
        factor = jnp.where(h < heads, scale, 1.0)
        a, b = a * factor, b * factor
        qkv_ref[pl.ds(base, half), :] = a.astype(BF16)
        qkv_ref[pl.ds(base + half, half), :] = b.astype(BF16)

    values = pl.ds((heads + 1) * HEAD_SIZE, HEAD_SIZE)
    qkv_ref[values, :] = act_ref[values, :].astype(BF16)
    saves[2].start()
    saves[3].start()
    mask_ref[...] = mask_block(block)
    kv_ref[...] = qkv_ref[pl.ds(heads * HEAD_SIZE, 2 * HEAD_SIZE), :].T

    @pl.loop(0, heads)
    def _(h):
        base = pl.multiple_of(h * HEAD_SIZE, HEAD_SIZE)
        for i in range(length // block):
            cols = pl.ds(i * block, block)
            query = qkv_ref[pl.ds(base, HEAD_SIZE), cols]
            scores = []
            peak = None
            for j in range(i + 1):
                s = mm(kv_ref[pl.ds(j * block, block), :HEAD_SIZE], query)
                if i == j:
                    s = s + mask_ref[...]
                top = jnp.max(s, axis=0, keepdims=True)
                peak = top if peak is None else jnp.maximum(peak, top)
                scores.append(s)
            weights = [jnp.exp(s - peak) for s in scores]
            total = sum(jnp.sum(w, axis=0, keepdims=True) for w in weights)
            log_ref[pl.ds(h, 1), cols] = peak + jnp.log(total)
            inverse = 1.0 / total
            mixed = None
            for j in range(i + 1):
                w = (weights[j] * inverse).astype(BF16)
                v = qkv_ref[values, pl.ds(j * block, block)]
                term = mm(v, w)
                mixed = term if mixed is None else mixed + term
            out_ref[pl.ds(base, HEAD_SIZE), cols] = mixed.astype(BF16)

    def part_save(index):
        cols = piece_rows(index, tile)
        return pltpu.make_async_copy(part_ref.at[:, cols], part_hbm.at[:, cols], save_sem.at[len(saves) + index])

    tile = even_tile(width)

    @pl.loop(0, width // tile)
    def _(index):
        cols = piece_rows(index, tile)
        part_ref[:, cols] = mm(out_ref[...], wo_ref[:, cols], 0, 0).astype(BF16)
        part_save(index).start()

    gather.finish()
    for save in saves:
        save.wait()

    @pl.loop(0, width // tile)
    def _(index):
        part_save(index).wait()

    @pl.loop(1, dp // 2)
    def _(offset):
        for i in range(4):
            even_copy(i, offset).wait_send()

    @pl.loop(0, dp // 2)
    def _(offset):
        for i in range(4):
            pair_copy(i, offset).wait_send()

    if n == 4:

        @pl.when(me == 1)
        def _():
            arrived(1, 2, me + 2)
            cot_copy(True, 2).wait_send()
            far_copy(False, me + 1).wait_send()

        @pl.when(me == 2)
        def _():
            arrived(0, 2, me - 2)
            cot_copy(False, 2).wait_send()
            far_copy(True, me - 1).wait_send()

        @pl.when(me == 0)
        def _():
            far_copy(False, me + 2).wait_recv()

        @pl.when(me == n - 1)
        def _():
            far_copy(True, me - 2).wait_recv()

    else:

        @pl.when(inner)
        def _():
            arrived(0, 1, me - 1)
            arrived(1, 1, me + 1)

    @pl.when(me == 0)
    def _():
        arrived(1, 1, me + 1)

    @pl.when(me == n - 1)
    def _():
        arrived(0, 1, me - 1)

    @pl.when(me < n - 1)
    def _():
        cot_copy(True, 1).wait_send()

    @pl.when(me > 0)
    def _():
        cot_copy(False, 1).wait_send()


def cot_copy_in(line, near_hbm, shard, recv, send, step):
    part = near_hbm.at[shard]
    return line.copy(part, part, send, recv, step)


def attend(n, dp, x, gains, weights, cos, sin, cotangent, block=256, pieces=4):
    assert n <= 4 and dp % 2 == 0
    rows, width = x.shape
    length = n * rows
    q_cols, k_cols = weights[0].shape[1], weights[1].shape[0]
    cols_in = q_cols + 2 * k_cols
    heads = cols_in // HEAD_SIZE - 2
    any_spec = pl.BlockSpec(memory_space=pl.ANY)
    dma = pltpu.SemaphoreType.DMA
    return pl.pallas_call(
        functools.partial(attend_kernel, n, dp, heads, block, pieces),
        out_shape=(
            jax.ShapeDtypeStruct((1, width), F32),
            jax.ShapeDtypeStruct((1, width), F32),
            jax.ShapeDtypeStruct((length, 2 * HEAD_SIZE), BF16),
            jax.ShapeDtypeStruct((heads * HEAD_SIZE, length), BF16),
            jax.ShapeDtypeStruct((heads, length), F32),
            jax.ShapeDtypeStruct((length, width), BF16),
            jax.ShapeDtypeStruct((cols_in, length), BF16),
            jax.ShapeDtypeStruct((length, width), BF16),
            jax.ShapeDtypeStruct((width, cols_in), BF16),
            jax.ShapeDtypeStruct((q_cols, width), BF16),
            jax.ShapeDtypeStruct((n,) + cotangent.shape, BF16),
            jax.ShapeDtypeStruct((n, rows, width), BF16),
        ),
        in_specs=[VMEM_SPEC] * 4 + [any_spec] * 5,
        out_specs=(VMEM_SPEC,) * 5 + (any_spec,) * 7,
        scratch_shapes=[
            pltpu.VMEM((length, width), BF16),
            pltpu.VMEM((cols_in, length), BF16),
            pltpu.VMEM((length, width), BF16),
            pltpu.VMEM((width, cols_in), BF16),
            pltpu.VMEM((q_cols, width), BF16),
            pltpu.VMEM((n, rows, width), BF16),
            pltpu.VMEM((cols_in, length), F32),
            pltpu.VMEM((block, block), F32),
            pltpu.VMEM((n * dp, 1, gains.shape[1]), F32),
        ]
        + [pltpu.VMEM((dp,) + w.shape, BF16) for w in weights]
        + sems(n, pieces)
        + [dma((n * dp,)), dma((n * dp,)), dma((2, 4, dp // 2)), dma((2, 4, dp // 2)), dma((4,))]
        + [dma((2, 2)), dma((2, 2)), dma((2,)), dma((2,)), dma((5 + width // even_tile(width),))],
        compiler_params=comm_params(1),
        cost_estimate=pl.CostEstimate(
            flops=2 * length * width * (cols_in + q_cols),
            bytes_accessed=350 * 1024 * 1024,
            transcendentals=heads * length * length,
        ),
        name="attend",
    )(x, gains, cos, sin, cotangent, *weights)


def attend_back_kernel(
    n, heads, block, pieces, kv_ref, log_ref, cos_ref, sin_ref,
    mid_hbm, low_hbm, hid_hbm, w_mlp_hbm, wo_hbm, w_hbm, qkv_hbm, out_hbm, norm_hbm,
    rows_ref, part_hbm, wgrad_hbm,
    mid_ref, part_ref, seq, hid, w_down, down_ref, buf, wo_ref, w_ref, qkv_ref, out_ref, norm_ref,
    dkv, mask_ref, grad_ref, dqkv_ref, wgrad, ssend, srecv, gsend, grecv, load_sem, save_sem,
):
    half = HEAD_SIZE // 2
    rows_all, width = mid_ref.shape
    units = hid.shape[2]
    cols_in = qkv_ref.shape[0]
    scale = 1.0 / math.sqrt(HEAD_SIZE)
    me = lax.axis_index("tensor")
    pairs = (
        (low_hbm, seq.at[me]),
        (hid_hbm, hid),
        (w_mlp_hbm.at[:, pl.ds(2 * units, units)], w_down),
        (wo_hbm, wo_ref),
        (qkv_hbm, qkv_ref),
        (out_hbm, out_ref),
        (w_hbm, w_ref),
        (norm_hbm, norm_ref),
        (mid_hbm, mid_ref),
    )
    loads = [pltpu.make_async_copy(src, dst, load_sem.at[i]) for i, (src, dst) in enumerate(pairs)]
    for load in loads:
        load.start()
    line = Line(n)
    line.barrier()
    scatter = Scatter(line, down_ref, buf, ssend, srecv, pieces)
    gather = Gather(line, seq, gsend, grecv, pieces)
    loads[0].wait()

    @pl.loop(0, pieces)
    def _(piece):
        gather.start_own(piece)

    dkv[...] = jnp.zeros_like(dkv)
    mask_ref[...] = mask_block(block)
    keys = pl.ds(heads * HEAD_SIZE, HEAD_SIZE)

    def project(shard):
        grad_ref[:, piece_rows(shard, rows_all)] = mm(wo_ref[...], seq[shard], 1, 1).astype(BF16)

    tile = even_tile(width)

    def start_sums():
        loads[1].wait()
        loads[2].wait()

        @pl.loop(0, pieces)
        def _(piece):
            rows = scatter.rows(piece)

            @pl.loop(0, width // tile)
            def _(index):
                cols = piece_rows(index, tile)
                value = hid[:, rows, :].reshape(n * scatter.size, units)
                value = mm(value, w_down[cols, :], 1, 1).astype(BF16)
                down_ref[:, rows, cols] = value.reshape(n, scatter.size, tile)

            scatter.start_ends(piece)

    def sum_piece(piece):
        scatter.middle(piece)
        rows = scatter.rows(piece)

        def store(total):
            rows_ref[rows, :] = (mid_ref[rows, :] + total).astype(BF16)

        scatter.result(piece, store)

    start_sums()
    for load in loads[3:]:
        load.wait()

    def attention_rows(i):
        cols = pl.ds(i * block, block)
        cos, sin = cos_ref[:, cols], sin_ref[:, cols]

        @pl.loop(0, heads)
        def _(h):
            base = pl.multiple_of(h * HEAD_SIZE, HEAD_SIZE)
            mine = pl.ds(base, HEAD_SIZE)
            query = qkv_ref[mine, cols]
            grad = grad_ref[mine, cols]
            delta = jnp.sum(
                grad.astype(F32) * out_ref[mine, cols].astype(F32), axis=0, keepdims=True
            )
            log_total = log_ref[pl.ds(h, 1), cols]
            dquery = None
            for j in range(i + 1):
                rows = pl.ds(j * block, block)
                s = mm(kv_ref[rows, :HEAD_SIZE], query)
                if i == j:
                    s = s + mask_ref[...]
                probs = jnp.exp(s - log_total)
                dprobs = mm(kv_ref[rows, HEAD_SIZE:], grad)
                dscores = (probs * (dprobs - delta)).astype(BF16)
                dkv[0, rows, :] += mm(dscores, query, 1, 1)
                dkv[1, rows, :] += mm(probs.astype(BF16), grad, 1, 1)
                term = mm(qkv_ref[keys, rows], dscores)
                dquery = term if dquery is None else dquery + term
            dquery = dquery * scale
            a, b = unrotate(dquery[:half], dquery[half:], cos, sin)
            dqkv_ref[pl.ds(base, half), cols] = a.astype(BF16)
            dqkv_ref[pl.ds(base + half, half), cols] = b.astype(BF16)

    @pl.loop(0, 2 * n - 1)
    def _(turn):
        hop = (turn + 1) // 2
        leftward = lax.rem(turn, 2) == 1
        shard = jnp.where(leftward, me - hop, me + hop)

        @pl.when(leftward)
        def _():
            @pl.loop(0, pieces)
            def _(piece):
                gather.receive(hop, piece)

        @pl.when(within(shard, n))
        def _():
            project(shard)
            for i in range(n):

                @pl.when(shard == i)
                def _():
                    attention_rows(i)

        @pl.when(jnp.logical_not(leftward) & within(hop - 1, min(n, pieces) - 1))
        def _():
            sum_piece(hop - 1)

    dkeys = dkv[0].T
    a, b = unrotate(dkeys[:half], dkeys[half:], cos_ref[...], sin_ref[...])
    dqkv_ref[pl.ds(heads * HEAD_SIZE, half), :] = a.astype(BF16)
    dqkv_ref[pl.ds(heads * HEAD_SIZE + half, half), :] = b.astype(BF16)
    dqkv_ref[pl.ds((heads + 1) * HEAD_SIZE, HEAD_SIZE), :] = dkv[1].T.astype(BF16)

    def part_save(index):
        cols = piece_rows(index, tile)
        return pltpu.make_async_copy(part_ref.at[:, cols], part_hbm.at[:, cols], save_sem.at[0, index])

    def wgrad_save(index):
        rows = piece_rows(index, tile)
        return pltpu.make_async_copy(wgrad.at[rows, :], wgrad_hbm.at[rows, :], save_sem.at[1, index])

    @pl.loop(0, width // tile)
    def _(index):
        cols = piece_rows(index, tile)
        part_ref[:, cols] = mm(dqkv_ref[...], w_ref[cols, :], 0, 1).astype(BF16)
        part_save(index).start()

    @pl.loop(0, width // tile)
    def _(index):
        cols = piece_rows(index, tile)
        wgrad[cols, :cols_in] = mm(norm_ref[:, cols], dqkv_ref[...], 0, 1).astype(BF16)
        for shard in range(n):
            term = mm(seq[shard, :, cols], out_ref[:, shard * rows_all : (shard + 1) * rows_all], 0, 1)
            total = term if shard == 0 else total + term
        wgrad[cols, cols_in:] = total.astype(BF16)
        wgrad_save(index).start()

    for piece in range(min(n, pieces) - 1, pieces):
        sum_piece(piece)
    scatter.finish()
    gather.finish()

    @pl.loop(0, width // tile)
    def _(index):
        part_save(index).wait()
        wgrad_save(index).wait()


def attend_back(
    n, mid, kv, log_total, cos, sin, low, hidden, w_mlp, w_out, w_qkv, qkv, out, norm, pieces=4
):
    rows, width = mid.shape
    block = rows
    length = n * rows
    cols_in = qkv.shape[0]
    heads = cols_in // HEAD_SIZE - 2
    units = hidden.shape[2]
    any_spec = pl.BlockSpec(memory_space=pl.ANY)
    wgrad_shape = (width, cols_in + w_out.shape[0])
    return pl.pallas_call(
        functools.partial(attend_back_kernel, n, heads, block, pieces),
        out_shape=(
            jax.ShapeDtypeStruct((rows, width), BF16),
            jax.ShapeDtypeStruct((length, width), BF16),
            jax.ShapeDtypeStruct(wgrad_shape, BF16),
        ),
        in_specs=[VMEM_SPEC] * 4 + [any_spec] * 9,
        out_specs=(VMEM_SPEC,) + (any_spec,) * 2,
        scratch_shapes=[
            pltpu.VMEM(mid.shape, F32),
            pltpu.VMEM((length, width), BF16),
            pltpu.VMEM((n, rows, width), BF16),
            pltpu.VMEM((n, rows, units), BF16),
            pltpu.VMEM((width, units), BF16),
            pltpu.VMEM((n, rows, width), BF16),
            pltpu.VMEM((n + 1, rows, width), BF16),
            pltpu.VMEM(w_out.shape, BF16),
            pltpu.VMEM(w_qkv.shape, BF16),
            pltpu.VMEM(qkv.shape, BF16),
            pltpu.VMEM(out.shape, BF16),
            pltpu.VMEM(norm.shape, BF16),
            pltpu.VMEM((2, length, HEAD_SIZE), F32),
            pltpu.VMEM((block, block), F32),
            pltpu.VMEM((heads * HEAD_SIZE, length), BF16),
            pltpu.VMEM((cols_in, length), BF16),
            pltpu.VMEM(wgrad_shape, BF16),
        ]
        + sems(n, pieces) * 2
        + [pltpu.SemaphoreType.DMA((9,)), pltpu.SemaphoreType.DMA((2, width // even_tile(width)))],
        compiler_params=comm_params(3),
        cost_estimate=pl.CostEstimate(
            flops=6 * length * width * wgrad_shape[1],
            bytes_accessed=350 * 1024 * 1024,
            transcendentals=heads * length * length,
        ),
        name="attend_back",
    )(kv, log_total, cos, sin, mid, low, hidden, w_mlp, w_out, w_qkv, qkv, out, norm)


def local(
    n, dp, x, gain_attn, gain_mlp, w_query, w_key, w_value, w_out, w_gate, w_up, w_down, cotangent
):
    rows, _ = x.shape
    length = n * rows
    per = gain_attn.shape[0]
    packed = 2 * per + (-2 * per) % LANES

    mlp_all = lax.all_gather(
        jnp.concatenate([w_gate, w_up, w_down.T], axis=1), "dp", axis=0, tiled=True
    )
    gains = [gain_attn, gain_mlp]
    if packed > 2 * per:
        gains.append(jnp.zeros((packed - 2 * per,), F32))
    cos, sin = tables(length)
    full_attn, full_mlp, kv, attended, log_total, norm_attn, qkv, out_part, w_qkv, w_out_all, near, x_seq = attend(
        n,
        dp,
        x,
        jnp.concatenate(gains).reshape(1, packed),
        (w_query, w_key.T, w_value.T, w_out),
        cos,
        sin,
        cotangent,
    )
    dgain_mlp, mid, grad_mid, hidden, mlp_grad, grad_low = mlp(
        n, out_part, x, full_mlp, mlp_all, cotangent, near
    )
    mlp_grad = lax.psum_scatter(mlp_grad, "dp", scatter_dimension=0, tiled=True)
    block_output, attn_part, attn_grad = attend_back(
        n, mid, kv, log_total, cos, sin, grad_low, hidden, mlp_all, w_out_all, w_qkv, qkv, attended, norm_attn
    )
    attn_grad = lax.psum_scatter(attn_grad, "dp", scatter_dimension=0, tiled=True)
    input_grad, dgains = sum_input_grad(
        n, dp, attn_part, x, full_attn, grad_mid, dgain_mlp, x_seq, packed
    )
    gate, up, down, query, key, value, out, dgain_attn, dgain_mlp, block_output, input_grad = widen(
        mlp_grad, attn_grad, dgains, block_output, input_grad, per, w_query.shape[1], w_key.shape[1]
    )
    return (
        block_output,
        input_grad,
        dgain_attn.reshape(per),
        dgain_mlp.reshape(per),
        query,
        key.T,
        value.T,
        out,
        gate,
        up,
        down,
    )


def solution(mesh):
    rows = P(("dp", "tensor"), None)
    gain = P(("dp", "tensor"))
    into = P("dp", "tensor")
    back = P("tensor", "dp")
    in_specs = (rows, gain, gain, into, into, into, back, into, into, back, rows)
    out_specs = (rows, rows, gain, gain, into, into, into, back, into, into, back)

    def body(*args):
        return local(mesh.shape["tensor"], mesh.shape["dp"], *args)

    return jax.shard_map(body, mesh=mesh, in_specs=in_specs, out_specs=out_specs, check_vma=False)
```
